1024 devices in a mesh: grp: 8 (over x, y_lo), sub: 128 (over z, y_hi, core).
Axes of the slice: x: 4, y: 8 (y_hi: 4, y_lo: 2; y = y_hi * 2 + y_lo), z: 16, core: 2. Of those that a mesh axis runs over, the one named last changes fastest.
Arguments:
- reg_disp: float32 [8, 128, 3, 384], P('grp', 'sub'), may hold values from -6 to 6
- reg_vel: float32 [8, 128, 3, 384], P('grp', 'sub'), may hold values from -0.6 to 0.6
- site_disp: float32 [8, 128, 3, 1536], P('grp', 'sub'), may hold values from -6 to 6
- site_vel: float32 [8, 128, 3, 1536], P('grp', 'sub'), may hold values from -0.6 to 0.6
- reg_nodes: int32 [8, 128, 10, 256], P('grp', 'sub'), may hold values from 0 to 383
- site_nodes: int32 [8, 128, 35, 128], P('grp', 'sub'), may hold values from 0 to 1535
- reg_coefs: float32 [8, 128, 3, 3, 4, 256], P('grp', 'sub'), may hold values from -1.5 to 6, as said below
- site_coefs: float32 [8, 128, 3, 3, 24, 128], P('grp', 'sub'), may hold values from -1.5 to 6, as said below
- reg_table: float32 [12, 10], replicated, may hold values from -2 to 2
- site_table: float32 [72, 35], replicated, may hold values from -1 to 1
- reg_minv: float32 [8, 128, 384], P('grp', 'sub'), may hold values from 0.003 to 0.015
- site_minv: float32 [8, 128, 1536], P('grp', 'sub'), may hold values from 0.003 to 0.015
- reg_send: int32 [8, 128, 2, 128], P('grp', 'sub'), may hold values from 0 to 383
- reg_recv: int32 [8, 128, 2, 128], P('grp', 'sub'), may hold values from 0 to 383
- site_send: int32 [8, 128, 2, 128], P('grp', 'sub'), may hold values from 0 to 1535
- site_recv: int32 [8, 128, 2, 128], P('grp', 'sub'), may hold values from 0 to 1535
- slot_fill: int32 [8, 128, 4], P('grp', 'sub'), may hold values from 1 to 128, 384 in all within a row
- layer_src: int32 [8, 128, 128], P('grp', 'sub'), may hold values from 0 to 383
- layer_fill: int32 [8, 128], P('grp', 'sub'), may hold values from 64 to 128, as said below
- layer_dst: int32 [8, 128, 3, 128], P('grp', 'sub'), may hold values from 0 to 1535
- layer_stiff: float32 [8, 128, 3, 128], P('grp', 'sub'), may hold values from 0.5 to 2
Outputs:
- reg_final: float32 [8, 128, 3, 384], P('grp', 'sub')
- site_final: float32 [8, 128, 3, 1536], P('grp', 'sub')
The draws below stay inside these ranges and needn't reach their ends.
Inputs may be any that keep to these rules, and one draw needn't show every extreme that they name: `slot_fill`: per partition the four entries count live slots toward the lower and higher neighbour, regional then site; they sum to 384. `layer_fill`: partition index 0 of every group fills all 128 slots. `reg_coefs`: each 3 x 3 tensor over the first two dimensions is symmetric positive definite. `site_coefs`: each 3 x 3 tensor over the first two dimensions is symmetric positive definite.
All inputs are finite; a program needn't handle non-finite values.
Results may differ from the reference program's by a relative error of at most 0.0003.
Values sent between devices are 32-bit elements; how exact they have to be, the bound alone decides.
A program may use at most 64 MiB of HBM per device.

```python
import math
import jax
import jax.numpy as jnp
import numpy as np
from jax import lax

PR = 10
QR = 4
PS = 35
QS = 24
STEPS = 8
ES = 128
SLOTS = 128
DRM = 128
ER = 256
NR = 384
NS = 1536
N_GRP = 8
N_SUB = 128


def tensor_draw(key, quad_count, elem_count):
    first_key, second_key = jax.random.split(key)
    shape_diag = (N_GRP, N_SUB, 3, quad_count, elem_count)
    diagonal = jnp.exp(jax.random.uniform(first_key, shape_diag, jnp.float32, math.log(0.5), math.log(4.0)))
    off_diag = jax.random.uniform(second_key, (N_GRP, N_SUB, 3, 3, quad_count, elem_count), jnp.float32, -0.25, 0.25)
    off_diag = 0.5 * (off_diag + jnp.swapaxes(off_diag, 2, 3))
    identity = jnp.eye(3, dtype=jnp.float32)[:, :, None, None]
    off_diag = off_diag * (1.0 - identity)
    root_scale = jnp.sqrt(diagonal)
    return root_scale[:, :, :, None] * root_scale[:, :, None, :] * (identity + off_diag)


def draw_reg_coefs(key, part):
    return tensor_draw(jax.random.fold_in(key, 11), QR, ER)


def draw_site_coefs(key, part):
    return tensor_draw(jax.random.fold_in(key, 23), QS, ES)


def draw_layer_fill(key, part):
    counts = jax.random.randint(jax.random.fold_in(key, 37), (N_GRP, N_SUB), DRM // 2, DRM + 1, dtype=jnp.int32)
    return counts.at[:, 0].set(DRM)


def touch_ends(array, rng, low, high):
    place = [jax.random.randint(jax.random.fold_in(rng, axis), (), 0, length) for axis, length in enumerate(array.shape)]
    main_axis = array.shape.index(max(array.shape))
    next_to = place[:main_axis] + [(place[main_axis] + 1) % array.shape[main_axis]] + place[main_axis + 1:]
    return array.at[tuple(place)].set(low).at[tuple(next_to)].set(high)


def block_scale(key, shape, shards, low, high):
    def one(dim, blocks):
        heights = jax.random.uniform(jax.random.fold_in(jax.random.fold_in(key, 6), dim), (blocks,), jnp.float32, low / len(shards), high / len(shards))
        return jnp.repeat(jnp.exp(heights), shape[dim] // blocks).reshape((-1,) + (1,) * (len(shape) - dim - 1))

    loudness = one(*shards[0])
    for cut in shards[1:]:
        loudness = loudness * one(*cut)
    return loudness


def length_profile(count, total, bound, slope):
    weights = [(1 << 20) // math.isqrt(grade ** slope) + 1 for grade in range(2, count + 1)]
    surplus, given = total - bound - (count - 1), [1] * (count - 1)
    while surplus > 0:
        free = [i for i in range(count - 1) if given[i] < bound]
        whole, budget = sum([weights[i] for i in free]), surplus
        for i in free:
            more = min(bound - given[i], max(1, budget * weights[i] // whole), surplus)
            given[i] = given[i] + more
            surplus = surplus - more
    return np.array([bound] + given)


def ragged_sizes(stream_key, amount, total, limit, lean):
    if amount == 2:
        one = jax.random.randint(stream_key, (), max(1, total - limit), min(limit, total - 1) + 1)
        return jnp.stack([one, total - one])
    tallies = jnp.asarray(length_profile(amount, total, limit, lean), jnp.int32)
    couples = (amount - 1) // 2
    donor, sink = tallies[1:1 + 2 * couples:2], tallies[2:2 + 2 * couples:2]
    margin = jnp.minimum(donor - 1, limit - sink)
    passed = jax.random.randint(jax.random.fold_in(stream_key, 1), (couples,), 0, 1 << 20) % (margin + 1)
    tallies = tallies.at[1:1 + 2 * couples:2].set(donor - passed).at[2:2 + 2 * couples:2].set(sink + passed)
    return tallies[jax.random.permutation(jax.random.fold_in(stream_key, 2), amount)]


def scatter_about(rng, shape, spread, bound, shards=(), held_as=jnp.bfloat16):
    entries = jax.random.normal(rng, shape, jnp.float32) * spread
    if len(shards) > 0:
        entries = block_scale(rng, shape, shards, -0.22, 0.18) * entries
    return jnp.clip(entries, min=-bound, max=bound).astype(held_as)


def setup_inputs(seed: int = 0) -> dict:
    key_list = jax.random.split(jax.random.key(seed), 22)
    reg_disp = scatter_about(key_list[0], (N_GRP, N_SUB, 3, NR), 1.0, 6.0, ((0, 8), (1, 128)), jnp.float32)
    reg_vel = scatter_about(key_list[1], (N_GRP, N_SUB, 3, NR), 0.1, 0.6, ((0, 8), (1, 128)), jnp.float32)
    site_disp = scatter_about(key_list[2], (N_GRP, N_SUB, 3, NS), 1.0, 6.0, ((0, 8), (1, 128)), jnp.float32)
    site_vel = scatter_about(key_list[3], (N_GRP, N_SUB, 3, NS), 0.1, 0.6, ((0, 8), (1, 128)), jnp.float32)
    reg_nodes = touch_ends(jax.random.randint(key_list[4], (N_GRP, N_SUB, PR, ER), 0, NR), jax.random.fold_in(key_list[4], 1), 0, NR - 1).astype(jnp.int32)
    site_nodes = touch_ends(jax.random.randint(key_list[5], (N_GRP, N_SUB, PS, ES), 0, NS), jax.random.fold_in(key_list[5], 1), 0, NS - 1).astype(jnp.int32)
    reg_coefs = draw_reg_coefs(jax.random.fold_in(key_list[21], 71), 0)
    site_coefs = draw_site_coefs(jax.random.fold_in(key_list[21], 71), 0)
    reg_table = scatter_about(key_list[8], (3 * QR, PR), PR ** -0.5, 2.0, (), jnp.float32)
    site_table = scatter_about(key_list[9], (3 * QS, PS), PS ** -0.5, 1.0, (), jnp.float32)
    reg_minv = jnp.clip(jnp.exp(math.log(0.015) - 1.60943788 * jax.random.uniform(key_list[10], (N_GRP, N_SUB, NR), jnp.float32) ** block_scale(key_list[10], (N_GRP, N_SUB, NR), ((0, 8), (1, 128)), -0.2, 0.2)), 0.003, 0.015)
    site_minv = jnp.clip(jnp.exp(math.log(0.015) - 1.60943788 * jax.random.uniform(key_list[11], (N_GRP, N_SUB, NS), jnp.float32) ** block_scale(key_list[11], (N_GRP, N_SUB, NS), ((0, 8), (1, 128)), -0.2, 0.2)), 0.003, 0.015)
    reg_send = touch_ends(jax.random.randint(key_list[12], (N_GRP, N_SUB, 2, SLOTS), 0, NR), jax.random.fold_in(key_list[12], 1), 0, NR - 1).astype(jnp.int32)
    reg_recv = touch_ends(jax.random.randint(key_list[13], (N_GRP, N_SUB, 2, SLOTS), 0, NR), jax.random.fold_in(key_list[13], 1), 0, NR - 1).astype(jnp.int32)
    site_send = touch_ends(jax.random.randint(key_list[14], (N_GRP, N_SUB, 2, SLOTS), 0, NS), jax.random.fold_in(key_list[14], 1), 0, NS - 1).astype(jnp.int32)
    site_recv = touch_ends(jax.random.randint(key_list[15], (N_GRP, N_SUB, 2, SLOTS), 0, NS), jax.random.fold_in(key_list[15], 1), 0, NS - 1).astype(jnp.int32)
    slot_fill = jax.vmap(lambda own: ragged_sizes(own, 4, 3 * SLOTS, SLOTS, 0))(jax.random.split(key_list[16], N_GRP * N_SUB)).reshape((N_GRP, N_SUB, 4)).astype(jnp.int32)
    layer_src = touch_ends(jax.random.randint(key_list[17], (N_GRP, N_SUB, DRM), 0, NR), jax.random.fold_in(key_list[17], 1), 0, NR - 1).astype(jnp.int32)
    layer_fill = draw_layer_fill(jax.random.fold_in(key_list[21], 71), 0)
    layer_dst = touch_ends(jax.random.randint(key_list[19], (N_GRP, N_SUB, 3, DRM), 0, NS), jax.random.fold_in(key_list[19], 1), 0, NS - 1).astype(jnp.int32)
    layer_stiff = jnp.clip(jnp.exp(math.log(2.0) - 1.3862944 * jax.random.uniform(key_list[20], (N_GRP, N_SUB, 3, DRM), jnp.float32) ** block_scale(key_list[20], (N_GRP, N_SUB, 3, DRM), ((0, 8), (1, 128)), -0.2, 0.2)), 0.5, 2.0)
    return {"reg_disp": reg_disp, "reg_vel": reg_vel, "site_disp": site_disp, "site_vel": site_vel, "reg_nodes": reg_nodes, "site_nodes": site_nodes, "reg_coefs": reg_coefs, "site_coefs": site_coefs, "reg_table": reg_table, "site_table": site_table, "reg_minv": reg_minv, "site_minv": site_minv, "reg_send": reg_send, "reg_recv": reg_recv, "site_send": site_send, "site_recv": site_recv, "slot_fill": slot_fill, "layer_src": layer_src, "layer_fill": layer_fill, "layer_dst": layer_dst, "layer_stiff": layer_stiff}


PRECISE = lax.Precision.HIGHEST


def stiff_force(displaced, element_nodes, coef_block, deriv_table):
    quad_count = coef_block.shape[2]
    node_count = element_nodes.shape[0]
    elem_count = element_nodes.shape[1]
    flat_nodes = element_nodes.reshape(-1)
    gathered = jnp.take(displaced, flat_nodes, axis=1).reshape(3, node_count, elem_count)
    gradient = jnp.einsum("kp,cpe->cke", deriv_table, gathered, precision=PRECISE)
    pieces = [gradient[:, b * quad_count:(b + 1) * quad_count] for b in range(3)]
    flux_rows = [coef_block[a, 0][None] * pieces[0] + coef_block[a, 1][None] * pieces[1] + coef_block[a, 2][None] * pieces[2] for a in range(3)]
    flux_terms = jnp.concatenate(flux_rows, axis=1)
    element_terms = jnp.einsum("kp,cke->cpe", deriv_table, flux_terms, precision=PRECISE)
    return -jnp.zeros_like(displaced).at[:, flat_nodes].add(element_terms.reshape(3, -1))


def pack_slots(forces, send_map, fill_pair):
    picked = jnp.take(forces, send_map, axis=1)
    live_slots = jnp.arange(send_map.shape[1], dtype=jnp.int32)[None, :] < fill_pair[:, None]
    return jnp.where(live_slots[:, None, :], jnp.transpose(picked, (1, 0, 2)), 0.0)


def take_slots(forces, recv_map, from_lower, from_upper):
    return forces.at[:, recv_map[0]].add(from_lower).at[:, recv_map[1]].add(from_upper)


def pack_layer(displaced, layer_src, layer_fill):
    picked = jnp.take(displaced, layer_src, axis=1)
    live_slots = jnp.arange(layer_src.shape[0], dtype=jnp.int32) < layer_fill
    return jnp.where(live_slots[None, :], picked, 0.0)


def add_layer(forces, layer_dst, layer_stiff, layer_block):
    for source in range(3):
        forces = forces.at[:, layer_dst[source]].add(layer_stiff[source][None, :] * layer_block[source])
    return forces


def neighbour_terms(send_rows, group_rows):
    shaped = send_rows.reshape((group_rows, N_SUB) + send_rows.shape[1:])
    blank_rows = jnp.zeros_like(shaped[:, :1, 0])
    from_lower = jnp.concatenate([blank_rows, shaped[:, :-1, 1]], axis=1)
    from_upper = jnp.concatenate([shaped[:, 1:, 0], blank_rows], axis=1)
    width = send_rows.shape[-1]
    return from_lower.reshape(-1, 3, width), from_upper.reshape(-1, 3, width)


def reference(reg_disp, reg_vel, site_disp, site_vel, reg_nodes, site_nodes, reg_coefs, site_coefs, reg_table, site_table, reg_minv, site_minv, reg_send, reg_recv, site_send, site_recv, slot_fill, layer_src, layer_fill, layer_dst, layer_stiff):
    site_groups = N_GRP // 4
    reg_groups = 3 * site_groups

    def regional(stacked):
        return stacked[:reg_groups].reshape((reg_groups * N_SUB,) + stacked.shape[2:])

    def sitewise(stacked):
        return stacked[reg_groups:].reshape((site_groups * N_SUB,) + stacked.shape[2:])

    reg_now = regional(reg_disp)
    reg_prev = reg_now - regional(reg_vel)
    r_nodes, r_coefs, r_minv = regional(reg_nodes), regional(reg_coefs), regional(reg_minv)
    r_send, r_recv, r_fill = regional(reg_send), regional(reg_recv), regional(slot_fill)[:, 0:2]
    r_src, r_layer_fill = regional(layer_src), regional(layer_fill)
    layers = []
    for step_no in range(STEPS):
        forces = lax.map(lambda device_items: stiff_force(device_items[0], device_items[1], device_items[2], reg_table), (reg_now, r_nodes, r_coefs))
        send_rows = jax.vmap(pack_slots)(forces, r_send, r_fill)
        from_lower, from_upper = neighbour_terms(send_rows, reg_groups)
        forces = jax.vmap(take_slots)(forces, r_recv, from_lower, from_upper)
        reg_next = 2.0 * reg_now - reg_prev + r_minv[:, None, :] * forces
        reg_prev, reg_now = reg_now, reg_next
        layers.append(jax.vmap(pack_layer)(reg_now, r_src, r_layer_fill))

    site_now = sitewise(site_disp)
    site_prev = site_now - sitewise(site_vel)
    s_nodes, s_coefs, s_minv = sitewise(site_nodes), sitewise(site_coefs), sitewise(site_minv)
    s_send, s_recv, s_fill = sitewise(site_send), sitewise(site_recv), sitewise(slot_fill)[:, 2:4]
    s_dst, s_stiff = sitewise(layer_dst), sitewise(layer_stiff)
    for step_no in range(STEPS):
        forces = lax.map(lambda device_items: stiff_force(device_items[0], device_items[1], device_items[2], site_table), (site_now, s_nodes, s_coefs))
        send_rows = jax.vmap(pack_slots)(forces, s_send, s_fill)
        from_lower, from_upper = neighbour_terms(send_rows, site_groups)
        forces = jax.vmap(take_slots)(forces, s_recv, from_lower, from_upper)
        layer_block = layers[step_no].reshape(3, site_groups, N_SUB, 3, -1)
        layer_block = jnp.transpose(layer_block, (1, 2, 0, 3, 4)).reshape(site_groups * N_SUB, 3, 3, -1)
        forces = jax.vmap(add_layer)(forces, s_dst, s_stiff, layer_block)
        site_next = 2.0 * site_now - site_prev + s_minv[:, None, :] * forces
        site_prev, site_now = site_now, site_next

    reg_final = jnp.concatenate([reg_now.reshape((reg_groups, N_SUB) + reg_now.shape[1:]),
                                 jnp.zeros((site_groups, N_SUB) + reg_now.shape[1:], jnp.float32)], axis=0)
    site_final = jnp.concatenate([jnp.zeros((reg_groups, N_SUB) + site_now.shape[1:], jnp.float32),
                                  site_now.reshape((site_groups, N_SUB) + site_now.shape[1:])], axis=0)
    return reg_final, site_final
```

```python
import functools

import jax
import jax.numpy as jnp
from jax import lax
from jax.experimental import pallas as pl
from jax.experimental.pallas import tpu as pltpu
from jax.sharding import PartitionSpec as P

STEPS = 8
MESH = pl.DeviceIdType.MESH
SHIFT = 13
BIG = 2047 << SHIFT
F32 = jnp.float32
BF16 = jnp.bfloat16


def pad_to(value, unit):
    return -(-value // unit) * unit


class Kind:
    def __init__(self, points, quads, elems, nodes):
        self.P, self.Q, self.E, self.N = points, quads, elems, nodes
        self.LC = elems // 128
        self.NR = nodes // 128
        self.NRP = pad_to(self.NR, 8)
        self.PP = pad_to(points, 8)
        self.QP = pad_to(quads, 8)
        self.KQ = 3 * self.QP
        self.SR = self.LC * self.PP
        self.R = 8
        while self.R < self.SR:
            self.R *= 2
        self.LAST = points * elems // 128
        self.R2 = pad_to(self.LAST + 1, 8)
        self.W = 3 * elems
        self.rows = [k * self.PP + p for k in range(self.LC) for p in range(points)]


def lane_take(x, idx):
    dims = lax.GatherDimensionNumbers(
        offset_dims=(),
        collapsed_slice_dims=(1,),
        start_index_map=(1,),
        operand_batching_dims=(0,),
        start_indices_batching_dims=(0,),
    )
    return lax.gather(
        x, idx[..., None], dims, (1, 1), mode=lax.GatherScatterMode.PROMISE_IN_BOUNDS
    )


def iota2(shape, dim):
    return lax.broadcasted_iota(jnp.int32, shape, dim)


def spread(row):
    return jnp.broadcast_to(row, (8, 128))


def split(x):
    hi = x.astype(BF16).astype(F32)
    return hi, x - hi


def mm(a, b):
    return jnp.dot(a.astype(BF16), b.astype(BF16), preferred_element_type=F32)


def sort_regs(regs):
    count = len(regs)
    depth = count * 8
    row_bits = depth.bit_length() - 1
    sub = iota2((8, 128), 0)
    lane = iota2((8, 128), 1)

    def bit_mask(bit, v):
        if bit < 3:
            return (sub >> bit) & 1
        if bit < row_bits:
            return (v >> (bit - 3)) & 1
        if bit >= row_bits + 7:
            return 0
        return (lane >> (bit - row_bits)) & 1

    total_bits = row_bits + 7
    for m in range(1, total_bits + 1):
        for jb in range(m - 1, -1, -1):
            new = list(regs)
            if 3 <= jb < row_bits:
                step = 1 << (jb - 3)
                for v in range(count):
                    if v & step:
                        continue
                    a, b = regs[v], regs[v + step]
                    low, high = jnp.minimum(a, b), jnp.maximum(a, b)
                    down = bit_mask(m, v)
                    if isinstance(down, int):
                        new[v], new[v + step] = (high, low) if down else (low, high)
                    else:
                        new[v] = jnp.where(down == 1, high, low)
                        new[v + step] = jnp.where(down == 1, low, high)
            else:
                for v in range(count):
                    x = regs[v]
                    if jb < 3:
                        dist = 1 << jb
                        if dist == 4:
                            other = pltpu.roll(x, 4, 0)
                        else:
                            other = jnp.where(
                                bit_mask(jb, v) == 1, pltpu.roll(x, dist, 0), pltpu.roll(x, 8 - dist, 0)
                            )
                    else:
                        dist = 1 << (jb - row_bits)
                        other = lane_take(x, lane ^ dist)
                    take_max = bit_mask(jb, v) ^ bit_mask(m, v)
                    new[v] = jnp.where(take_max == 1, jnp.maximum(x, other), jnp.minimum(x, other))
            regs = new
    return regs


def gather_three(idx_row, idx_lane, load_row, rows):
    out = [jnp.zeros((8, 128), F32) for _ in range(3)]
    for r in rows:
        here = idx_row == r
        for c in range(3):
            out[c] = jnp.where(here, lane_take(spread(load_row(c, r)), idx_lane), out[c])
    return out


def setup_state(kind, disp, vel, u, prev):
    for ref in (u, prev):
        ref[...] = jnp.zeros(ref.shape, F32)
    for c in range(3):
        u[c : c + 1, :] = disp[0, c]
        prev[c : c + 1, :] = disp[0, c] - vel[0, c]


def setup_tables(kind, table, flipped, tpad, d1, d2):
    tpad[...] = jnp.zeros(tpad.shape, F32)
    if flipped:
        tpad[0 : kind.P, 0 : kind.KQ] = table[...]
        across = tpad[...]
        whole = across.T
    else:
        for b in range(3):
            tpad[b * kind.QP : b * kind.QP + kind.Q, 0 : kind.P] = table[b * kind.Q : (b + 1) * kind.Q, :]
        whole = tpad[...]
        across = whole.T
    hi, lo = split(across[0 : kind.PP])
    stack = [hi, hi, lo]
    left = 128 - 3 * kind.PP
    if left:
        stack.append(jnp.zeros((left, 128), F32))
    d1[...] = jnp.concatenate(stack, axis=0).T
    hi, lo = split(-whole[0 : kind.KQ])
    depth = d2.shape[1]
    stack = [hi, hi, lo]
    left = depth - 3 * kind.KQ
    if left:
        stack.append(jnp.zeros((left, 128), F32))
    stack = jnp.concatenate(stack, axis=0)
    for k in range(depth // 128):
        d2[:, k * 128 : (k + 1) * 128] = stack[k * 128 : (k + 1) * 128].T


def setup_plan(kind, nodes, node_s, key_s, plan_s, pos_s):
    sub = iota2((8, 128), 0)
    lane = iota2((8, 128), 1)
    node_s[...] = jnp.zeros(node_s.shape, jnp.int32)
    for k in range(kind.LC):
        for p in range(kind.P):
            at = k * kind.PP + p
            node_s[at : at + 1, :] = nodes[0, p, :, k * 128 : (k + 1) * 128]
    regs = []
    for v in range(kind.R // 8):
        if v * 8 >= kind.SR:
            regs.append(jnp.full((8, 128), BIG, jnp.int32))
            continue
        row = sub + v * 8
        inside = (row % kind.PP) < kind.P
        found = jnp.where(inside, node_s[v * 8 : v * 8 + 8, :], BIG >> SHIFT)
        regs.append((found << SHIFT) | (row << 7) | lane)
    regs = sort_regs(regs)
    for v, reg in enumerate(regs):
        key_s[v * 8 : v * 8 + 8, :] = reg
    bits = kind.R.bit_length() - 1
    for v in range(kind.R2 // 8):
        place = (sub + v * 8) * 128 + lane
        src_row, src_lane = place & (kind.R - 1), place >> bits
        out = jnp.zeros((8, 128), jnp.int32)
        for r in range(kind.R):
            out = jnp.where(src_row == r, lane_take(spread(key_s[r : r + 1, :]), src_lane), out)
        live = out < BIG
        slot = out & ((1 << SHIFT) - 1)
        plan_s[0, v * 8 : v * 8 + 8, :] = jnp.where(live, slot >> 7, 1000)
        plan_s[1, v * 8 : v * 8 + 8, :] = slot & 127
    last = spread(key_s[kind.R - 1 : kind.R, :])
    for v in range(kind.NRP // 8):
        target = ((sub + v * 8) * 128 + lane + 1) << SHIFT
        column = jnp.zeros((8, 128), jnp.int32)
        for step in (64, 32, 16, 8, 4, 2, 1):
            column = jnp.where(lane_take(last, column + (step - 1)) < target, column + step, column)
        count = jnp.zeros((8, 128), jnp.int32)
        for r in range(kind.R):
            count = count + jnp.where(lane_take(spread(key_s[r : r + 1, :]), column) < target, 1, 0)
        place = column * kind.R + count
        pos_s[0, v * 8 : v * 8 + 8, :] = place >> 7
        pos_s[1, v * 8 : v * 8 + 8, :] = place & 127


def setup_scan(scan):
    row = iota2(scan.shape, 0) % 128
    col = iota2(scan.shape, 1)
    scan[...] = jnp.where(row < col, 1.0, 0.0).astype(BF16)


def rows_ahead(kind, totals):
    sub = iota2((8, 128), 0)
    run = jnp.zeros((8, 128), F32)
    out = []
    for v in range(kind.R2 // 8):
        upto = totals[v * 8 : v * 8 + 8]
        for dist in (1, 2, 4):
            upto = upto + jnp.where(sub >= dist, pltpu.roll(upto, dist, 0), 0.0)
        out.append(run + jnp.where(sub >= 1, pltpu.roll(upto, 1, 0), 0.0))
        run = run + jnp.broadcast_to(upto[7:8], (8, 128))
    return out


def setup_hot(kind, maps, hot):
    rows = iota2((kind.N, 128), 0)
    for k, load in enumerate(maps):
        hot[:, k * 128 : (k + 1) * 128] = jnp.where(rows == load(), 1.0, 0.0).astype(BF16)


def stiff_force(kind, u, coef, node_s, plan_s, pos_s, d1, d2, scan, fe_s, cx_s, f_s):
    blocks = {}
    for k in range(kind.LC):
        for v in range(kind.PP // 8):
            at = k * kind.PP + v * 8
            index = node_s[at : at + 8, :]
            found = gather_three(
                index >> 7,
                index & 127,
                lambda c, r: u[c : c + 1, r * 128 : (r + 1) * 128],
                range(kind.NR),
            )
            for c in range(3):
                blocks[c, k, v] = found[c]
    chunks = [(c, k) for c in range(3) for k in range(kind.LC)]
    cols = []
    for c, k in chunks:
        ve = jnp.concatenate([blocks[c, k, v] for v in range(kind.PP // 8)], axis=0)
        hi, lo = split(ve)
        parts = [hi, lo, hi]
        left = 128 - 3 * kind.PP
        if left:
            parts.append(jnp.zeros((left, 128), F32))
        cols.append(jnp.concatenate(parts, axis=0).astype(BF16))
    gathered = jnp.concatenate(cols, axis=1)
    grad = jnp.dot(d1[0 : kind.KQ, :].astype(BF16), gathered, preferred_element_type=F32)
    cols = []
    depth = d2.shape[1]
    for i, (c, k) in enumerate(chunks):
        piece = grad[:, i * 128 : (i + 1) * 128]
        terms = []
        for a in range(3):
            total = coef(a, 0, k) * piece[0 : kind.QP]
            for b in (1, 2):
                total = total + coef(a, b, k) * piece[b * kind.QP : (b + 1) * kind.QP]
            terms.append(total)
        flux = jnp.concatenate(terms, axis=0)
        hi, lo = split(flux)
        parts = [hi, lo, hi]
        left = depth - 3 * kind.KQ
        if left:
            parts.append(jnp.zeros((left, 128), F32))
        cols.append(jnp.concatenate(parts, axis=0).astype(BF16))
    flux = jnp.concatenate(cols, axis=1)
    fe = jnp.dot(d2[0 : kind.PP, :].astype(BF16), flux, preferred_element_type=F32)
    for i, (c, k) in enumerate(chunks):
        fe_s[c, k * kind.PP : (k + 1) * kind.PP, :] = fe[:, i * 128 : (i + 1) * 128]
    cols = [[], [], []]
    for v in range(kind.R2 // 8):
        found = gather_three(
            plan_s[0, v * 8 : v * 8 + 8, :],
            plan_s[1, v * 8 : v * 8 + 8, :],
            lambda c, r: fe_s[c, r : r + 1, :],
            kind.rows,
        )
        for c in range(3):
            cols[c].append(found[c])
    both = []
    for c in range(3):
        hi, lo = split(jnp.concatenate(cols[c], axis=0))
        both.append(jnp.concatenate([hi, lo], axis=1).astype(BF16))
    sums = jnp.dot(jnp.concatenate(both, axis=0), scan[...], preferred_element_type=F32)
    for c in range(3):
        rows = sums[c * kind.R2 : (c + 1) * kind.R2]
        for v, ahead in enumerate(rows_ahead(kind, rows[:, 128:256])):
            cx_s[c, v * 8 : v * 8 + 8, :] = rows[v * 8 : v * 8 + 8, 0:128] + ahead
    corner_row = iota2((kind.NRP, 128), 0)
    corner_lane = iota2((kind.NRP, 128), 1)
    found = [
        gather_three(
            pos_s[0, v * 8 : v * 8 + 8, :],
            pos_s[1, v * 8 : v * 8 + 8, :],
            lambda c, r: cx_s[c, r : r + 1, :],
            range(kind.LAST + 1),
        )
        for v in range(kind.NRP // 8)
    ]
    for c in range(3):
        ends = jnp.concatenate([block[c] for block in found], axis=0)
        before = pltpu.roll(ends, 1, 1)
        above = pltpu.roll(before, 1, 0)
        before = jnp.where(corner_lane == 0, above, before)
        before = jnp.where((corner_lane == 0) & (corner_row == 0), 0.0, before)
        forces = ends - before
        for r in range(kind.NR):
            f_s[c : c + 1, r * 128 : (r + 1) * 128] = forces[r : r + 1, :]


def pick(kind, source, index):
    idx_row, idx_lane = spread(index >> 7), spread(index & 127)
    out = jnp.zeros((8, 128), F32)
    for r in range(kind.NR):
        out = jnp.where(
            idx_row == r, lane_take(source[:, r * 128 : (r + 1) * 128], idx_lane), out
        )
    return out


def drop(kind, parts, hot):
    r = jnp.concatenate(parts, axis=1)
    hi, lo = split(r)
    both = jnp.concatenate([hi, lo], axis=0).astype(BF16)
    out = lax.dot_general(
        both, hot[...], (((1,), (1,)), ((), ())), preferred_element_type=F32
    )
    return out[0:8] + out[8:16]


def body(
    reg, site, reg_groups, site_groups, sub_count,
    reg_disp, reg_vel, site_disp, site_vel, reg_nodes, site_nodes, reg_coefs, site_coefs,
    reg_table, site_table, reg_minv, site_minv, reg_send, reg_recv, site_send, site_recv,
    slot_fill, layer_src, layer_fill, layer_dst, layer_stiff,
    reg_out, site_out,
    u_r, prev_r, f_r, tpad_r, d1_r, d2_r, node_r, key_r, plan_r, pos_r, hot_r, fe_r, cx_r, coef_r,
    u_s, prev_s, f_s, tpad_s, d1_s, d2_s, node_s, key_s, plan_s, pos_s, hot_s, fe_s, cx_s,
    hot_l, scan, sends, recvs, layer_out, layer_in,
    send_sem, recv_sem, layer_send_sem, layer_recv_sem,
):
    grp = lax.axis_index("grp")
    sub = lax.axis_index("sub")
    is_site = grp >= reg_groups
    has_lower = sub > 0
    has_upper = sub < sub_count - 1
    source = grp // site_groups
    target = reg_groups + grp % site_groups
    barrier = pltpu.get_barrier_semaphore()

    def hello(g, s):
        pl.semaphore_signal(barrier, inc=1, device_id=(g, s), device_id_type=MESH)

    @pl.when(has_lower)
    def _():
        hello(grp, sub - 1)

    @pl.when(has_upper)
    def _():
        hello(grp, sub + 1)

    @pl.when(is_site)
    def _():
        for m in range(3):
            hello(m * site_groups + grp - reg_groups, sub)

    @pl.when(jnp.logical_not(is_site))
    def _():
        hello(target, sub)

    for there, side in ((has_lower, 0), (has_upper, 1)):

        @pl.when(jnp.logical_not(there))
        def _():
            for n in range(STEPS):
                recvs[n, side] = jnp.zeros((8, 128), F32)

    lane = iota2((8, 128), 1)
    greeted = has_lower.astype(jnp.int32) + has_upper.astype(jnp.int32) + jnp.where(is_site, 3, 1)

    def edge(n, side):
        peer = sub - 1 if side == 0 else sub + 1
        return pltpu.make_async_remote_copy(
            src_ref=sends.at[n, side],
            dst_ref=recvs.at[n, 1 - side],
            send_sem=send_sem.at[n, side],
            recv_sem=recv_sem.at[n, 1 - side],
            device_id=(grp, peer),
            device_id_type=MESH,
        )

    def layer_copy(n, m):
        return pltpu.make_async_remote_copy(
            src_ref=layer_out.at[n],
            dst_ref=layer_in.at[n, m],
            send_sem=layer_send_sem.at[n],
            recv_sem=layer_recv_sem.at[n, m],
            device_id=(target, sub),
            device_id_type=MESH,
        )

    sides = ((has_lower, 0), (has_upper, 1))

    def exchange(kind, n, f, send_map, fills):
        for there, side in sides:
            found = pick(kind, f, send_map[0, 0, side : side + 1, :])
            sends[n, side] = jnp.where(lane < fills[side], found, 0.0)

            @pl.when(there)
            def _():
                edge(n, side).start()

    def arrive(n):
        for there, side in sides:

            @pl.when(there)
            def _():
                edge(n, 1 - side).wait_recv()

    def finish(n, carry):
        for there, side in sides:

            @pl.when(there)
            def _():
                edge(n, side).wait_send()

        return carry

    setup_scan(scan)

    @pl.when(jnp.logical_not(is_site))
    def _():
        kind = reg
        setup_state(kind, reg_disp, reg_vel, u_r, prev_r)
        f_r[...] = jnp.zeros(f_r.shape, F32)
        setup_tables(kind, reg_table, False, tpad_r, d1_r, d2_r)
        coef_r[...] = jnp.zeros(coef_r.shape, F32)
        coef_r[:, :, 0 : kind.Q, :] = reg_coefs[0, 0]
        setup_plan(kind, reg_nodes, node_r, key_r, plan_r, pos_r)
        setup_hot(kind, [lambda i=i: reg_recv[0, 0, i : i + 1, :] for i in range(2)], hot_r)
        pl.semaphore_wait(barrier, greeted)
        fills = (slot_fill[0, 0, 0], slot_fill[0, 0, 1])

        def step(n, carry):
            stiff_force(
                kind, u_r, lambda a, b, k: coef_r[a, b, :, k * 128 : (k + 1) * 128],
                node_r, plan_r, pos_r, d1_r, d2_r, scan, fe_r, cx_r, f_r,
            )
            exchange(kind, n, f_r, reg_send, fills)
            minv = reg_minv[0]
            now = u_r[...]
            ahead = 2.0 * now - prev_r[...] + minv * f_r[...]
            prev_r[...] = now
            arrive(n)
            u_r[...] = ahead + minv * drop(kind, [recvs[n, 0], recvs[n, 1]], hot_r)
            found = pick(kind, u_r, layer_src[0])
            layer_out[n] = jnp.where(lane < layer_fill[0, 0], found, 0.0)
            layer_copy(n, source).start()
            return carry

        lax.fori_loop(0, STEPS, step, 0)
        for c in range(3):
            reg_out[0, c] = u_r[c : c + 1, :]
        site_out[...] = jnp.zeros(site_out.shape, F32)

        def drain(n, carry):
            layer_copy(n, source).wait_send()
            return finish(n, carry)

        lax.fori_loop(0, STEPS, drain, 0)

    @pl.when(is_site)
    def _():
        kind = site
        setup_state(kind, site_disp, site_vel, u_s, prev_s)
        f_s[...] = jnp.zeros(f_s.shape, F32)
        setup_tables(kind, site_table, True, tpad_s, d1_s, d2_s)
        setup_plan(kind, site_nodes, node_s, key_s, plan_s, pos_s)
        setup_hot(kind, [lambda i=i: site_recv[0, 0, i : i + 1, :] for i in range(2)], hot_s)
        setup_hot(kind, [lambda i=i: layer_dst[0, i] for i in range(3)], hot_l)
        pl.semaphore_wait(barrier, greeted)
        fills = (slot_fill[0, 0, 2], slot_fill[0, 0, 3])

        def step(n, carry):
            stiff_force(
                kind, u_s, lambda a, b, k: site_coefs[0, 0, a, b],
                node_s, plan_s, pos_s, d1_s, d2_s, scan, fe_s, cx_s, f_s,
            )
            exchange(kind, n, f_s, site_send, fills)
            minv = site_minv[0]
            now = u_s[...]
            ahead = 2.0 * now - prev_s[...] + minv * f_s[...]
            prev_s[...] = now
            parts = []
            for m in range(3):
                layer_copy(n, m).wait_recv()
                parts.append(layer_in[n, m] * layer_stiff[0, m])
            ahead = ahead + minv * drop(kind, parts, hot_l)
            arrive(n)
            u_s[...] = ahead + minv * drop(kind, [recvs[n, 0], recvs[n, 1]], hot_s)
            return carry

        lax.fori_loop(0, STEPS, step, 0)
        for c in range(3):
            site_out[0, c] = u_s[c : c + 1, :]
        reg_out[...] = jnp.zeros(reg_out.shape, F32)
        lax.fori_loop(0, STEPS, finish, 0)


def kind_scratch(kind):
    depth = pad_to(3 * kind.KQ, 128)
    i32 = jnp.int32
    return [
        pltpu.VMEM((8, kind.N), F32),
        pltpu.VMEM((8, kind.N), F32),
        pltpu.VMEM((8, kind.N), F32),
        pltpu.VMEM((128, 128), F32),
        pltpu.VMEM((128, 128), F32),
        pltpu.VMEM((128, depth), F32),
        pltpu.VMEM((kind.SR, 128), i32),
        pltpu.VMEM((kind.R, 128), i32),
        pltpu.VMEM((2, kind.R2, 128), i32),
        pltpu.VMEM((2, kind.NRP, 128), i32),
        pltpu.VMEM((kind.N, 256), BF16),
        pltpu.VMEM((3, kind.SR, 128), F32),
        pltpu.VMEM((3, kind.R2, 128), F32),
    ]


def shards(*args):
    group_count = lax.axis_size("grp")
    site_groups = group_count // 4
    reg_groups = 3 * site_groups
    reg = Kind(args[4].shape[2], args[6].shape[4], args[4].shape[3], args[0].shape[3])
    site = Kind(args[5].shape[2], args[7].shape[4], args[5].shape[3], args[2].shape[3])
    args = list(args)
    for i in (0, 1, 2, 3, 4, 5, 19, 20):
        args[i] = jnp.transpose(args[i], (0, 2, 1, 3))
    args[9] = args[9].T
    vmem = pl.BlockSpec(memory_space=pltpu.VMEM)
    smem = pl.BlockSpec(memory_space=pltpu.SMEM)
    in_specs = [vmem] * len(args)
    in_specs[16] = smem
    in_specs[18] = smem
    kernel = functools.partial(body, reg, site, reg_groups, site_groups, lax.axis_size("sub"))
    outs = pl.pallas_call(
        kernel,
        name="drm_window",
        out_shape=(
            jax.ShapeDtypeStruct((1, 3, 1, reg.N), F32),
            jax.ShapeDtypeStruct((1, 3, 1, site.N), F32),
        ),
        in_specs=in_specs,
        out_specs=(vmem, vmem),
        scratch_shapes=kind_scratch(reg)
        + [pltpu.VMEM((3, 3, reg.QP, reg.E), F32)]
        + kind_scratch(site)
        + [
            pltpu.VMEM((site.N, 384), BF16),
            pltpu.VMEM((256, 256), BF16),
            pltpu.VMEM((STEPS, 2, 8, 128), F32),
            pltpu.VMEM((STEPS, 2, 8, 128), F32),
            pltpu.VMEM((STEPS, 8, 128), F32),
            pltpu.VMEM((STEPS, 3, 8, 128), F32),
            pltpu.SemaphoreType.DMA((STEPS, 2)),
            pltpu.SemaphoreType.DMA((STEPS, 2)),
            pltpu.SemaphoreType.DMA((STEPS,)),
            pltpu.SemaphoreType.DMA((STEPS, 3)),
        ],
        compiler_params=pltpu.CompilerParams(collective_id=0, has_side_effects=True),
    )(*args)
    return tuple(jnp.transpose(out, (0, 2, 1, 3)) for out in outs)


def solution(mesh):
    whole = P("grp", "sub")
    specs = [whole] * 21
    specs[8] = P()
    specs[9] = P()
    return jax.shard_map(
        shards,
        mesh=mesh,
        in_specs=tuple(specs),
        out_specs=(whole, whole),
        check_vma=False,
    )
```

```python
import functools

import jax
import jax.numpy as jnp
from jax import lax
from jax.experimental import pallas as pl
from jax.experimental.pallas import tpu as pltpu
from jax.sharding import PartitionSpec as P

STEPS = 8
MESH = pl.DeviceIdType.MESH
SHIFT = 13
BIG = 2047 << SHIFT
F32 = jnp.float32
BF16 = jnp.bfloat16


def pad_to(value, unit):
    return -(-value // unit) * unit


class Kind:
    def __init__(self, points, quads, elems, nodes):
        self.P, self.Q, self.E, self.N = points, quads, elems, nodes
        self.LC = elems // 128
        self.NR = nodes // 128
        self.NRP = pad_to(self.NR, 8)
        self.PP = pad_to(points, 8)
        self.QP = pad_to(quads, 8)
        self.KQ = 3 * self.QP
        self.SR = self.LC * self.PP
        self.W8 = self.SR // 8


def lane_take(x, idx):
    dims = lax.GatherDimensionNumbers(
        offset_dims=(),
        collapsed_slice_dims=(1,),
        start_index_map=(1,),
        operand_batching_dims=(0,),
        start_indices_batching_dims=(0,),
    )
    return lax.gather(
        x, idx[..., None], dims, (1, 1), mode=lax.GatherScatterMode.PROMISE_IN_BOUNDS
    )


def iota2(shape, dim):
    return lax.broadcasted_iota(jnp.int32, shape, dim)


def spread(row):
    return jnp.broadcast_to(row, (8, 128))


def split(x):
    hi = x.astype(BF16).astype(F32)
    return hi, x - hi


def mm(a, b):
    return jnp.dot(a.astype(BF16), b.astype(BF16), preferred_element_type=F32)


def sort_regs(regs):
    count = len(regs)
    depth = count * 8
    row_bits = depth.bit_length() - 1
    sub = iota2((8, 128), 0)
    lane = iota2((8, 128), 1)

    def bit_mask(bit, v):
        if bit < 3:
            return (sub >> bit) & 1
        if bit < row_bits:
            return (v >> (bit - 3)) & 1
        if bit >= row_bits + 7:
            return 0
        return (lane >> (bit - row_bits)) & 1

    total_bits = row_bits + 7
    for m in range(1, total_bits + 1):
        for jb in range(m - 1, -1, -1):
            new = list(regs)
            if 3 <= jb < row_bits:
                step = 1 << (jb - 3)
                for v in range(count):
                    if v & step:
                        continue
                    a, b = regs[v], regs[v + step]
                    low, high = jnp.minimum(a, b), jnp.maximum(a, b)
                    down = bit_mask(m, v)
                    if isinstance(down, int):
                        new[v], new[v + step] = (high, low) if down else (low, high)
                    else:
                        new[v] = jnp.where(down == 1, high, low)
                        new[v + step] = jnp.where(down == 1, low, high)
            else:
                for v in range(count):
                    x = regs[v]
                    if jb < 3:
                        dist = 1 << jb
                        if dist == 4:
                            other = pltpu.roll(x, 4, 0)
                        else:
                            other = jnp.where(
                                bit_mask(jb, v) == 1, pltpu.roll(x, dist, 0), pltpu.roll(x, 8 - dist, 0)
                            )
                    else:
                        dist = 1 << (jb - row_bits)
                        other = lane_take(x, lane ^ dist)
                    take_max = bit_mask(jb, v) ^ bit_mask(m, v)
                    new[v] = jnp.where(take_max == 1, jnp.maximum(x, other), jnp.minimum(x, other))
            regs = new
    return regs


def gather_three(idx_row, idx_lane, load_row, rows):
    out = [jnp.zeros((8, 128), F32) for _ in range(3)]
    for r in rows:
        here = idx_row == r
        for c in range(3):
            out[c] = jnp.where(here, lane_take(spread(load_row(c, r)), idx_lane), out[c])
    return out


def setup_state(kind, disp, vel, u, prev):
    for ref in (u, prev):
        ref[...] = jnp.zeros(ref.shape, F32)
    for c in range(3):
        u[c : c + 1, :] = disp[0, c]
        prev[c : c + 1, :] = disp[0, c] - vel[0, c]


def setup_tables(kind, table, flipped, tpad, d1, d2):
    tpad[...] = jnp.zeros(tpad.shape, F32)
    if flipped:
        tpad[0 : kind.P, 0 : kind.KQ] = table[...]
        across = tpad[...]
        whole = across.T
    else:
        for b in range(3):
            tpad[b * kind.QP : b * kind.QP + kind.Q, 0 : kind.P] = table[b * kind.Q : (b + 1) * kind.Q, :]
        whole = tpad[...]
        across = whole.T
    hi, lo = split(across[0 : kind.PP])
    stack = [hi, hi, lo]
    left = 128 - 3 * kind.PP
    if left:
        stack.append(jnp.zeros((left, 128), F32))
    d1[...] = jnp.concatenate(stack, axis=0).T
    hi, lo = split(-whole[0 : kind.KQ])
    depth = d2.shape[1]
    stack = [hi, hi, lo]
    left = depth - 3 * kind.KQ
    if left:
        stack.append(jnp.zeros((left, 128), F32))
    stack = jnp.concatenate(stack, axis=0)
    for k in range(depth // 128):
        d2[:, k * 128 : (k + 1) * 128] = stack[k * 128 : (k + 1) * 128].T


def setup_plan(kind, nodes, send_map, node_s, key_s, plan_s, pos_s):
    sub = iota2((8, 128), 0)
    lane = iota2((8, 128), 1)
    node_s[...] = jnp.zeros(node_s.shape, jnp.int32)
    for k in range(kind.LC):
        for p in range(kind.P):
            at = k * kind.PP + p
            node_s[at : at + 1, :] = nodes[0, p, :, k * 128 : (k + 1) * 128]
    for w in range(kind.W8):
        inside = ((sub + w * 8) % kind.PP) < kind.P
        found = jnp.where(inside, node_s[w * 8 : w * 8 + 8, :], BIG >> SHIFT)
        keys = sort_regs([(found << SHIFT) | (sub << 7) | lane])[0]
        key_s[w * 8 : w * 8 + 8, :] = keys
        slot = keys & ((1 << SHIFT) - 1)
        plan_s[0, w * 8 : w * 8 + 8, :] = jnp.where(keys < BIG, slot >> 7, 1000)
        plan_s[1, w * 8 : w * 8 + 8, :] = slot & 127
    targets = [((sub + v * 8) * 128 + lane + 1) << SHIFT for v in range(kind.NRP // 8)]
    sent = jnp.zeros((8, 128), jnp.int32)
    for side in range(2):
        wanted = spread(send_map[0, 0, side : side + 1, :])
        sent = jnp.where(sub == 2 * side, wanted + 1, sent)
        sent = jnp.where(sub == 2 * side + 1, wanted, sent)
    targets.append(sent << SHIFT)
    for w in range(kind.W8):
        last = spread(key_s[w * 8 + 7 : w * 8 + 8, :])
        for v, target in enumerate(targets):
            column = jnp.zeros((8, 128), jnp.int32)
            for step in (64, 32, 16, 8, 4, 2, 1):
                column = jnp.where(lane_take(last, column + (step - 1)) < target, column + step, column)
            place = column * 8 - 1
            for r in range(8):
                row = spread(key_s[w * 8 + r : w * 8 + r + 1, :])
                place = place + jnp.where(lane_take(row, column) < target, 1, 0)
            pos_s[v, w, 0] = jnp.where(place < 0, 1000, place & 7)
            pos_s[v, w, 1] = jnp.where(place < 0, 0, place >> 3)


def setup_scan(scan):
    row = iota2(scan.shape, 0) % 128
    col = iota2(scan.shape, 1)
    scan[...] = jnp.where(row < col, 1.0, 0.0).astype(BF16)


def setup_hot(kind, maps, hot):
    rows = iota2((kind.N, 128), 0)
    for k, load in enumerate(maps):
        hot[:, k * 128 : (k + 1) * 128] = jnp.where(rows == load(), 1.0, 0.0).astype(BF16)


def stiff_force(kind, u, coef, node_s, plan_s, d1, d2, scan, fe_s, cx_s):
    blocks = {}
    for k in range(kind.LC):
        for v in range(kind.PP // 8):
            at = k * kind.PP + v * 8
            index = node_s[at : at + 8, :]
            found = gather_three(
                index >> 7,
                index & 127,
                lambda c, r: u[c : c + 1, r * 128 : (r + 1) * 128],
                range(kind.NR),
            )
            for c in range(3):
                blocks[c, k, v] = found[c]
    chunks = [(c, k) for c in range(3) for k in range(kind.LC)]
    cols = []
    for c, k in chunks:
        ve = jnp.concatenate([blocks[c, k, v] for v in range(kind.PP // 8)], axis=0)
        hi, lo = split(ve)
        parts = [hi, lo, hi]
        left = 128 - 3 * kind.PP
        if left:
            parts.append(jnp.zeros((left, 128), F32))
        cols.append(jnp.concatenate(parts, axis=0).astype(BF16))
    gathered = jnp.concatenate(cols, axis=1)
    grad = jnp.dot(d1[0 : kind.KQ, :].astype(BF16), gathered, preferred_element_type=F32)
    cols = []
    depth = d2.shape[1]
    for i, (c, k) in enumerate(chunks):
        piece = grad[:, i * 128 : (i + 1) * 128]
        terms = []
        for a in range(3):
            total = coef(a, 0, k) * piece[0 : kind.QP]
            for b in (1, 2):
                total = total + coef(a, b, k) * piece[b * kind.QP : (b + 1) * kind.QP]
            terms.append(total)
        flux = jnp.concatenate(terms, axis=0)
        hi, lo = split(flux)
        parts = [hi, lo, hi]
        left = depth - 3 * kind.KQ
        if left:
            parts.append(jnp.zeros((left, 128), F32))
        cols.append(jnp.concatenate(parts, axis=0).astype(BF16))
    flux = jnp.concatenate(cols, axis=1)
    fe = jnp.dot(d2[0 : kind.PP, :].astype(BF16), flux, preferred_element_type=F32)
    for i, (c, k) in enumerate(chunks):
        fe_s[c, k * kind.PP : (k + 1) * kind.PP, :] = fe[:, i * 128 : (i + 1) * 128]
    sub = iota2((8, 128), 0)
    terms = {}
    both = []
    for w in range(kind.W8):
        found = gather_three(
            plan_s[0, w * 8 : w * 8 + 8, :],
            plan_s[1, w * 8 : w * 8 + 8, :],
            lambda c, r: fe_s[c, w * 8 + r : w * 8 + r + 1, :],
            [r for r in range(8) if (w * 8 + r) % kind.PP < kind.P],
        )
        for c in range(3):
            hi, lo = split(found[c])
            both.append(jnp.concatenate([hi, lo], axis=1))
            upto = found[c]
            for dist in (1, 2, 4):
                upto = upto + jnp.where(sub >= dist, pltpu.roll(upto, dist, 0), 0.0)
            terms[w, c] = upto
    sums = jnp.dot(
        jnp.concatenate(both, axis=0).astype(BF16), scan[...], preferred_element_type=F32
    )
    for w in range(kind.W8):
        for c in range(3):
            at = (w * 3 + c) * 8
            ahead = sums[at : at + 8]
            for dist in (4, 2, 1):
                ahead = ahead + pltpu.roll(ahead, dist, 0)
            cx_s[c, w * 8 : w * 8 + 8, :] = terms[w, c] + ahead


def read_ends(kind, v, pos_s, cx_s):
    total = None
    for w in range(kind.W8):
        found = gather_three(
            pos_s[v, w, 0],
            pos_s[v, w, 1],
            lambda c, r: cx_s[c, w * 8 + r : w * 8 + r + 1, :],
            range(8),
        )
        total = found if total is None else [a + b for a, b in zip(total, found)]
    return total


def node_forces(kind, pos_s, cx_s, f_s):
    corner_row = iota2((kind.NRP, 128), 0)
    corner_lane = iota2((kind.NRP, 128), 1)
    found = [read_ends(kind, v, pos_s, cx_s) for v in range(kind.NRP // 8)]
    for c in range(3):
        ends = jnp.concatenate([block[c] for block in found], axis=0)
        before = pltpu.roll(ends, 1, 1)
        above = pltpu.roll(before, 1, 0)
        before = jnp.where(corner_lane == 0, above, before)
        before = jnp.where((corner_lane == 0) & (corner_row == 0), 0.0, before)
        forces = ends - before
        for r in range(kind.NR):
            f_s[c : c + 1, r * 128 : (r + 1) * 128] = forces[r : r + 1, :]


def pick(kind, source, index):
    idx_row, idx_lane = spread(index >> 7), spread(index & 127)
    out = jnp.zeros((8, 128), F32)
    for r in range(kind.NR):
        out = jnp.where(
            idx_row == r, lane_take(source[:, r * 128 : (r + 1) * 128], idx_lane), out
        )
    return out


def drop(kind, parts, hot):
    r = jnp.concatenate(parts, axis=1)
    hi, lo = split(r)
    both = jnp.concatenate([hi, lo], axis=0).astype(BF16)
    out = lax.dot_general(
        both, hot[...], (((1,), (1,)), ((), ())), preferred_element_type=F32
    )
    return out[0:8] + out[8:16]


def body(
    reg, site, reg_groups, site_groups, sub_count,
    reg_disp, reg_vel, site_disp, site_vel, reg_nodes, site_nodes, reg_coefs, site_coefs,
    reg_table, site_table, reg_minv, site_minv, reg_send, reg_recv, site_send, site_recv,
    slot_fill, layer_src, layer_fill, layer_dst, layer_stiff,
    reg_out, site_out,
    u_r, prev_r, f_r, tpad_r, d1_r, d2_r, node_r, key_r, plan_r, pos_r, hot_r, fe_r, cx_r, coef_r,
    u_s, prev_s, f_s, tpad_s, d1_s, d2_s, node_s, key_s, plan_s, pos_s, hot_s, fe_s, cx_s,
    hot_l, scan, sends, recvs, layer_out, layer_in,
    send_sem, recv_sem, layer_send_sem, layer_recv_sem,
):
    grp = lax.axis_index("grp")
    sub = lax.axis_index("sub")
    is_site = grp >= reg_groups
    has_lower = sub > 0
    has_upper = sub < sub_count - 1
    source = grp // site_groups
    target = reg_groups + grp % site_groups
    barrier = pltpu.get_barrier_semaphore()

    def hello(g, s):
        pl.semaphore_signal(barrier, inc=1, device_id=(g, s), device_id_type=MESH)

    @pl.when(has_lower)
    def _():
        hello(grp, sub - 1)

    @pl.when(has_upper)
    def _():
        hello(grp, sub + 1)

    @pl.when(is_site)
    def _():
        for m in range(3):
            hello(m * site_groups + grp - reg_groups, sub)

    @pl.when(jnp.logical_not(is_site))
    def _():
        hello(target, sub)

    for there, side in ((has_lower, 0), (has_upper, 1)):

        @pl.when(jnp.logical_not(there))
        def _():
            for n in range(STEPS):
                recvs[n, side] = jnp.zeros((8, 128), F32)

    lane = iota2((8, 128), 1)
    greeted = has_lower.astype(jnp.int32) + has_upper.astype(jnp.int32) + jnp.where(is_site, 3, 1)

    def edge(n, side):
        peer = sub - 1 if side == 0 else sub + 1
        return pltpu.make_async_remote_copy(
            src_ref=sends.at[n, side],
            dst_ref=recvs.at[n, 1 - side],
            send_sem=send_sem.at[n, side],
            recv_sem=recv_sem.at[n, 1 - side],
            device_id=(grp, peer),
            device_id_type=MESH,
        )

    def layer_copy(n, m):
        return pltpu.make_async_remote_copy(
            src_ref=layer_out.at[n],
            dst_ref=layer_in.at[n, m],
            send_sem=layer_send_sem.at[n],
            recv_sem=layer_recv_sem.at[n, m],
            device_id=(target, sub),
            device_id_type=MESH,
        )

    sides = ((has_lower, 0), (has_upper, 1))

    def exchange(kind, n, pos, cx, fills):
        found = read_ends(kind, kind.NRP // 8, pos, cx)
        for there, side in sides:
            for c in range(3):
                force = found[c][2 * side : 2 * side + 1] - found[c][2 * side + 1 : 2 * side + 2]
                sends[n, side, c : c + 1, :] = jnp.where(lane[0:1] < fills[side], force, 0.0)

            @pl.when(there)
            def _():
                edge(n, side).start()

    def arrive(n):
        for there, side in sides:

            @pl.when(there)
            def _():
                edge(n, 1 - side).wait_recv()

    def finish(n, carry):
        for there, side in sides:

            @pl.when(there)
            def _():
                edge(n, side).wait_send()

        return carry

    setup_scan(scan)
    sends[...] = jnp.zeros(sends.shape, F32)

    @pl.when(jnp.logical_not(is_site))
    def _():
        kind = reg
        setup_state(kind, reg_disp, reg_vel, u_r, prev_r)
        f_r[...] = jnp.zeros(f_r.shape, F32)
        setup_tables(kind, reg_table, False, tpad_r, d1_r, d2_r)
        coef_r[...] = jnp.zeros(coef_r.shape, F32)
        coef_r[:, :, 0 : kind.Q, :] = reg_coefs[0, 0]
        setup_plan(kind, reg_nodes, reg_send, node_r, key_r, plan_r, pos_r)
        setup_hot(kind, [lambda i=i: reg_recv[0, 0, i : i + 1, :] for i in range(2)], hot_r)
        pl.semaphore_wait(barrier, greeted)
        fills = (slot_fill[0, 0, 0], slot_fill[0, 0, 1])

        def step(n, carry):
            stiff_force(
                kind, u_r, lambda a, b, k: coef_r[a, b, :, k * 128 : (k + 1) * 128],
                node_r, plan_r, d1_r, d2_r, scan, fe_r, cx_r,
            )
            exchange(kind, n, pos_r, cx_r, fills)
            node_forces(kind, pos_r, cx_r, f_r)
            minv = reg_minv[0]
            now = u_r[...]
            ahead = 2.0 * now - prev_r[...] + minv * f_r[...]
            prev_r[...] = now
            arrive(n)
            u_r[...] = ahead + minv * drop(kind, [recvs[n, 0], recvs[n, 1]], hot_r)
            found = pick(kind, u_r, layer_src[0])
            layer_out[n] = jnp.where(lane < layer_fill[0, 0], found, 0.0)
            layer_copy(n, source).start()
            return carry

        lax.fori_loop(0, STEPS, step, 0)
        for c in range(3):
            reg_out[0, c] = u_r[c : c + 1, :]
        site_out[...] = jnp.zeros(site_out.shape, F32)

        def drain(n, carry):
            layer_copy(n, source).wait_send()
            return finish(n, carry)

        lax.fori_loop(0, STEPS, drain, 0)

    @pl.when(is_site)
    def _():
        kind = site
        setup_state(kind, site_disp, site_vel, u_s, prev_s)
        f_s[...] = jnp.zeros(f_s.shape, F32)
        setup_tables(kind, site_table, True, tpad_s, d1_s, d2_s)
        setup_plan(kind, site_nodes, site_send, node_s, key_s, plan_s, pos_s)
        setup_hot(kind, [lambda i=i: site_recv[0, 0, i : i + 1, :] for i in range(2)], hot_s)
        setup_hot(kind, [lambda i=i: layer_dst[0, i] for i in range(3)], hot_l)
        pl.semaphore_wait(barrier, greeted)
        fills = (slot_fill[0, 0, 2], slot_fill[0, 0, 3])

        def step(n, carry):
            stiff_force(
                kind, u_s, lambda a, b, k: site_coefs[0, 0, a, b],
                node_s, plan_s, d1_s, d2_s, scan, fe_s, cx_s,
            )
            exchange(kind, n, pos_s, cx_s, fills)
            node_forces(kind, pos_s, cx_s, f_s)
            minv = site_minv[0]
            now = u_s[...]
            ahead = 2.0 * now - prev_s[...] + minv * f_s[...]
            prev_s[...] = now
            parts = []
            for m in range(3):
                layer_copy(n, m).wait_recv()
                parts.append(layer_in[n, m] * layer_stiff[0, m])
            ahead = ahead + minv * drop(kind, parts, hot_l)
            arrive(n)
            u_s[...] = ahead + minv * drop(kind, [recvs[n, 0], recvs[n, 1]], hot_s)
            return carry

        lax.fori_loop(0, STEPS, step, 0)
        for c in range(3):
            site_out[0, c] = u_s[c : c + 1, :]
        reg_out[...] = jnp.zeros(reg_out.shape, F32)
        lax.fori_loop(0, STEPS, finish, 0)


def kind_scratch(kind):
    depth = pad_to(3 * kind.KQ, 128)
    i32 = jnp.int32
    return [
        pltpu.VMEM((8, kind.N), F32),
        pltpu.VMEM((8, kind.N), F32),
        pltpu.VMEM((8, kind.N), F32),
        pltpu.VMEM((128, 128), F32),
        pltpu.VMEM((128, 128), F32),
        pltpu.VMEM((128, depth), F32),
        pltpu.VMEM((kind.SR, 128), i32),
        pltpu.VMEM((kind.SR, 128), i32),
        pltpu.VMEM((2, kind.SR, 128), i32),
        pltpu.VMEM((kind.NRP // 8 + 1, kind.W8, 2, 8, 128), i32),
        pltpu.VMEM((kind.N, 256), BF16),
        pltpu.VMEM((3, kind.SR, 128), F32),
        pltpu.VMEM((3, kind.SR, 128), F32),
    ]


def shards(*args):
    group_count = lax.axis_size("grp")
    site_groups = group_count // 4
    reg_groups = 3 * site_groups
    reg = Kind(args[4].shape[2], args[6].shape[4], args[4].shape[3], args[0].shape[3])
    site = Kind(args[5].shape[2], args[7].shape[4], args[5].shape[3], args[2].shape[3])
    args = list(args)
    for i in (0, 1, 2, 3, 4, 5, 19, 20):
        args[i] = jnp.transpose(args[i], (0, 2, 1, 3))
    args[9] = args[9].T
    vmem = pl.BlockSpec(memory_space=pltpu.VMEM)
    smem = pl.BlockSpec(memory_space=pltpu.SMEM)
    in_specs = [vmem] * len(args)
    in_specs[16] = smem
    in_specs[18] = smem
    kernel = functools.partial(body, reg, site, reg_groups, site_groups, lax.axis_size("sub"))
    outs = pl.pallas_call(
        kernel,
        name="drm_window",
        out_shape=(
            jax.ShapeDtypeStruct((1, 3, 1, reg.N), F32),
            jax.ShapeDtypeStruct((1, 3, 1, site.N), F32),
        ),
        in_specs=in_specs,
        out_specs=(vmem, vmem),
        scratch_shapes=kind_scratch(reg)
        + [pltpu.VMEM((3, 3, reg.QP, reg.E), F32)]
        + kind_scratch(site)
        + [
            pltpu.VMEM((site.N, 384), BF16),
            pltpu.VMEM((256, 128), BF16),
            pltpu.VMEM((STEPS, 2, 8, 128), F32),
            pltpu.VMEM((STEPS, 2, 8, 128), F32),
            pltpu.VMEM((STEPS, 8, 128), F32),
            pltpu.VMEM((STEPS, 3, 8, 128), F32),
            pltpu.SemaphoreType.DMA((STEPS, 2)),
            pltpu.SemaphoreType.DMA((STEPS, 2)),
            pltpu.SemaphoreType.DMA((STEPS,)),
            pltpu.SemaphoreType.DMA((STEPS, 3)),
        ],
        compiler_params=pltpu.CompilerParams(collective_id=0, has_side_effects=True),
    )(*args)
    return tuple(jnp.transpose(out, (0, 2, 1, 3)) for out in outs)


def solution(mesh):
    whole = P("grp", "sub")
    specs = [whole] * 21
    specs[8] = P()
    specs[9] = P()
    return jax.shard_map(
        shards,
        mesh=mesh,
        in_specs=tuple(specs),
        out_specs=(whole, whole),
        check_vma=False,
    )
```

```python
import functools

import jax
import jax.numpy as jnp
from jax import lax
from jax.experimental import pallas as pl
from jax.experimental.pallas import tpu as pltpu
from jax.sharding import PartitionSpec as P

STEPS = 8
MESH = pl.DeviceIdType.MESH
SHIFT = 13
BIG = 2047 << SHIFT
F32 = jnp.float32
BF16 = jnp.bfloat16


def pad_to(value, unit):
    return -(-value // unit) * unit


class Kind:
    def __init__(self, points, quads, elems, nodes):
        self.P, self.Q, self.E, self.N = points, quads, elems, nodes
        self.LC = elems // 128
        self.NR = nodes // 128
        self.NRP = pad_to(self.NR, 8)
        self.PP = pad_to(points, 8)
        self.QP = pad_to(quads, 8)
        self.KQ = 3 * self.QP
        self.SR = self.LC * self.PP
        self.W8 = self.SR // 8


def lane_take(x, idx):
    dims = lax.GatherDimensionNumbers(
        offset_dims=(),
        collapsed_slice_dims=(1,),
        start_index_map=(1,),
        operand_batching_dims=(0,),
        start_indices_batching_dims=(0,),
    )
    return lax.gather(
        x, idx[..., None], dims, (1, 1), mode=lax.GatherScatterMode.PROMISE_IN_BOUNDS
    )


def iota2(shape, dim):
    return lax.broadcasted_iota(jnp.int32, shape, dim)


def spread(row):
    return jnp.broadcast_to(row, (8, 128))


def split(x):
    hi = x.astype(BF16).astype(F32)
    return hi, x - hi


def mm(a, b):
    return jnp.dot(a.astype(BF16), b.astype(BF16), preferred_element_type=F32)


def sort_regs(regs):
    count = len(regs)
    depth = count * 8
    row_bits = depth.bit_length() - 1
    sub = iota2((8, 128), 0)
    lane = iota2((8, 128), 1)

    def bit_mask(bit, v):
        if bit < 3:
            return (sub >> bit) & 1
        if bit < row_bits:
            return (v >> (bit - 3)) & 1
        if bit >= row_bits + 7:
            return 0
        return (lane >> (bit - row_bits)) & 1

    total_bits = row_bits + 7
    for m in range(1, total_bits + 1):
        for jb in range(m - 1, -1, -1):
            new = list(regs)
            if 3 <= jb < row_bits:
                step = 1 << (jb - 3)
                for v in range(count):
                    if v & step:
                        continue
                    a, b = regs[v], regs[v + step]
                    low, high = jnp.minimum(a, b), jnp.maximum(a, b)
                    down = bit_mask(m, v)
                    if isinstance(down, int):
                        new[v], new[v + step] = (high, low) if down else (low, high)
                    else:
                        new[v] = jnp.where(down == 1, high, low)
                        new[v + step] = jnp.where(down == 1, low, high)
            else:
                for v in range(count):
                    x = regs[v]
                    if jb < 3:
                        dist = 1 << jb
                        if dist == 4:
                            other = pltpu.roll(x, 4, 0)
                        else:
                            other = jnp.where(
                                bit_mask(jb, v) == 1, pltpu.roll(x, dist, 0), pltpu.roll(x, 8 - dist, 0)
                            )
                    else:
                        dist = 1 << (jb - row_bits)
                        other = lane_take(x, lane ^ dist)
                    take_max = bit_mask(jb, v) ^ bit_mask(m, v)
                    new[v] = jnp.where(take_max == 1, jnp.maximum(x, other), jnp.minimum(x, other))
            regs = new
    return regs


def gather_three(idx_row, idx_lane, load_row, rows):
    out = [jnp.zeros((8, 128), F32) for _ in range(3)]
    for r in rows:
        here = idx_row == r
        for c in range(3):
            out[c] = jnp.where(here, lane_take(spread(load_row(c, r)), idx_lane), out[c])
    return out


def setup_state(kind, disp, vel, u, prev):
    for ref in (u, prev):
        ref[...] = jnp.zeros(ref.shape, F32)
    for c in range(3):
        u[c : c + 1, :] = disp[0, c]
        prev[c : c + 1, :] = disp[0, c] - vel[0, c]


def setup_tables(kind, table, flipped, tpad, d1, d2):
    tpad[...] = jnp.zeros(tpad.shape, F32)
    if flipped:
        tpad[0 : kind.P, 0 : kind.KQ] = table[...]
        across = tpad[...]
        whole = across.T
    else:
        for b in range(3):
            tpad[b * kind.QP : b * kind.QP + kind.Q, 0 : kind.P] = table[b * kind.Q : (b + 1) * kind.Q, :]
        whole = tpad[...]
        across = whole.T
    hi, lo = split(across[0 : kind.PP])
    stack = [hi, hi, lo]
    left = 128 - 3 * kind.PP
    if left:
        stack.append(jnp.zeros((left, 128), F32))
    d1[...] = jnp.concatenate(stack, axis=0).T
    hi, lo = split(-whole[0 : kind.KQ])
    depth = d2.shape[1]
    stack = [hi, hi, lo]
    left = depth - 3 * kind.KQ
    if left:
        stack.append(jnp.zeros((left, 128), F32))
    stack = jnp.concatenate(stack, axis=0)
    for k in range(depth // 128):
        d2[:, k * 128 : (k + 1) * 128] = stack[k * 128 : (k + 1) * 128].T


def setup_plan(kind, nodes, send_map, node_s, key_s, plan_s, pos_s):
    sub = iota2((8, 128), 0)
    lane = iota2((8, 128), 1)
    node_s[...] = jnp.zeros(node_s.shape, jnp.int32)
    for k in range(kind.LC):
        for p in range(kind.P):
            at = k * kind.PP + p
            node_s[at : at + 1, :] = nodes[0, p, :, k * 128 : (k + 1) * 128]
    for w in range(kind.W8):
        inside = ((sub + w * 8) % kind.PP) < kind.P
        found = jnp.where(inside, node_s[w * 8 : w * 8 + 8, :], BIG >> SHIFT)
        keys = sort_regs([(found << SHIFT) | (sub << 7) | lane])[0]
        key_s[w * 8 : w * 8 + 8, :] = keys
        slot = keys & ((1 << SHIFT) - 1)
        plan_s[0, w * 8 : w * 8 + 8, :] = jnp.where(keys < BIG, slot >> 7, 1000)
        plan_s[1, w * 8 : w * 8 + 8, :] = slot & 127
    sent = jnp.zeros((8, 128), jnp.int32)
    for side in range(2):
        wanted = spread(send_map[0, 0, side : side + 1, :])
        sent = jnp.where(sub == 2 * side, wanted + 1, sent)
        sent = jnp.where(sub == 2 * side + 1, wanted, sent)
    find_places(kind, [(kind.NRP // 8, sent << SHIFT)], key_s, pos_s)


def setup_ends(kind, key_s, pos_s):
    sub = iota2((8, 128), 0)
    lane = iota2((8, 128), 1)
    targets = [(v, ((sub + v * 8) * 128 + lane + 1) << SHIFT) for v in range(kind.NRP // 8)]
    find_places(kind, targets, key_s, pos_s)


def find_places(kind, targets, key_s, pos_s):
    for w in range(kind.W8):
        last = spread(key_s[w * 8 + 7 : w * 8 + 8, :])
        for v, target in targets:
            column = jnp.zeros((8, 128), jnp.int32)
            for step in (64, 32, 16, 8, 4, 2, 1):
                column = jnp.where(lane_take(last, column + (step - 1)) < target, column + step, column)
            place = column * 8 - 1
            for r in range(8):
                row = spread(key_s[w * 8 + r : w * 8 + r + 1, :])
                place = place + jnp.where(lane_take(row, column) < target, 1, 0)
            pos_s[v, w, 0] = jnp.where(place < 0, 1000, place & 7)
            pos_s[v, w, 1] = jnp.where(place < 0, 0, place >> 3)


def setup_scan(scan):
    row = iota2(scan.shape, 0) % 128
    col = iota2(scan.shape, 1)
    scan[...] = jnp.where(row < col, 1.0, 0.0).astype(BF16)


def setup_hot(kind, maps, hot):
    rows = iota2((kind.N, 128), 0)
    for k, load in enumerate(maps):
        hot[:, k * 128 : (k + 1) * 128] = jnp.where(rows == load(), 1.0, 0.0).astype(BF16)


def stiff_force(kind, u, coef, node_s, plan_s, d1, d2, scan, fe_s, cx_s):
    blocks = {}
    for k in range(kind.LC):
        for v in range(kind.PP // 8):
            at = k * kind.PP + v * 8
            index = node_s[at : at + 8, :]
            found = gather_three(
                index >> 7,
                index & 127,
                lambda c, r: u[c : c + 1, r * 128 : (r + 1) * 128],
                range(kind.NR),
            )
            for c in range(3):
                blocks[c, k, v] = found[c]
    chunks = [(c, k) for c in range(3) for k in range(kind.LC)]
    cols = []
    for c, k in chunks:
        ve = jnp.concatenate([blocks[c, k, v] for v in range(kind.PP // 8)], axis=0)
        hi, lo = split(ve)
        parts = [hi, lo, hi]
        left = 128 - 3 * kind.PP
        if left:
            parts.append(jnp.zeros((left, 128), F32))
        cols.append(jnp.concatenate(parts, axis=0).astype(BF16))
    gathered = jnp.concatenate(cols, axis=1)
    grad = jnp.dot(d1[0 : kind.KQ, :].astype(BF16), gathered, preferred_element_type=F32)
    cols = []
    depth = d2.shape[1]
    for i, (c, k) in enumerate(chunks):
        piece = grad[:, i * 128 : (i + 1) * 128]
        terms = []
        for a in range(3):
            total = coef(a, 0, k) * piece[0 : kind.QP]
            for b in (1, 2):
                total = total + coef(a, b, k) * piece[b * kind.QP : (b + 1) * kind.QP]
            terms.append(total)
        flux = jnp.concatenate(terms, axis=0)
        hi, lo = split(flux)
        parts = [hi, lo, hi]
        left = depth - 3 * kind.KQ
        if left:
            parts.append(jnp.zeros((left, 128), F32))
        cols.append(jnp.concatenate(parts, axis=0).astype(BF16))
    flux = jnp.concatenate(cols, axis=1)
    fe = jnp.dot(d2[0 : kind.PP, :].astype(BF16), flux, preferred_element_type=F32)
    for i, (c, k) in enumerate(chunks):
        fe_s[c, k * kind.PP : (k + 1) * kind.PP, :] = fe[:, i * 128 : (i + 1) * 128]
    sub = iota2((8, 128), 0)
    terms = {}
    both = []
    for w in range(kind.W8):
        found = gather_three(
            plan_s[0, w * 8 : w * 8 + 8, :],
            plan_s[1, w * 8 : w * 8 + 8, :],
            lambda c, r: fe_s[c, w * 8 + r : w * 8 + r + 1, :],
            [r for r in range(8) if (w * 8 + r) % kind.PP < kind.P],
        )
        for c in range(3):
            hi, lo = split(found[c])
            both.append(jnp.concatenate([hi, lo], axis=1))
            upto = found[c]
            for dist in (1, 2, 4):
                upto = upto + jnp.where(sub >= dist, pltpu.roll(upto, dist, 0), 0.0)
            terms[w, c] = upto
    sums = jnp.dot(
        jnp.concatenate(both, axis=0).astype(BF16), scan[...], preferred_element_type=F32
    )
    for w in range(kind.W8):
        for c in range(3):
            at = (w * 3 + c) * 8
            ahead = sums[at : at + 8]
            for dist in (4, 2, 1):
                ahead = ahead + pltpu.roll(ahead, dist, 0)
            cx_s[c, w * 8 : w * 8 + 8, :] = terms[w, c] + ahead


def read_ends(kind, v, pos_s, cx_s):
    total = None
    for w in range(kind.W8):
        found = gather_three(
            pos_s[v, w, 0],
            pos_s[v, w, 1],
            lambda c, r: cx_s[c, w * 8 + r : w * 8 + r + 1, :],
            range(8),
        )
        total = found if total is None else [a + b for a, b in zip(total, found)]
    return total


def node_forces(kind, pos_s, cx_s, f_s):
    corner_row = iota2((kind.NRP, 128), 0)
    corner_lane = iota2((kind.NRP, 128), 1)
    found = [read_ends(kind, v, pos_s, cx_s) for v in range(kind.NRP // 8)]
    for c in range(3):
        ends = jnp.concatenate([block[c] for block in found], axis=0)
        before = pltpu.roll(ends, 1, 1)
        above = pltpu.roll(before, 1, 0)
        before = jnp.where(corner_lane == 0, above, before)
        before = jnp.where((corner_lane == 0) & (corner_row == 0), 0.0, before)
        forces = ends - before
        for r in range(kind.NR):
            f_s[c : c + 1, r * 128 : (r + 1) * 128] = forces[r : r + 1, :]


def pick(kind, source, index):
    idx_row, idx_lane = spread(index >> 7), spread(index & 127)
    out = jnp.zeros((8, 128), F32)
    for r in range(kind.NR):
        out = jnp.where(
            idx_row == r, lane_take(source[:, r * 128 : (r + 1) * 128], idx_lane), out
        )
    return out


def drop(kind, parts, hot):
    r = jnp.concatenate(parts, axis=1)
    hi, lo = split(r)
    both = jnp.concatenate([hi, lo], axis=0).astype(BF16)
    out = lax.dot_general(
        both, hot[...], (((1,), (1,)), ((), ())), preferred_element_type=F32
    )
    return out[0:8] + out[8:16]


def body(
    reg, site, reg_groups, site_groups, sub_count,
    reg_disp, reg_vel, site_disp, site_vel, reg_nodes, site_nodes, reg_coefs, site_coefs,
    reg_table, site_table, reg_minv, site_minv, reg_send, reg_recv, site_send, site_recv,
    slot_fill, layer_src, layer_fill, layer_dst, layer_stiff,
    reg_out, site_out,
    u_r, prev_r, f_r, tpad_r, d1_r, d2_r, node_r, key_r, plan_r, pos_r, hot_r, fe_r, cx_r, coef_r,
    u_s, prev_s, f_s, tpad_s, d1_s, d2_s, node_s, key_s, plan_s, pos_s, hot_s, fe_s, cx_s,
    hot_l, scan, fills, sends, recvs, layer_out, layer_in,
    send_sem, recv_sem, layer_send_sem, layer_recv_sem,
):
    grp = lax.axis_index("grp")
    sub = lax.axis_index("sub")
    is_site = grp >= reg_groups
    has_lower = sub > 0
    has_upper = sub < sub_count - 1
    source = grp // site_groups
    target = reg_groups + grp % site_groups
    barrier = pltpu.get_barrier_semaphore()

    def hello(g, s):
        pl.semaphore_signal(barrier, inc=1, device_id=(g, s), device_id_type=MESH)

    @pl.when(has_lower)
    def _():
        hello(grp, sub - 1)

    @pl.when(has_upper)
    def _():
        hello(grp, sub + 1)

    @pl.when(is_site)
    def _():
        for m in range(3):
            hello(m * site_groups + grp - reg_groups, sub)

    @pl.when(jnp.logical_not(is_site))
    def _():
        hello(target, sub)

    for there, side in ((has_lower, 0), (has_upper, 1)):

        @pl.when(jnp.logical_not(there))
        def _():
            for n in range(STEPS):
                recvs[n, side] = jnp.zeros((8, 128), F32)

    lane = iota2((8, 128), 1)
    live = iota2((8, 128), 0) < 3
    greeted = has_lower.astype(jnp.int32) + has_upper.astype(jnp.int32) + jnp.where(is_site, 3, 1)

    def edge(n, side):
        peer = sub - 1 if side == 0 else sub + 1
        return pltpu.make_async_remote_copy(
            src_ref=sends.at[n, side, 0:3],
            dst_ref=recvs.at[n, 1 - side, 0:3],
            send_sem=send_sem.at[n, side],
            recv_sem=recv_sem.at[n, 1 - side],
            device_id=(grp, peer),
            device_id_type=MESH,
        )

    def layer_copy(n, m):
        return pltpu.make_async_remote_copy(
            src_ref=layer_out.at[n, 0:3],
            dst_ref=layer_in.at[n, m, 0:3],
            send_sem=layer_send_sem.at[n],
            recv_sem=layer_recv_sem.at[n, m],
            device_id=(target, sub),
            device_id_type=MESH,
        )

    sides = ((has_lower, 0), (has_upper, 1))

    def exchange(kind, n, pos, cx):
        found = read_ends(kind, kind.NRP // 8, pos, cx)
        for there, side in sides:
            for c in range(3):
                force = found[c][2 * side : 2 * side + 1] - found[c][2 * side + 1 : 2 * side + 2]
                sends[n, side, c : c + 1, :] = jnp.where(lane[0:1] < fills[side : side + 1, :], force, 0.0)

            @pl.when(there)
            def _():
                edge(n, side).start()

    def arrive(n):
        for there, side in sides:

            @pl.when(there)
            def _():
                edge(n, 1 - side).wait_recv()

    def arrived(n, side):
        return jnp.where(live, recvs[n, side], 0.0)

    def finish(n, carry):
        for there, side in sides:

            @pl.when(there)
            def _():
                edge(n, side).wait_send()

        return carry

    setup_scan(scan)
    sends[...] = jnp.zeros(sends.shape, F32)

    @pl.when(jnp.logical_not(is_site))
    def _():
        kind = reg
        setup_state(kind, reg_disp, reg_vel, u_r, prev_r)
        f_r[...] = jnp.zeros(f_r.shape, F32)
        setup_tables(kind, reg_table, False, tpad_r, d1_r, d2_r)
        coef_r[...] = jnp.zeros(coef_r.shape, F32)
        coef_r[:, :, 0 : kind.Q, :] = reg_coefs[0, 0]
        setup_plan(kind, reg_nodes, reg_send, node_r, key_r, plan_r, pos_r)
        pl.semaphore_wait(barrier, greeted)
        for i in range(2):
            fills[i : i + 1, :] = jnp.broadcast_to(slot_fill[0, :, i : i + 1], (1, 128))
        fills[2:3, :] = jnp.broadcast_to(layer_fill[...], (1, 128))

        def step(n, carry):
            stiff_force(
                kind, u_r, lambda a, b, k: coef_r[a, b, :, k * 128 : (k + 1) * 128],
                node_r, plan_r, d1_r, d2_r, scan, fe_r, cx_r,
            )
            exchange(kind, n, pos_r, cx_r)

            @pl.when(n == 0)
            def _():
                setup_ends(kind, key_r, pos_r)
                setup_hot(kind, [lambda i=i: reg_recv[0, 0, i : i + 1, :] for i in range(2)], hot_r)

            node_forces(kind, pos_r, cx_r, f_r)
            minv = reg_minv[0]
            now = u_r[...]
            ahead = 2.0 * now - prev_r[...] + minv * f_r[...]
            prev_r[...] = now
            arrive(n)
            u_r[...] = ahead + minv * drop(kind, [arrived(n, i) for i in range(2)], hot_r)
            found = pick(kind, u_r, layer_src[0])
            layer_out[n] = jnp.where(lane < fills[2:3, :], found, 0.0)
            layer_copy(n, source).start()
            return carry

        lax.fori_loop(0, STEPS, step, 0)
        for c in range(3):
            reg_out[0, c] = u_r[c : c + 1, :]
        site_out[...] = jnp.zeros(site_out.shape, F32)

        def drain(n, carry):
            layer_copy(n, source).wait_send()
            return finish(n, carry)

        lax.fori_loop(0, STEPS, drain, 0)

    @pl.when(is_site)
    def _():
        kind = site
        setup_state(kind, site_disp, site_vel, u_s, prev_s)
        f_s[...] = jnp.zeros(f_s.shape, F32)
        setup_tables(kind, site_table, True, tpad_s, d1_s, d2_s)
        setup_plan(kind, site_nodes, site_send, node_s, key_s, plan_s, pos_s)
        pl.semaphore_wait(barrier, greeted)
        for i in range(2):
            fills[i : i + 1, :] = jnp.broadcast_to(slot_fill[0, :, i + 2 : i + 3], (1, 128))

        def step(n, carry):
            stiff_force(
                kind, u_s, lambda a, b, k: site_coefs[0, 0, a, b],
                node_s, plan_s, d1_s, d2_s, scan, fe_s, cx_s,
            )
            exchange(kind, n, pos_s, cx_s)

            @pl.when(n == 0)
            def _():
                setup_ends(kind, key_s, pos_s)
                setup_hot(kind, [lambda i=i: site_recv[0, 0, i : i + 1, :] for i in range(2)], hot_s)
                setup_hot(kind, [lambda i=i: layer_dst[0, i] for i in range(3)], hot_l)

            node_forces(kind, pos_s, cx_s, f_s)
            minv = site_minv[0]
            now = u_s[...]
            ahead = 2.0 * now - prev_s[...] + minv * f_s[...]
            prev_s[...] = now
            parts = []
            for m in range(3):
                layer_copy(n, m).wait_recv()
                parts.append(jnp.where(live, layer_in[n, m], 0.0) * layer_stiff[0, m])
            ahead = ahead + minv * drop(kind, parts, hot_l)
            arrive(n)
            u_s[...] = ahead + minv * drop(kind, [arrived(n, i) for i in range(2)], hot_s)
            return carry

        lax.fori_loop(0, STEPS, step, 0)
        for c in range(3):
            site_out[0, c] = u_s[c : c + 1, :]
        reg_out[...] = jnp.zeros(reg_out.shape, F32)
        lax.fori_loop(0, STEPS, finish, 0)


def kind_scratch(kind):
    depth = pad_to(3 * kind.KQ, 128)
    i32 = jnp.int32
    return [
        pltpu.VMEM((8, kind.N), F32),
        pltpu.VMEM((8, kind.N), F32),
        pltpu.VMEM((8, kind.N), F32),
        pltpu.VMEM((128, 128), F32),
        pltpu.VMEM((128, 128), F32),
        pltpu.VMEM((128, depth), F32),
        pltpu.VMEM((kind.SR, 128), i32),
        pltpu.VMEM((kind.SR, 128), i32),
        pltpu.VMEM((2, kind.SR, 128), i32),
        pltpu.VMEM((kind.NRP // 8 + 1, kind.W8, 2, 8, 128), i32),
        pltpu.VMEM((kind.N, 256), BF16),
        pltpu.VMEM((3, kind.SR, 128), F32),
        pltpu.VMEM((3, kind.SR, 128), F32),
    ]


def shards(*args):
    group_count = lax.axis_size("grp")
    site_groups = group_count // 4
    reg_groups = 3 * site_groups
    reg = Kind(args[4].shape[2], args[6].shape[4], args[4].shape[3], args[0].shape[3])
    site = Kind(args[5].shape[2], args[7].shape[4], args[5].shape[3], args[2].shape[3])
    args = list(args)
    for i in (0, 1, 2, 3, 4, 5, 19, 20):
        args[i] = jnp.transpose(args[i], (0, 2, 1, 3))
    args[9] = args[9].T
    vmem = pl.BlockSpec(memory_space=pltpu.VMEM)
    in_specs = [vmem] * len(args)
    kernel = functools.partial(body, reg, site, reg_groups, site_groups, lax.axis_size("sub"))
    outs = pl.pallas_call(
        kernel,
        name="drm_window",
        out_shape=(
            pltpu.VMEM((1, 3, 1, reg.N), F32),
            pltpu.VMEM((1, 3, 1, site.N), F32),
        ),
        in_specs=in_specs,
        out_specs=(vmem, vmem),
        scratch_shapes=kind_scratch(reg)
        + [pltpu.VMEM((3, 3, reg.QP, reg.E), F32)]
        + kind_scratch(site)
        + [
            pltpu.VMEM((site.N, 384), BF16),
            pltpu.VMEM((256, 128), BF16),
            pltpu.VMEM((8, 128), jnp.int32),
            pltpu.VMEM((STEPS, 2, 8, 128), F32),
            pltpu.VMEM((STEPS, 2, 8, 128), F32),
            pltpu.VMEM((STEPS, 8, 128), F32),
            pltpu.VMEM((STEPS, 3, 8, 128), F32),
            pltpu.SemaphoreType.DMA((STEPS, 2)),
            pltpu.SemaphoreType.DMA((STEPS, 2)),
            pltpu.SemaphoreType.DMA((STEPS,)),
            pltpu.SemaphoreType.DMA((STEPS, 3)),
        ],
        compiler_params=pltpu.CompilerParams(collective_id=0, has_side_effects=True),
    )(*args)
    return tuple(jnp.transpose(out, (0, 2, 1, 3)) for out in outs)


def solution(mesh):
    whole = P("grp", "sub")
    specs = [whole] * 21
    specs[8] = P()
    specs[9] = P()
    return jax.shard_map(
        shards,
        mesh=mesh,
        in_specs=tuple(specs),
        out_specs=(whole, whole),
        check_vma=False,
    )
```

```python
import functools

import jax
import jax.numpy as jnp
from jax import lax
from jax.experimental import pallas as pl
from jax.experimental.pallas import tpu as pltpu
from jax.sharding import PartitionSpec as P

STEPS = 8
MESH = pl.DeviceIdType.MESH
SHIFT = 13
BIG = 2047 << SHIFT
F32 = jnp.float32
BF16 = jnp.bfloat16


def pad_to(value, unit):
    return -(-value // unit) * unit


class Kind:
    def __init__(self, points, quads, elems, nodes):
        self.P, self.Q, self.E, self.N = points, quads, elems, nodes
        self.LC = elems // 128
        self.NR = nodes // 128
        self.NRP = pad_to(self.NR, 8)
        self.PP = pad_to(points, 8)
        self.QP = pad_to(quads, 8)
        self.KQ = 3 * self.QP
        self.SR = self.LC * self.PP
        self.W8 = self.SR // 8


def lane_take(x, idx):
    dims = lax.GatherDimensionNumbers(
        offset_dims=(),
        collapsed_slice_dims=(1,),
        start_index_map=(1,),
        operand_batching_dims=(0,),
        start_indices_batching_dims=(0,),
    )
    return lax.gather(
        x, idx[..., None], dims, (1, 1), mode=lax.GatherScatterMode.PROMISE_IN_BOUNDS
    )


def iota2(shape, dim):
    return lax.broadcasted_iota(jnp.int32, shape, dim)


def spread(row):
    return jnp.broadcast_to(row, (8, 128))


def split(x):
    hi = x.astype(BF16).astype(F32)
    return hi, x - hi


def mm(a, b):
    return jnp.dot(a.astype(BF16), b.astype(BF16), preferred_element_type=F32)


def sort_regs(regs):
    count = len(regs)
    depth = count * 8
    row_bits = depth.bit_length() - 1
    sub = iota2((8, 128), 0)
    lane = iota2((8, 128), 1)

    def bit_mask(bit, v):
        if bit < 3:
            return (sub >> bit) & 1
        if bit < row_bits:
            return (v >> (bit - 3)) & 1
        if bit >= row_bits + 7:
            return 0
        return (lane >> (bit - row_bits)) & 1

    total_bits = row_bits + 7
    for m in range(1, total_bits + 1):
        for jb in range(m - 1, -1, -1):
            new = list(regs)
            if 3 <= jb < row_bits:
                step = 1 << (jb - 3)
                for v in range(count):
                    if v & step:
                        continue
                    a, b = regs[v], regs[v + step]
                    low, high = jnp.minimum(a, b), jnp.maximum(a, b)
                    down = bit_mask(m, v)
                    if isinstance(down, int):
                        new[v], new[v + step] = (high, low) if down else (low, high)
                    else:
                        new[v] = jnp.where(down == 1, high, low)
                        new[v + step] = jnp.where(down == 1, low, high)
            else:
                for v in range(count):
                    x = regs[v]
                    if jb < 3:
                        dist = 1 << jb
                        if dist == 4:
                            other = pltpu.roll(x, 4, 0)
                        else:
                            other = jnp.where(
                                bit_mask(jb, v) == 1, pltpu.roll(x, dist, 0), pltpu.roll(x, 8 - dist, 0)
                            )
                    else:
                        dist = 1 << (jb - row_bits)
                        other = lane_take(x, lane ^ dist)
                    take_max = bit_mask(jb, v) ^ bit_mask(m, v)
                    new[v] = jnp.where(take_max == 1, jnp.maximum(x, other), jnp.minimum(x, other))
            regs = new
    return regs


def gather_three(idx_row, idx_lane, load_row, rows):
    out = [jnp.zeros((8, 128), F32) for _ in range(3)]
    for r in rows:
        here = idx_row == r
        for c in range(3):
            out[c] = jnp.where(here, lane_take(spread(load_row(c, r)), idx_lane), out[c])
    return out


def setup_state(kind, disp, vel, u, prev):
    for ref in (u, prev):
        ref[...] = jnp.zeros(ref.shape, F32)
    for c in range(3):
        u[c : c + 1, :] = disp[0, c]
        prev[c : c + 1, :] = disp[0, c] - vel[0, c]


def setup_tables(kind, table, flipped, tpad, d1, d2):
    tpad[...] = jnp.zeros(tpad.shape, F32)
    if flipped:
        tpad[0 : kind.P, 0 : kind.KQ] = table[...]
        across = tpad[...]
        whole = across.T
    else:
        for b in range(3):
            tpad[b * kind.QP : b * kind.QP + kind.Q, 0 : kind.P] = table[b * kind.Q : (b + 1) * kind.Q, :]
        whole = tpad[...]
        across = whole.T
    hi, lo = split(across[0 : kind.PP])
    stack = [hi, hi, lo]
    left = 128 - 3 * kind.PP
    if left:
        stack.append(jnp.zeros((left, 128), F32))
    d1[...] = jnp.concatenate(stack, axis=0).T
    hi, lo = split(-whole[0 : kind.KQ])
    depth = d2.shape[1]
    stack = [hi, hi, lo]
    left = depth - 3 * kind.KQ
    if left:
        stack.append(jnp.zeros((left, 128), F32))
    stack = jnp.concatenate(stack, axis=0)
    for k in range(depth // 128):
        d2[:, k * 128 : (k + 1) * 128] = stack[k * 128 : (k + 1) * 128].T


def setup_plan(kind, nodes, send_map, node_s, key_s, plan_s, pos_s):
    sub = iota2((8, 128), 0)
    lane = iota2((8, 128), 1)
    node_s[...] = jnp.zeros(node_s.shape, jnp.int32)
    for k in range(kind.LC):
        for p in range(kind.P):
            at = k * kind.PP + p
            node_s[at : at + 1, :] = nodes[0, p, :, k * 128 : (k + 1) * 128]
    for w in range(kind.W8):
        inside = ((sub + w * 8) % kind.PP) < kind.P
        found = jnp.where(inside, node_s[w * 8 : w * 8 + 8, :], BIG >> SHIFT)
        keys = sort_regs([(found << SHIFT) | (sub << 7) | lane])[0]
        key_s[w * 8 : w * 8 + 8, :] = keys
        slot = keys & ((1 << SHIFT) - 1)
        plan_s[0, w * 8 : w * 8 + 8, :] = jnp.where(keys < BIG, slot >> 7, 1000)
        plan_s[1, w * 8 : w * 8 + 8, :] = slot & 127
    sent = jnp.zeros((8, 128), jnp.int32)
    for side in range(2):
        wanted = spread(send_map[0, 0, side : side + 1, :])
        sent = jnp.where(sub == 2 * side, wanted + 1, sent)
        sent = jnp.where(sub == 2 * side + 1, wanted, sent)
    find_places(kind, [(kind.NRP // 8, sent << SHIFT)], key_s, pos_s)


def setup_ends(kind, key_s, pos_s):
    sub = iota2((8, 128), 0)
    lane = iota2((8, 128), 1)
    targets = [(v, ((sub + v * 8) * 128 + lane + 1) << SHIFT) for v in range(kind.NRP // 8)]
    find_places(kind, targets, key_s, pos_s)


def find_places(kind, targets, key_s, pos_s):
    for w in range(kind.W8):
        last = spread(key_s[w * 8 + 7 : w * 8 + 8, :])
        for v, target in targets:
            column = jnp.zeros((8, 128), jnp.int32)
            for step in (64, 32, 16, 8, 4, 2, 1):
                column = jnp.where(lane_take(last, column + (step - 1)) < target, column + step, column)
            place = column * 8 - 1
            for r in range(8):
                row = spread(key_s[w * 8 + r : w * 8 + r + 1, :])
                place = place + jnp.where(lane_take(row, column) < target, 1, 0)
            pos_s[v, w, 0] = jnp.where(place < 0, 1000, place & 7)
            pos_s[v, w, 1] = jnp.where(place < 0, 0, place >> 3)


def setup_scan(scan):
    row = iota2(scan.shape, 0) % 128
    col = iota2(scan.shape, 1)
    scan[...] = jnp.where(row < col, 1.0, 0.0).astype(BF16)


def setup_hot(kind, maps, hot):
    rows = iota2((kind.N, 128), 0)
    for k, load in enumerate(maps):
        hot[:, k * 128 : (k + 1) * 128] = jnp.where(rows == load(), 1.0, 0.0).astype(BF16)


def gather_nodes(kind, u, node_s):
    blocks = {}
    for w in range(kind.W8):
        index = node_s[w * 8 : w * 8 + 8, :]
        found = gather_three(
            index >> 7,
            index & 127,
            lambda c, r: u[c : c + 1, r * 128 : (r + 1) * 128],
            range(kind.NR),
        )
        for c in range(3):
            blocks[c, w] = found[c]
    return blocks


def setup_compact(kind, recv_map, minv, node_s, hot, equal, minv_c, slot_j):
    rows = [recv_map[0, 0, i : i + 1, :] for i in range(2)]
    wide = jnp.concatenate(rows, axis=1)
    down = jnp.concatenate(
        [jnp.broadcast_to(row.astype(F32), (128, 128)).T for row in rows], axis=0
    ).astype(jnp.int32)
    across = jnp.concatenate([down, down], axis=1) == wide
    equal[...] = jnp.where(across, 1.0, 0.0).astype(BF16)
    row = iota2((256, 256), 0)
    col = iota2((256, 256), 1)
    earlier = jnp.where(across & (row < col), 1.0, 0.0)
    count = mm(jnp.ones((16, 256), F32), earlier)
    name = jnp.where(count < 0.5, iota2((16, 256), 1) + 1, 0).astype(F32)
    table = lax.dot_general(
        name.astype(BF16), hot[...], (((1,), (1,)), ((), ())), preferred_element_type=F32
    )
    spread_minv = jnp.broadcast_to(minv, (8, kind.N))
    for i in range(2):
        minv_c[:, i * 128 : (i + 1) * 128] = pick(kind, spread_minv, rows[i])
    for w in range(kind.W8):
        index = node_s[w * 8 : w * 8 + 8, :]
        idx_row, idx_lane = index >> 7, index & 127
        found = jnp.zeros((8, 128), F32)
        for r in range(kind.NR):
            part = lane_take(spread(table[0:1, r * 128 : (r + 1) * 128]), idx_lane)
            found = jnp.where(idx_row == r, part, found)
        found = found.astype(jnp.int32) - 1
        slot_j[0, w * 8 : w * 8 + 8, :] = jnp.where(found < 0, 1000, found >> 7)
        slot_j[1, w * 8 : w * 8 + 8, :] = jnp.where(found < 0, 0, found & 127)


def stiff_force(kind, values, coef, plan_s, d1, d2, scan, fe_s, cx_s):
    blocks = {}
    for k in range(kind.LC):
        for v in range(kind.PP // 8):
            for c in range(3):
                blocks[c, k, v] = values[c, (k * kind.PP) // 8 + v]
    chunks = [(c, k) for c in range(3) for k in range(kind.LC)]
    cols = []
    for c, k in chunks:
        ve = jnp.concatenate([blocks[c, k, v] for v in range(kind.PP // 8)], axis=0)
        hi, lo = split(ve)
        parts = [hi, lo, hi]
        left = 128 - 3 * kind.PP
        if left:
            parts.append(jnp.zeros((left, 128), F32))
        cols.append(jnp.concatenate(parts, axis=0).astype(BF16))
    gathered = jnp.concatenate(cols, axis=1)
    grad = jnp.dot(d1[0 : kind.KQ, :].astype(BF16), gathered, preferred_element_type=F32)
    cols = []
    depth = d2.shape[1]
    for i, (c, k) in enumerate(chunks):
        piece = grad[:, i * 128 : (i + 1) * 128]
        terms = []
        for a in range(3):
            total = coef(a, 0, k) * piece[0 : kind.QP]
            for b in (1, 2):
                total = total + coef(a, b, k) * piece[b * kind.QP : (b + 1) * kind.QP]
            terms.append(total)
        flux = jnp.concatenate(terms, axis=0)
        hi, lo = split(flux)
        parts = [hi, lo, hi]
        left = depth - 3 * kind.KQ
        if left:
            parts.append(jnp.zeros((left, 128), F32))
        cols.append(jnp.concatenate(parts, axis=0).astype(BF16))
    flux = jnp.concatenate(cols, axis=1)
    fe = jnp.dot(d2[0 : kind.PP, :].astype(BF16), flux, preferred_element_type=F32)
    for i, (c, k) in enumerate(chunks):
        fe_s[c, k * kind.PP : (k + 1) * kind.PP, :] = fe[:, i * 128 : (i + 1) * 128]
    sub = iota2((8, 128), 0)
    terms = {}
    both = []
    for w in range(kind.W8):
        found = gather_three(
            plan_s[0, w * 8 : w * 8 + 8, :],
            plan_s[1, w * 8 : w * 8 + 8, :],
            lambda c, r: fe_s[c, w * 8 + r : w * 8 + r + 1, :],
            [r for r in range(8) if (w * 8 + r) % kind.PP < kind.P],
        )
        for c in range(3):
            hi, lo = split(found[c])
            both.append(jnp.concatenate([hi, lo], axis=1))
            upto = found[c]
            for dist in (1, 2, 4):
                upto = upto + jnp.where(sub >= dist, pltpu.roll(upto, dist, 0), 0.0)
            terms[w, c] = upto
    sums = jnp.dot(
        jnp.concatenate(both, axis=0).astype(BF16), scan[...], preferred_element_type=F32
    )
    for w in range(kind.W8):
        for c in range(3):
            at = (w * 3 + c) * 8
            ahead = sums[at : at + 8]
            for dist in (4, 2, 1):
                ahead = ahead + pltpu.roll(ahead, dist, 0)
            cx_s[c, w * 8 : w * 8 + 8, :] = terms[w, c] + ahead


def read_ends(kind, v, pos_s, cx_s):
    total = None
    for w in range(kind.W8):
        found = gather_three(
            pos_s[v, w, 0],
            pos_s[v, w, 1],
            lambda c, r: cx_s[c, w * 8 + r : w * 8 + r + 1, :],
            range(8),
        )
        total = found if total is None else [a + b for a, b in zip(total, found)]
    return total


def node_forces(kind, pos_s, cx_s, f_s):
    corner_row = iota2((kind.NRP, 128), 0)
    corner_lane = iota2((kind.NRP, 128), 1)
    found = [read_ends(kind, v, pos_s, cx_s) for v in range(kind.NRP // 8)]
    for c in range(3):
        ends = jnp.concatenate([block[c] for block in found], axis=0)
        before = pltpu.roll(ends, 1, 1)
        above = pltpu.roll(before, 1, 0)
        before = jnp.where(corner_lane == 0, above, before)
        before = jnp.where((corner_lane == 0) & (corner_row == 0), 0.0, before)
        forces = ends - before
        for r in range(kind.NR):
            f_s[c : c + 1, r * 128 : (r + 1) * 128] = forces[r : r + 1, :]


def pick(kind, source, index):
    idx_row, idx_lane = spread(index >> 7), spread(index & 127)
    out = jnp.zeros((8, 128), F32)
    for r in range(kind.NR):
        out = jnp.where(
            idx_row == r, lane_take(source[:, r * 128 : (r + 1) * 128], idx_lane), out
        )
    return out


def drop(kind, parts, hot):
    r = jnp.concatenate(parts, axis=1)
    hi, lo = split(r)
    both = jnp.concatenate([hi, lo], axis=0).astype(BF16)
    out = lax.dot_general(
        both, hot[...], (((1,), (1,)), ((), ())), preferred_element_type=F32
    )
    return out[0:8] + out[8:16]


def body(
    reg, site, reg_groups, site_groups, sub_count,
    reg_disp, reg_vel, site_disp, site_vel, reg_nodes, site_nodes, reg_coefs, site_coefs,
    reg_table, site_table, reg_minv, site_minv, reg_send, reg_recv, site_send, site_recv,
    slot_fill, layer_src, layer_fill, layer_dst, layer_stiff,
    reg_out, site_out,
    u_r, prev_r, f_r, tpad_r, d1_r, d2_r, node_r, key_r, plan_r, pos_r, hot_r, fe_r, cx_r, coef_r,
    u_s, prev_s, f_s, tpad_s, d1_s, d2_s, node_s, key_s, plan_s, pos_s, hot_s, fe_s, cx_s,
    hot_l, kept, slot_c, equal, minv_c, small, scan, fills, sends, recvs, layer_out, layer_in,
    send_sem, recv_sem, layer_send_sem, layer_recv_sem,
):
    grp = lax.axis_index("grp")
    sub = lax.axis_index("sub")
    is_site = grp >= reg_groups
    has_lower = sub > 0
    has_upper = sub < sub_count - 1
    source = grp // site_groups
    target = reg_groups + grp % site_groups
    barrier = pltpu.get_barrier_semaphore()

    def hello(g, s):
        pl.semaphore_signal(barrier, inc=1, device_id=(g, s), device_id_type=MESH)

    @pl.when(has_lower)
    def _():
        hello(grp, sub - 1)

    @pl.when(has_upper)
    def _():
        hello(grp, sub + 1)

    @pl.when(is_site)
    def _():
        for m in range(3):
            hello(m * site_groups + grp - reg_groups, sub)

    @pl.when(jnp.logical_not(is_site))
    def _():
        hello(target, sub)

    for there, side in ((has_lower, 0), (has_upper, 1)):

        @pl.when(jnp.logical_not(there))
        def _():
            for n in range(STEPS):
                recvs[n, side] = jnp.zeros((8, 128), F32)

    lane = iota2((8, 128), 1)
    live = iota2((8, 128), 0) < 3
    greeted = has_lower.astype(jnp.int32) + has_upper.astype(jnp.int32) + jnp.where(is_site, 3, 1)

    def edge(n, side):
        peer = sub - 1 if side == 0 else sub + 1
        return pltpu.make_async_remote_copy(
            src_ref=sends.at[n, side, 0:3],
            dst_ref=recvs.at[n, 1 - side, 0:3],
            send_sem=send_sem.at[n, side],
            recv_sem=recv_sem.at[n, 1 - side],
            device_id=(grp, peer),
            device_id_type=MESH,
        )

    def layer_copy(n, m):
        return pltpu.make_async_remote_copy(
            src_ref=layer_out.at[n, 0:3],
            dst_ref=layer_in.at[n, m, 0:3],
            send_sem=layer_send_sem.at[n],
            recv_sem=layer_recv_sem.at[n, m],
            device_id=(target, sub),
            device_id_type=MESH,
        )

    sides = ((has_lower, 0), (has_upper, 1))

    def exchange(kind, n, pos, cx):
        found = read_ends(kind, kind.NRP // 8, pos, cx)
        for there, side in sides:
            for c in range(3):
                force = found[c][2 * side : 2 * side + 1] - found[c][2 * side + 1 : 2 * side + 2]
                sends[n, side, c : c + 1, :] = jnp.where(lane[0:1] < fills[side : side + 1, :], force, 0.0)

            @pl.when(there)
            def _():
                edge(n, side).start()

    def arrive(n):
        for there, side in sides:

            @pl.when(there)
            def _():
                edge(n, 1 - side).wait_recv()

    def arrived(n, side):
        return jnp.where(live, recvs[n, side], 0.0)

    def finish(n, carry):
        for there, side in sides:

            @pl.when(there)
            def _():
                edge(n, side).wait_send()

        return carry

    setup_scan(scan)
    sends[...] = jnp.zeros(sends.shape, F32)

    @pl.when(jnp.logical_not(is_site))
    def _():
        kind = reg
        setup_state(kind, reg_disp, reg_vel, u_r, prev_r)
        f_r[...] = jnp.zeros(f_r.shape, F32)
        setup_tables(kind, reg_table, False, tpad_r, d1_r, d2_r)
        coef_r[...] = jnp.zeros(coef_r.shape, F32)
        coef_r[:, :, 0 : kind.Q, :] = reg_coefs[0, 0]
        setup_plan(kind, reg_nodes, reg_send, node_r, key_r, plan_r, pos_r)
        pl.semaphore_wait(barrier, greeted)
        for i in range(2):
            fills[i : i + 1, :] = jnp.broadcast_to(slot_fill[0, :, i : i + 1], (1, 128))
        fills[2:3, :] = jnp.broadcast_to(layer_fill[...], (1, 128))

        def step(n, carry):
            stiff_force(
                kind, gather_nodes(kind, u_r, node_r),
                lambda a, b, k: coef_r[a, b, :, k * 128 : (k + 1) * 128],
                plan_r, d1_r, d2_r, scan, fe_r, cx_r,
            )
            exchange(kind, n, pos_r, cx_r)

            @pl.when(n == 0)
            def _():
                setup_ends(kind, key_r, pos_r)
                setup_hot(kind, [lambda i=i: reg_recv[0, 0, i : i + 1, :] for i in range(2)], hot_r)

            node_forces(kind, pos_r, cx_r, f_r)
            minv = reg_minv[0]
            now = u_r[...]
            ahead = 2.0 * now - prev_r[...] + minv * f_r[...]
            prev_r[...] = now
            arrive(n)
            u_r[...] = ahead + minv * drop(kind, [arrived(n, i) for i in range(2)], hot_r)
            found = pick(kind, u_r, layer_src[0])
            layer_out[n] = jnp.where(lane < fills[2:3, :], found, 0.0)
            layer_copy(n, source).start()
            return carry

        lax.fori_loop(0, STEPS, step, 0)
        for c in range(3):
            reg_out[0, c] = u_r[c : c + 1, :]
        site_out[...] = jnp.zeros(site_out.shape, F32)

        def drain(n, carry):
            layer_copy(n, source).wait_send()
            return finish(n, carry)

        lax.fori_loop(0, STEPS, drain, 0)

    @pl.when(is_site)
    def _():
        kind = site
        setup_state(kind, site_disp, site_vel, u_s, prev_s)
        f_s[...] = jnp.zeros(f_s.shape, F32)
        setup_tables(kind, site_table, True, tpad_s, d1_s, d2_s)
        setup_plan(kind, site_nodes, site_send, node_s, key_s, plan_s, pos_s)
        pl.semaphore_wait(barrier, greeted)
        for i in range(2):
            fills[i : i + 1, :] = jnp.broadcast_to(slot_fill[0, :, i + 2 : i + 3], (1, 128))

        slot_c[...] = jnp.full(slot_c.shape, 1000, jnp.int32)
        slot_c[1] = jnp.zeros(slot_c.shape[1:], jnp.int32)
        small[...] = jnp.zeros(small.shape, F32)
        hot_s[...] = jnp.zeros(hot_s.shape, BF16)

        def keep_gathered(field):
            for (c, w), block in gather_nodes(kind, field, node_s).items():
                kept[c, w * 8 : w * 8 + 8, :] = block

        def complete():
            last = jnp.concatenate([small[0:8], small[8:16]], axis=0)
            out = lax.dot_general(
                last.astype(BF16), hot_s[...], (((1,), (1,)), ((), ())), preferred_element_type=F32
            )
            return u_s[...] + site_minv[0] * (out[0:8] + out[8:16])

        keep_gathered(u_s)

        def step(n, carry):
            values = {}
            for w in range(kind.W8):
                found = gather_three(
                    slot_c[0, w * 8 : w * 8 + 8, :],
                    slot_c[1, w * 8 : w * 8 + 8, :],
                    lambda c, r: small[16 + c : 17 + c, r * 128 : (r + 1) * 128],
                    range(2),
                )
                for c in range(3):
                    values[c, w] = kept[c, w * 8 : w * 8 + 8, :] + found[c]
            stiff_force(
                kind, values, lambda a, b, k: site_coefs[0, 0, a, b],
                plan_s, d1_s, d2_s, scan, fe_s, cx_s,
            )
            exchange(kind, n, pos_s, cx_s)
            now = complete()

            @pl.when(n == 0)
            def _():
                setup_ends(kind, key_s, pos_s)
                setup_hot(kind, [lambda i=i: site_recv[0, 0, i : i + 1, :] for i in range(2)], hot_s)
                setup_hot(kind, [lambda i=i: layer_dst[0, i] for i in range(3)], hot_l)
                setup_compact(kind, site_recv, site_minv[0], node_s, hot_s, equal, minv_c, slot_c)

            node_forces(kind, pos_s, cx_s, f_s)
            minv = site_minv[0]
            ahead = 2.0 * now - prev_s[...] + minv * f_s[...]
            prev_s[...] = now
            parts = []
            for m in range(3):
                layer_copy(n, m).wait_recv()
                parts.append(jnp.where(live, layer_in[n, m], 0.0) * layer_stiff[0, m])
            u_s[...] = ahead + minv * drop(kind, parts, hot_l)
            keep_gathered(u_s)
            arrive(n)
            hi, lo = split(jnp.concatenate([arrived(n, i) for i in range(2)], axis=1))
            small[0:8] = hi
            small[8:16] = lo
            sums = mm(jnp.concatenate([hi, lo], axis=0), equal[...])
            small[16:24] = (sums[0:8] + sums[8:16]) * minv_c[...]
            return carry

        lax.fori_loop(0, STEPS, step, 0)
        u_s[...] = complete()
        for c in range(3):
            site_out[0, c] = u_s[c : c + 1, :]
        reg_out[...] = jnp.zeros(reg_out.shape, F32)
        lax.fori_loop(0, STEPS, finish, 0)


def kind_scratch(kind):
    depth = pad_to(3 * kind.KQ, 128)
    i32 = jnp.int32
    return [
        pltpu.VMEM((8, kind.N), F32),
        pltpu.VMEM((8, kind.N), F32),
        pltpu.VMEM((8, kind.N), F32),
        pltpu.VMEM((128, 128), F32),
        pltpu.VMEM((128, 128), F32),
        pltpu.VMEM((128, depth), F32),
        pltpu.VMEM((kind.SR, 128), i32),
        pltpu.VMEM((kind.SR, 128), i32),
        pltpu.VMEM((2, kind.SR, 128), i32),
        pltpu.VMEM((kind.NRP // 8 + 1, kind.W8, 2, 8, 128), i32),
        pltpu.VMEM((kind.N, 256), BF16),
        pltpu.VMEM((3, kind.SR, 128), F32),
        pltpu.VMEM((3, kind.SR, 128), F32),
    ]


def shards(*args):
    group_count = lax.axis_size("grp")
    site_groups = group_count // 4
    reg_groups = 3 * site_groups
    reg = Kind(args[4].shape[2], args[6].shape[4], args[4].shape[3], args[0].shape[3])
    site = Kind(args[5].shape[2], args[7].shape[4], args[5].shape[3], args[2].shape[3])
    args = list(args)
    for i in (0, 1, 2, 3, 4, 5, 19, 20):
        args[i] = jnp.transpose(args[i], (0, 2, 1, 3))
    args[9] = args[9].T
    vmem = pl.BlockSpec(memory_space=pltpu.VMEM)
    in_specs = [vmem] * len(args)
    kernel = functools.partial(body, reg, site, reg_groups, site_groups, lax.axis_size("sub"))
    outs = pl.pallas_call(
        kernel,
        name="drm_window",
        out_shape=(
            pltpu.VMEM((1, 3, 1, reg.N), F32),
            pltpu.VMEM((1, 3, 1, site.N), F32),
        ),
        in_specs=in_specs,
        out_specs=(vmem, vmem),
        scratch_shapes=kind_scratch(reg)
        + [pltpu.VMEM((3, 3, reg.QP, reg.E), F32)]
        + kind_scratch(site)
        + [
            pltpu.VMEM((site.N, 384), BF16),
            pltpu.VMEM((3, site.SR, 128), F32),
            pltpu.VMEM((2, site.SR, 128), jnp.int32),
            pltpu.VMEM((256, 256), BF16),
            pltpu.VMEM((8, 256), F32),
            pltpu.VMEM((24, 256), F32),
            pltpu.VMEM((256, 128), BF16),
            pltpu.VMEM((8, 128), jnp.int32),
            pltpu.VMEM((STEPS, 2, 8, 128), F32),
            pltpu.VMEM((STEPS, 2, 8, 128), F32),
            pltpu.VMEM((STEPS, 8, 128), F32),
            pltpu.VMEM((STEPS, 3, 8, 128), F32),
            pltpu.SemaphoreType.DMA((STEPS, 2)),
            pltpu.SemaphoreType.DMA((STEPS, 2)),
            pltpu.SemaphoreType.DMA((STEPS,)),
            pltpu.SemaphoreType.DMA((STEPS, 3)),
        ],
        compiler_params=pltpu.CompilerParams(collective_id=0, has_side_effects=True),
    )(*args)
    return tuple(jnp.transpose(out, (0, 2, 1, 3)) for out in outs)


def solution(mesh):
    whole = P("grp", "sub")
    specs = [whole] * 21
    specs[8] = P()
    specs[9] = P()
    return jax.shard_map(
        shards,
        mesh=mesh,
        in_specs=tuple(specs),
        out_specs=(whole, whole),
        check_vma=False,
    )
```

```python
import functools

import jax
import jax.numpy as jnp
from jax import lax
from jax.experimental import pallas as pl
from jax.experimental.pallas import tpu as pltpu
from jax.sharding import PartitionSpec as P

STEPS = 8
MESH = pl.DeviceIdType.MESH
SHIFT = 13
BIG = 2047 << SHIFT
F32 = jnp.float32
BF16 = jnp.bfloat16


def pad_to(value, unit):
    return -(-value // unit) * unit


class Kind:
    def __init__(self, points, quads, elems, nodes):
        self.P, self.Q, self.E, self.N = points, quads, elems, nodes
        self.LC = elems // 128
        self.NR = nodes // 128
        self.NRP = pad_to(self.NR, 8)
        self.PP = pad_to(points, 8)
        self.QP = pad_to(quads, 8)
        self.KQ = 3 * self.QP
        self.SR = self.LC * self.PP
        self.W8 = self.SR // 8


def lane_take(x, idx):
    dims = lax.GatherDimensionNumbers(
        offset_dims=(),
        collapsed_slice_dims=(1,),
        start_index_map=(1,),
        operand_batching_dims=(0,),
        start_indices_batching_dims=(0,),
    )
    return lax.gather(
        x, idx[..., None], dims, (1, 1), mode=lax.GatherScatterMode.PROMISE_IN_BOUNDS
    )


def iota2(shape, dim):
    return lax.broadcasted_iota(jnp.int32, shape, dim)


def spread(row):
    return jnp.broadcast_to(row, (8, 128))


def split(x):
    hi = x.astype(BF16).astype(F32)
    return hi, x - hi


def mm(a, b):
    return jnp.dot(a.astype(BF16), b.astype(BF16), preferred_element_type=F32)


def sort_regs(regs):
    count = len(regs)
    depth = count * 8
    row_bits = depth.bit_length() - 1
    sub = iota2((8, 128), 0)
    lane = iota2((8, 128), 1)

    def bit_mask(bit, v):
        if bit < 3:
            return (sub >> bit) & 1
        if bit < row_bits:
            return (v >> (bit - 3)) & 1
        if bit >= row_bits + 7:
            return 0
        return (lane >> (bit - row_bits)) & 1

    total_bits = row_bits + 7
    for m in range(1, total_bits + 1):
        for jb in range(m - 1, -1, -1):
            new = list(regs)
            if 3 <= jb < row_bits:
                step = 1 << (jb - 3)
                for v in range(count):
                    if v & step:
                        continue
                    a, b = regs[v], regs[v + step]
                    low, high = jnp.minimum(a, b), jnp.maximum(a, b)
                    down = bit_mask(m, v)
                    if isinstance(down, int):
                        new[v], new[v + step] = (high, low) if down else (low, high)
                    else:
                        new[v] = jnp.where(down == 1, high, low)
                        new[v + step] = jnp.where(down == 1, low, high)
            else:
                for v in range(count):
                    x = regs[v]
                    if jb < 3:
                        dist = 1 << jb
                        if dist == 4:
                            other = pltpu.roll(x, 4, 0)
                        else:
                            other = jnp.where(
                                bit_mask(jb, v) == 1, pltpu.roll(x, dist, 0), pltpu.roll(x, 8 - dist, 0)
                            )
                    else:
                        dist = 1 << (jb - row_bits)
                        other = lane_take(x, lane ^ dist)
                    take_max = bit_mask(jb, v) ^ bit_mask(m, v)
                    new[v] = jnp.where(take_max == 1, jnp.maximum(x, other), jnp.minimum(x, other))
            regs = new
    return regs


def gather_three(idx_row, idx_lane, load_row, rows):
    out = [jnp.zeros((8, 128), F32) for _ in range(3)]
    for r in rows:
        here = idx_row == r
        for c in range(3):
            out[c] = jnp.where(here, lane_take(spread(load_row(c, r)), idx_lane), out[c])
    return out


def setup_state(kind, disp, vel, u, prev):
    for ref in (u, prev):
        ref[...] = jnp.zeros(ref.shape, F32)
    for c in range(3):
        u[c : c + 1, :] = disp[0, c]
        prev[c : c + 1, :] = disp[0, c] - vel[0, c]


def setup_tables(kind, table, tpad, d1, d2):
    tpad[...] = jnp.zeros(tpad.shape, F32)
    tpad[0 : kind.P, 0 : kind.KQ] = table[...]
    across = tpad[...]
    whole = across.T
    hi, lo = split(across[0 : kind.PP])
    stack = [hi, hi, lo]
    left = 128 - 3 * kind.PP
    if left:
        stack.append(jnp.zeros((left, 128), F32))
    d1[...] = jnp.concatenate(stack, axis=0).T
    hi, lo = split(-whole[0 : kind.KQ])
    depth = d2.shape[1]
    stack = [hi, hi, lo]
    left = depth - 3 * kind.KQ
    if left:
        stack.append(jnp.zeros((left, 128), F32))
    stack = jnp.concatenate(stack, axis=0)
    for k in range(depth // 128):
        d2[:, k * 128 : (k + 1) * 128] = stack[k * 128 : (k + 1) * 128].T


def setup_plan(kind, nodes, send_map, node_s, key_s, plan_s, pos_s):
    sub = iota2((8, 128), 0)
    lane = iota2((8, 128), 1)
    node_s[...] = jnp.zeros(node_s.shape, jnp.int32)
    for k in range(kind.LC):
        for p in range(kind.P):
            at = k * kind.PP + p
            node_s[at : at + 1, :] = nodes[0, p, :, k * 128 : (k + 1) * 128]
    for w in range(kind.W8):
        inside = ((sub + w * 8) % kind.PP) < kind.P
        found = jnp.where(inside, node_s[w * 8 : w * 8 + 8, :], BIG >> SHIFT)
        keys = sort_regs([(found << SHIFT) | (sub << 7) | lane])[0]
        key_s[w * 8 : w * 8 + 8, :] = keys
        slot = keys & ((1 << SHIFT) - 1)
        plan_s[0, w * 8 : w * 8 + 8, :] = jnp.where(keys < BIG, slot >> 7, 1000)
        plan_s[1, w * 8 : w * 8 + 8, :] = slot & 127
    sent = jnp.zeros((8, 128), jnp.int32)
    for side in range(2):
        wanted = spread(send_map[0, 0, side : side + 1, :])
        sent = jnp.where(sub == 2 * side, wanted + 1, sent)
        sent = jnp.where(sub == 2 * side + 1, wanted, sent)
    find_places(kind, [(kind.NRP // 8, sent << SHIFT)], key_s, pos_s)


def setup_ends(kind, key_s, pos_s):
    sub = iota2((8, 128), 0)
    lane = iota2((8, 128), 1)
    targets = [(v, ((sub + v * 8) * 128 + lane + 1) << SHIFT) for v in range(kind.NRP // 8)]
    find_places(kind, targets, key_s, pos_s)


def find_places(kind, targets, key_s, pos_s):
    for w in range(kind.W8):
        last = spread(key_s[w * 8 + 7 : w * 8 + 8, :])
        for v, target in targets:
            column = jnp.zeros((8, 128), jnp.int32)
            for step in (64, 32, 16, 8, 4, 2, 1):
                column = jnp.where(lane_take(last, column + (step - 1)) < target, column + step, column)
            place = column * 8 - 1
            for r in range(8):
                row = spread(key_s[w * 8 + r : w * 8 + r + 1, :])
                place = place + jnp.where(lane_take(row, column) < target, 1, 0)
            pos_s[v, w, 0] = jnp.where(place < 0, 1000, place & 7)
            pos_s[v, w, 1] = jnp.where(place < 0, 0, place >> 3)


def setup_scan(scan):
    row = iota2(scan.shape, 0) % 128
    col = iota2(scan.shape, 1)
    scan[...] = jnp.where(row < col, 1.0, 0.0).astype(BF16)


def setup_hot(kind, maps, hot):
    rows = iota2((kind.N, 128), 0)
    for k, load in enumerate(maps):
        hot[:, k * 128 : (k + 1) * 128] = jnp.where(rows == load(), 1.0, 0.0).astype(BF16)


def gather_nodes(kind, u, node_s):
    blocks = {}
    for w in range(kind.W8):
        index = node_s[w * 8 : w * 8 + 8, :]
        found = gather_three(
            index >> 7,
            index & 127,
            lambda c, r: u[c : c + 1, r * 128 : (r + 1) * 128],
            range(kind.NR),
        )
        for c in range(3):
            blocks[c, w] = found[c]
    return blocks


def setup_compact(kind, recv_map, minv, node_s, hot, equal, minv_c, slot_j):
    rows = [recv_map[0, 0, i : i + 1, :] for i in range(2)]
    wide = jnp.concatenate(rows, axis=1)
    down = jnp.concatenate(
        [jnp.broadcast_to(row.astype(F32), (128, 128)).T for row in rows], axis=0
    ).astype(jnp.int32)
    across = jnp.concatenate([down, down], axis=1) == wide
    equal[...] = jnp.where(across, 1.0, 0.0).astype(BF16)
    row = iota2((256, 256), 0)
    col = iota2((256, 256), 1)
    earlier = jnp.where(across & (row < col), 1.0, 0.0)
    count = mm(jnp.ones((16, 256), F32), earlier)
    name = jnp.where(count < 0.5, iota2((16, 256), 1) + 1, 0).astype(F32)
    table = lax.dot_general(
        name.astype(BF16), hot[...], (((1,), (1,)), ((), ())), preferred_element_type=F32
    )
    spread_minv = jnp.broadcast_to(minv, (8, kind.N))
    for i in range(2):
        minv_c[:, i * 128 : (i + 1) * 128] = pick(kind, spread_minv, rows[i])
    for w in range(kind.W8):
        index = node_s[w * 8 : w * 8 + 8, :]
        idx_row, idx_lane = index >> 7, index & 127
        found = jnp.zeros((8, 128), F32)
        for r in range(kind.NR):
            part = lane_take(spread(table[0:1, r * 128 : (r + 1) * 128]), idx_lane)
            found = jnp.where(idx_row == r, part, found)
        found = found.astype(jnp.int32) - 1
        slot_j[0, w * 8 : w * 8 + 8, :] = jnp.where(found < 0, 1000, found >> 7)
        slot_j[1, w * 8 : w * 8 + 8, :] = jnp.where(found < 0, 0, found & 127)


def setup_wide(kind, table, wide_1, wide_2):
    for b in range(3):
        for q in range(kind.Q):
            entry = jnp.concatenate(
                [table[b * kind.Q + q : b * kind.Q + q + 1, :], jnp.zeros((1, 128 - kind.P), F32)],
                axis=1,
            )
            down = jnp.broadcast_to(entry, (128, 128)).T
            wide_2[b * kind.Q + q] = -down[0 : kind.PP]
    for p in range(kind.P):
        for b in range(3):
            for q in range(kind.Q):
                wide_1[p, b * 8 + q : b * 8 + q + 1, :] = -wide_2[b * kind.Q + q, p : p + 1, :]


def small_products(kind, values, coef, wide_1, wide_2, fe_s):
    for k in range(kind.LC):
        for c in range(3):
            grad = [None] * 3
            for p in range(kind.P):
                block = values[c, (k * kind.PP + p) // 8]
                row = jnp.broadcast_to(block[p % 8 : p % 8 + 1], (8, 128))
                for b in range(3):
                    term = wide_1[p, b * 8 : b * 8 + 8, :] * row
                    grad[b] = term if p == 0 else grad[b] + term
            terms = [None] * (kind.PP // 8)
            for a in range(3):
                flux = coef(a, 0, k) * grad[0] + coef(a, 1, k) * grad[1] + coef(a, 2, k) * grad[2]
                for q in range(kind.Q):
                    row = jnp.broadcast_to(flux[q : q + 1], (8, 128))
                    for v in range(kind.PP // 8):
                        term = wide_2[a * kind.Q + q, v * 8 : v * 8 + 8, :] * row
                        terms[v] = term if a + q == 0 else terms[v] + term
            for v in range(kind.PP // 8):
                fe_s[c, k * kind.PP + v * 8 : k * kind.PP + v * 8 + 8, :] = terms[v]


def large_products(kind, values, coef, d1, d2, fe_s):
    blocks = {}
    for k in range(kind.LC):
        for v in range(kind.PP // 8):
            for c in range(3):
                blocks[c, k, v] = values[c, (k * kind.PP) // 8 + v]
    chunks = [(c, k) for c in range(3) for k in range(kind.LC)]
    cols = []
    for c, k in chunks:
        ve = jnp.concatenate([blocks[c, k, v] for v in range(kind.PP // 8)], axis=0)
        hi, lo = split(ve)
        parts = [hi, lo, hi]
        left = 128 - 3 * kind.PP
        if left:
            parts.append(jnp.zeros((left, 128), F32))
        cols.append(jnp.concatenate(parts, axis=0).astype(BF16))
    gathered = jnp.concatenate(cols, axis=1)
    grad = jnp.dot(d1[0 : kind.KQ, :].astype(BF16), gathered, preferred_element_type=F32)
    cols = []
    depth = d2.shape[1]
    for i, (c, k) in enumerate(chunks):
        piece = grad[:, i * 128 : (i + 1) * 128]
        terms = []
        for a in range(3):
            total = coef(a, 0, k) * piece[0 : kind.QP]
            for b in (1, 2):
                total = total + coef(a, b, k) * piece[b * kind.QP : (b + 1) * kind.QP]
            terms.append(total)
        flux = jnp.concatenate(terms, axis=0)
        hi, lo = split(flux)
        parts = [hi, lo, hi]
        left = depth - 3 * kind.KQ
        if left:
            parts.append(jnp.zeros((left, 128), F32))
        cols.append(jnp.concatenate(parts, axis=0).astype(BF16))
    flux = jnp.concatenate(cols, axis=1)
    fe = jnp.dot(d2[0 : kind.PP, :].astype(BF16), flux, preferred_element_type=F32)
    for i, (c, k) in enumerate(chunks):
        fe_s[c, k * kind.PP : (k + 1) * kind.PP, :] = fe[:, i * 128 : (i + 1) * 128]


def sum_sorted(kind, plan_s, scan, fe_s, cx_s):
    sub = iota2((8, 128), 0)
    terms = {}
    both = []
    for w in range(kind.W8):
        found = gather_three(
            plan_s[0, w * 8 : w * 8 + 8, :],
            plan_s[1, w * 8 : w * 8 + 8, :],
            lambda c, r: fe_s[c, w * 8 + r : w * 8 + r + 1, :],
            [r for r in range(8) if (w * 8 + r) % kind.PP < kind.P],
        )
        for c in range(3):
            hi, lo = split(found[c])
            both.append(jnp.concatenate([hi, lo], axis=1))
            upto = found[c]
            for dist in (1, 2, 4):
                upto = upto + jnp.where(sub >= dist, pltpu.roll(upto, dist, 0), 0.0)
            terms[w, c] = upto
    sums = jnp.dot(
        jnp.concatenate(both, axis=0).astype(BF16), scan[...], preferred_element_type=F32
    )
    for w in range(kind.W8):
        for c in range(3):
            at = (w * 3 + c) * 8
            ahead = sums[at : at + 8]
            for dist in (4, 2, 1):
                ahead = ahead + pltpu.roll(ahead, dist, 0)
            cx_s[c, w * 8 : w * 8 + 8, :] = terms[w, c] + ahead


def read_ends(kind, v, pos_s, cx_s):
    total = None
    for w in range(kind.W8):
        found = gather_three(
            pos_s[v, w, 0],
            pos_s[v, w, 1],
            lambda c, r: cx_s[c, w * 8 + r : w * 8 + r + 1, :],
            range(8),
        )
        total = found if total is None else [a + b for a, b in zip(total, found)]
    return total


def node_forces(kind, pos_s, cx_s, f_s):
    corner_row = iota2((kind.NRP, 128), 0)
    corner_lane = iota2((kind.NRP, 128), 1)
    found = [read_ends(kind, v, pos_s, cx_s) for v in range(kind.NRP // 8)]
    for c in range(3):
        ends = jnp.concatenate([block[c] for block in found], axis=0)
        before = pltpu.roll(ends, 1, 1)
        above = pltpu.roll(before, 1, 0)
        before = jnp.where(corner_lane == 0, above, before)
        before = jnp.where((corner_lane == 0) & (corner_row == 0), 0.0, before)
        forces = ends - before
        for r in range(kind.NR):
            f_s[c : c + 1, r * 128 : (r + 1) * 128] = forces[r : r + 1, :]


def pick(kind, source, index):
    idx_row, idx_lane = spread(index >> 7), spread(index & 127)
    out = jnp.zeros((8, 128), F32)
    for r in range(kind.NR):
        out = jnp.where(
            idx_row == r, lane_take(source[:, r * 128 : (r + 1) * 128], idx_lane), out
        )
    return out


def drop(kind, parts, hot):
    r = jnp.concatenate(parts, axis=1)
    hi, lo = split(r)
    both = jnp.concatenate([hi, lo], axis=0).astype(BF16)
    out = lax.dot_general(
        both, hot[...], (((1,), (1,)), ((), ())), preferred_element_type=F32
    )
    return out[0:8] + out[8:16]


def body(
    reg, site, reg_groups, site_groups, sub_count,
    reg_disp, reg_vel, site_disp, site_vel, reg_nodes, site_nodes, reg_coefs, site_coefs,
    reg_table, site_table, reg_minv, site_minv, reg_send, reg_recv, site_send, site_recv,
    slot_fill, layer_src, layer_fill, layer_dst, layer_stiff,
    reg_out, site_out,
    u_r, prev_r, f_r, wide_1, wide_2, node_r, key_r, plan_r, pos_r, hot_r, fe_r, cx_r, coef_r,
    u_s, prev_s, f_s, tpad_s, d1_s, d2_s, node_s, key_s, plan_s, pos_s, hot_s, fe_s, cx_s,
    hot_l, kept, slot_c, equal, minv_c, small, scan, fills, sends, recvs, layer_out, layer_in,
    send_sem, recv_sem, layer_send_sem, layer_recv_sem,
):
    grp = lax.axis_index("grp")
    sub = lax.axis_index("sub")
    is_site = grp >= reg_groups
    has_lower = sub > 0
    has_upper = sub < sub_count - 1
    source = grp // site_groups
    target = reg_groups + grp % site_groups
    barrier = pltpu.get_barrier_semaphore()

    def hello(g, s):
        pl.semaphore_signal(barrier, inc=1, device_id=(g, s), device_id_type=MESH)

    @pl.when(has_lower)
    def _():
        hello(grp, sub - 1)

    @pl.when(has_upper)
    def _():
        hello(grp, sub + 1)

    @pl.when(is_site)
    def _():
        for m in range(3):
            hello(m * site_groups + grp - reg_groups, sub)

    @pl.when(jnp.logical_not(is_site))
    def _():
        hello(target, sub)

    for there, side in ((has_lower, 0), (has_upper, 1)):

        @pl.when(jnp.logical_not(there))
        def _():
            for n in range(STEPS):
                recvs[n, side] = jnp.zeros((8, 128), F32)

    lane = iota2((8, 128), 1)
    live = iota2((8, 128), 0) < 3
    greeted = has_lower.astype(jnp.int32) + has_upper.astype(jnp.int32) + jnp.where(is_site, 3, 1)

    def edge(n, side):
        peer = sub - 1 if side == 0 else sub + 1
        return pltpu.make_async_remote_copy(
            src_ref=sends.at[n, side, 0:3],
            dst_ref=recvs.at[n, 1 - side, 0:3],
            send_sem=send_sem.at[n, side],
            recv_sem=recv_sem.at[n, 1 - side],
            device_id=(grp, peer),
            device_id_type=MESH,
        )

    def layer_copy(n, m):
        return pltpu.make_async_remote_copy(
            src_ref=layer_out.at[n, 0:3],
            dst_ref=layer_in.at[n, m, 0:3],
            send_sem=layer_send_sem.at[n],
            recv_sem=layer_recv_sem.at[n, m],
            device_id=(target, sub),
            device_id_type=MESH,
        )

    sides = ((has_lower, 0), (has_upper, 1))

    def exchange(kind, n, pos, cx):
        found = read_ends(kind, kind.NRP // 8, pos, cx)
        for there, side in sides:
            for c in range(3):
                force = found[c][2 * side : 2 * side + 1] - found[c][2 * side + 1 : 2 * side + 2]
                sends[n, side, c : c + 1, :] = jnp.where(lane[0:1] < fills[side : side + 1, :], force, 0.0)

            @pl.when(there)
            def _():
                edge(n, side).start()

    def arrive(n):
        for there, side in sides:

            @pl.when(there)
            def _():
                edge(n, 1 - side).wait_recv()

    def arrived(n, side):
        return jnp.where(live, recvs[n, side], 0.0)

    def finish(n, carry):
        for there, side in sides:

            @pl.when(there)
            def _():
                edge(n, side).wait_send()

        return carry

    setup_scan(scan)
    sends[...] = jnp.zeros(sends.shape, F32)

    @pl.when(jnp.logical_not(is_site))
    def _():
        kind = reg
        setup_state(kind, reg_disp, reg_vel, u_r, prev_r)
        f_r[...] = jnp.zeros(f_r.shape, F32)
        wide_1[...] = jnp.zeros(wide_1.shape, F32)
        setup_wide(kind, reg_table, wide_1, wide_2)
        coef_r[...] = jnp.zeros(coef_r.shape, F32)
        coef_r[:, :, 0 : kind.Q, :] = reg_coefs[0, 0]
        setup_plan(kind, reg_nodes, reg_send, node_r, key_r, plan_r, pos_r)
        pl.semaphore_wait(barrier, greeted)
        for i in range(2):
            fills[i : i + 1, :] = jnp.broadcast_to(slot_fill[0, :, i : i + 1], (1, 128))
        fills[2:3, :] = jnp.broadcast_to(layer_fill[...], (1, 128))

        def step(n, carry):
            small_products(
                kind, gather_nodes(kind, u_r, node_r),
                lambda a, b, k: coef_r[a, b, :, k * 128 : (k + 1) * 128],
                wide_1, wide_2, fe_r,
            )
            sum_sorted(kind, plan_r, scan, fe_r, cx_r)
            exchange(kind, n, pos_r, cx_r)

            @pl.when(n == 0)
            def _():
                setup_ends(kind, key_r, pos_r)
                setup_hot(kind, [lambda i=i: reg_recv[0, 0, i : i + 1, :] for i in range(2)], hot_r)

            node_forces(kind, pos_r, cx_r, f_r)
            minv = reg_minv[0]
            now = u_r[...]
            ahead = 2.0 * now - prev_r[...] + minv * f_r[...]
            prev_r[...] = now
            arrive(n)
            u_r[...] = ahead + minv * drop(kind, [arrived(n, i) for i in range(2)], hot_r)
            found = pick(kind, u_r, layer_src[0])
            layer_out[n] = jnp.where(lane < fills[2:3, :], found, 0.0)
            layer_copy(n, source).start()
            return carry

        lax.fori_loop(0, STEPS, step, 0)
        for c in range(3):
            reg_out[0, c] = u_r[c : c + 1, :]
        site_out[...] = jnp.zeros(site_out.shape, F32)

        def drain(n, carry):
            layer_copy(n, source).wait_send()
            return finish(n, carry)

        lax.fori_loop(0, STEPS, drain, 0)

    @pl.when(is_site)
    def _():
        kind = site
        setup_state(kind, site_disp, site_vel, u_s, prev_s)
        f_s[...] = jnp.zeros(f_s.shape, F32)
        setup_tables(kind, site_table, tpad_s, d1_s, d2_s)
        setup_plan(kind, site_nodes, site_send, node_s, key_s, plan_s, pos_s)
        pl.semaphore_wait(barrier, greeted)
        for i in range(2):
            fills[i : i + 1, :] = jnp.broadcast_to(slot_fill[0, :, i + 2 : i + 3], (1, 128))

        slot_c[...] = jnp.full(slot_c.shape, 1000, jnp.int32)
        slot_c[1] = jnp.zeros(slot_c.shape[1:], jnp.int32)
        small[...] = jnp.zeros(small.shape, F32)
        hot_s[...] = jnp.zeros(hot_s.shape, BF16)

        def keep_gathered(field):
            for (c, w), block in gather_nodes(kind, field, node_s).items():
                kept[c, w * 8 : w * 8 + 8, :] = block

        def complete():
            last = jnp.concatenate([small[0:8], small[8:16]], axis=0)
            out = lax.dot_general(
                last.astype(BF16), hot_s[...], (((1,), (1,)), ((), ())), preferred_element_type=F32
            )
            return u_s[...] + site_minv[0] * (out[0:8] + out[8:16])

        keep_gathered(u_s)

        def step(n, carry):
            values = {}
            for w in range(kind.W8):
                found = gather_three(
                    slot_c[0, w * 8 : w * 8 + 8, :],
                    slot_c[1, w * 8 : w * 8 + 8, :],
                    lambda c, r: small[16 + c : 17 + c, r * 128 : (r + 1) * 128],
                    range(2),
                )
                for c in range(3):
                    values[c, w] = kept[c, w * 8 : w * 8 + 8, :] + found[c]
            large_products(
                kind, values, lambda a, b, k: site_coefs[0, 0, a, b], d1_s, d2_s, fe_s
            )
            sum_sorted(kind, plan_s, scan, fe_s, cx_s)
            exchange(kind, n, pos_s, cx_s)
            now = complete()

            @pl.when(n == 0)
            def _():
                setup_ends(kind, key_s, pos_s)
                setup_hot(kind, [lambda i=i: site_recv[0, 0, i : i + 1, :] for i in range(2)], hot_s)
                setup_hot(kind, [lambda i=i: layer_dst[0, i] for i in range(3)], hot_l)
                setup_compact(kind, site_recv, site_minv[0], node_s, hot_s, equal, minv_c, slot_c)

            node_forces(kind, pos_s, cx_s, f_s)
            minv = site_minv[0]
            ahead = 2.0 * now - prev_s[...] + minv * f_s[...]
            prev_s[...] = now
            parts = []
            for m in range(3):
                layer_copy(n, m).wait_recv()
                parts.append(jnp.where(live, layer_in[n, m], 0.0) * layer_stiff[0, m])
            u_s[...] = ahead + minv * drop(kind, parts, hot_l)
            keep_gathered(u_s)
            arrive(n)
            hi, lo = split(jnp.concatenate([arrived(n, i) for i in range(2)], axis=1))
            small[0:8] = hi
            small[8:16] = lo
            sums = mm(jnp.concatenate([hi, lo], axis=0), equal[...])
            small[16:24] = (sums[0:8] + sums[8:16]) * minv_c[...]
            return carry

        lax.fori_loop(0, STEPS, step, 0)
        u_s[...] = complete()
        for c in range(3):
            site_out[0, c] = u_s[c : c + 1, :]
        reg_out[...] = jnp.zeros(reg_out.shape, F32)
        lax.fori_loop(0, STEPS, finish, 0)


def kind_scratch(kind, tables):
    i32 = jnp.int32
    return [
        pltpu.VMEM((8, kind.N), F32),
        pltpu.VMEM((8, kind.N), F32),
        pltpu.VMEM((8, kind.N), F32),
        *tables,
        pltpu.VMEM((kind.SR, 128), i32),
        pltpu.VMEM((kind.SR, 128), i32),
        pltpu.VMEM((2, kind.SR, 128), i32),
        pltpu.VMEM((kind.NRP // 8 + 1, kind.W8, 2, 8, 128), i32),
        pltpu.VMEM((kind.N, 256), BF16),
        pltpu.VMEM((3, kind.SR, 128), F32),
        pltpu.VMEM((3, kind.SR, 128), F32),
    ]


def shards(*args):
    group_count = lax.axis_size("grp")
    site_groups = group_count // 4
    reg_groups = 3 * site_groups
    reg = Kind(args[4].shape[2], args[6].shape[4], args[4].shape[3], args[0].shape[3])
    site = Kind(args[5].shape[2], args[7].shape[4], args[5].shape[3], args[2].shape[3])
    args = list(args)
    for i in (0, 1, 2, 3, 4, 5, 19, 20):
        args[i] = jnp.transpose(args[i], (0, 2, 1, 3))
    args[9] = args[9].T
    vmem = pl.BlockSpec(memory_space=pltpu.VMEM)
    in_specs = [vmem] * len(args)
    kernel = functools.partial(body, reg, site, reg_groups, site_groups, lax.axis_size("sub"))
    outs = pl.pallas_call(
        kernel,
        name="drm_window",
        out_shape=(
            pltpu.VMEM((1, 3, 1, reg.N), F32),
            pltpu.VMEM((1, 3, 1, site.N), F32),
        ),
        in_specs=in_specs,
        out_specs=(vmem, vmem),
        scratch_shapes=kind_scratch(
            reg,
            [
                pltpu.VMEM((reg.P, 24, 128), F32),
                pltpu.VMEM((3 * reg.Q, reg.PP, 128), F32),
            ],
        )
        + [pltpu.VMEM((3, 3, reg.QP, reg.E), F32)]
        + kind_scratch(
            site,
            [
                pltpu.VMEM((128, 128), F32),
                pltpu.VMEM((128, 128), F32),
                pltpu.VMEM((128, pad_to(3 * site.KQ, 128)), F32),
            ],
        )
        + [
            pltpu.VMEM((site.N, 384), BF16),
            pltpu.VMEM((3, site.SR, 128), F32),
            pltpu.VMEM((2, site.SR, 128), jnp.int32),
            pltpu.VMEM((256, 256), BF16),
            pltpu.VMEM((8, 256), F32),
            pltpu.VMEM((24, 256), F32),
            pltpu.VMEM((256, 128), BF16),
            pltpu.VMEM((8, 128), jnp.int32),
            pltpu.VMEM((STEPS, 2, 8, 128), F32),
            pltpu.VMEM((STEPS, 2, 8, 128), F32),
            pltpu.VMEM((STEPS, 8, 128), F32),
            pltpu.VMEM((STEPS, 3, 8, 128), F32),
            pltpu.SemaphoreType.DMA((STEPS, 2)),
            pltpu.SemaphoreType.DMA((STEPS, 2)),
            pltpu.SemaphoreType.DMA((STEPS,)),
            pltpu.SemaphoreType.DMA((STEPS, 3)),
        ],
        compiler_params=pltpu.CompilerParams(collective_id=0, has_side_effects=True),
    )(*args)
    return tuple(jnp.transpose(out, (0, 2, 1, 3)) for out in outs)


def solution(mesh):
    whole = P("grp", "sub")
    specs = [whole] * 21
    specs[8] = P()
    specs[9] = P()
    return jax.shard_map(
        shards,
        mesh=mesh,
        in_specs=tuple(specs),
        out_specs=(whole, whole),
        check_vma=False,
    )
```

```python
import functools

import jax
import jax.numpy as jnp
from jax import lax
from jax.experimental import pallas as pl
from jax.experimental.pallas import tpu as pltpu
from jax.sharding import PartitionSpec as P

STEPS = 8
MESH = pl.DeviceIdType.MESH
SHIFT = 13
BIG = 2047 << SHIFT
F32 = jnp.float32
BF16 = jnp.bfloat16


def pad_to(value, unit):
    return -(-value // unit) * unit


class Kind:
    def __init__(self, points, quads, elems, nodes):
        self.P, self.Q, self.E, self.N = points, quads, elems, nodes
        self.LC = elems // 128
        self.NR = nodes // 128
        self.NRP = pad_to(self.NR, 8)
        self.PP = pad_to(points, 8)
        self.QP = pad_to(quads, 8)
        self.KQ = 3 * self.QP
        self.SR = self.LC * self.PP
        self.W8 = self.SR // 8


def lane_take(x, idx):
    dims = lax.GatherDimensionNumbers(
        offset_dims=(),
        collapsed_slice_dims=(1,),
        start_index_map=(1,),
        operand_batching_dims=(0,),
        start_indices_batching_dims=(0,),
    )
    return lax.gather(
        x, idx[..., None], dims, (1, 1), mode=lax.GatherScatterMode.PROMISE_IN_BOUNDS
    )


def iota2(shape, dim):
    return lax.broadcasted_iota(jnp.int32, shape, dim)


def spread(row):
    return jnp.broadcast_to(row, (8, 128))


def split(x):
    hi = x.astype(BF16).astype(F32)
    return hi, x - hi


def mm(a, b):
    return jnp.dot(a.astype(BF16), b.astype(BF16), preferred_element_type=F32)


def sort_regs(regs):
    count = len(regs)
    depth = count * 8
    row_bits = depth.bit_length() - 1
    sub = iota2((8, 128), 0)
    lane = iota2((8, 128), 1)

    def bit_mask(bit, v):
        if bit < 3:
            return (sub >> bit) & 1
        if bit < row_bits:
            return (v >> (bit - 3)) & 1
        if bit >= row_bits + 7:
            return 0
        return (lane >> (bit - row_bits)) & 1

    total_bits = row_bits + 7
    for m in range(1, total_bits + 1):
        jb = m
        while jb > 0:
            jb -= 1
            new = list(regs)
            if jb - 1 >= row_bits:
                far, near = 1 << (jb - row_bits), 1 << (jb - 1 - row_bits)
                for v in range(count):
                    x = regs[v]
                    first = (bit_mask(jb, v) ^ bit_mask(m, v)) == 1
                    second = (bit_mask(jb - 1, v) ^ bit_mask(m, v)) == 1
                    other = lane_take(x, lane ^ far)
                    mine = jnp.where(first, jnp.maximum(x, other), jnp.minimum(x, other))
                    x = lane_take(regs[v], lane ^ near)
                    other = lane_take(regs[v], lane ^ (far + near))
                    theirs = jnp.where(first, jnp.maximum(x, other), jnp.minimum(x, other))
                    new[v] = jnp.where(
                        second, jnp.maximum(mine, theirs), jnp.minimum(mine, theirs)
                    )
                regs = new
                jb -= 1
                continue
            if 3 <= jb < row_bits:
                step = 1 << (jb - 3)
                for v in range(count):
                    if v & step:
                        continue
                    a, b = regs[v], regs[v + step]
                    low, high = jnp.minimum(a, b), jnp.maximum(a, b)
                    down = bit_mask(m, v)
                    if isinstance(down, int):
                        new[v], new[v + step] = (high, low) if down else (low, high)
                    else:
                        new[v] = jnp.where(down == 1, high, low)
                        new[v + step] = jnp.where(down == 1, low, high)
            else:
                for v in range(count):
                    x = regs[v]
                    if jb < 3:
                        dist = 1 << jb
                        if dist == 4:
                            other = pltpu.roll(x, 4, 0)
                        else:
                            other = jnp.where(
                                bit_mask(jb, v) == 1, pltpu.roll(x, dist, 0), pltpu.roll(x, 8 - dist, 0)
                            )
                    else:
                        dist = 1 << (jb - row_bits)
                        other = lane_take(x, lane ^ dist)
                    take_max = bit_mask(jb, v) ^ bit_mask(m, v)
                    new[v] = jnp.where(take_max == 1, jnp.maximum(x, other), jnp.minimum(x, other))
            regs = new
    return regs


def gather_three(idx_row, idx_lane, load_row, rows):
    out = [jnp.zeros((8, 128), F32) for _ in range(3)]
    for r in rows:
        here = idx_row == r
        for c in range(3):
            out[c] = jnp.where(here, lane_take(spread(load_row(c, r)), idx_lane), out[c])
    return out


def setup_state(kind, disp, vel, u, prev):
    for ref in (u, prev):
        ref[...] = jnp.zeros(ref.shape, F32)
    for c in range(3):
        u[c : c + 1, :] = disp[0, c]
        prev[c : c + 1, :] = disp[0, c] - vel[0, c]


def setup_tables(kind, table, tpad, d1, d2):
    tpad[...] = jnp.zeros(tpad.shape, F32)
    tpad[0 : kind.P, 0 : kind.KQ] = table[...]
    across = tpad[...]
    whole = across.T
    hi, lo = split(across[0 : kind.PP])
    stack = [hi, hi, lo]
    left = 128 - 3 * kind.PP
    if left:
        stack.append(jnp.zeros((left, 128), F32))
    d1[...] = jnp.concatenate(stack, axis=0).T
    hi, lo = split(-whole[0 : kind.KQ])
    depth = d2.shape[1]
    stack = [hi, hi, lo]
    left = depth - 3 * kind.KQ
    if left:
        stack.append(jnp.zeros((left, 128), F32))
    stack = jnp.concatenate(stack, axis=0)
    for k in range(depth // 128):
        d2[:, k * 128 : (k + 1) * 128] = stack[k * 128 : (k + 1) * 128].T


def setup_plan(kind, nodes, send_map, node_s, key_s, plan_s, pos_s):
    sub = iota2((8, 128), 0)
    lane = iota2((8, 128), 1)
    node_s[...] = jnp.zeros(node_s.shape, jnp.int32)
    for k in range(kind.LC):
        for p in range(kind.P):
            at = k * kind.PP + p
            node_s[at : at + 1, :] = nodes[0, p, :, k * 128 : (k + 1) * 128]
    for w in range(kind.W8):
        inside = ((sub + w * 8) % kind.PP) < kind.P
        found = jnp.where(inside, node_s[w * 8 : w * 8 + 8, :], BIG >> SHIFT)
        keys = sort_regs([(found << SHIFT) | (sub << 7) | lane])[0]
        key_s[w * 8 : w * 8 + 8, :] = keys
        slot = keys & ((1 << SHIFT) - 1)
        plan_s[0, w * 8 : w * 8 + 8, :] = jnp.where(keys < BIG, slot >> 7, 1000)
        plan_s[1, w * 8 : w * 8 + 8, :] = slot & 127
    sent = jnp.zeros((8, 128), jnp.int32)
    for side in range(2):
        wanted = spread(send_map[0, 0, side : side + 1, :])
        sent = jnp.where(sub == 2 * side, wanted + 1, sent)
        sent = jnp.where(sub == 2 * side + 1, wanted, sent)
    find_places(kind, [(kind.NRP // 8, sent << SHIFT)], key_s, pos_s)


def setup_ends(kind, key_s, pos_s):
    sub = iota2((8, 128), 0)
    lane = iota2((8, 128), 1)
    targets = [(v, ((sub + v * 8) * 128 + lane + 1) << SHIFT) for v in range(kind.NRP // 8)]
    find_places(kind, targets, key_s, pos_s)


def find_places(kind, targets, key_s, pos_s):
    for w in range(kind.W8):
        last = spread(key_s[w * 8 + 7 : w * 8 + 8, :])
        for v, target in targets:
            column = jnp.zeros((8, 128), jnp.int32)
            for step in (32, 8, 2):
                passed = [
                    jnp.where(lane_take(last, column + (i * step - 1)) < target, step, 0)
                    for i in (1, 2, 3)
                ]
                column = column + passed[0] + passed[1] + passed[2]
            column = jnp.where(lane_take(last, column) < target, column + 1, column)
            place = column * 8 - 1
            for r in range(8):
                row = spread(key_s[w * 8 + r : w * 8 + r + 1, :])
                place = place + jnp.where(lane_take(row, column) < target, 1, 0)
            pos_s[v, w, 0] = jnp.where(place < 0, 1000, place & 7)
            pos_s[v, w, 1] = jnp.where(place < 0, 0, place >> 3)


def setup_scan(scan):
    row = iota2(scan.shape, 0) % 128
    col = iota2(scan.shape, 1)
    scan[...] = jnp.where(row < col, 1.0, 0.0).astype(BF16)


def setup_hot(kind, maps, hot):
    rows = iota2((kind.N, 128), 0)
    for k, load in enumerate(maps):
        hot[:, k * 128 : (k + 1) * 128] = jnp.where(rows == load(), 1.0, 0.0).astype(BF16)


def gather_nodes(kind, u, node_s):
    blocks = {}
    for w in range(kind.W8):
        index = node_s[w * 8 : w * 8 + 8, :]
        found = gather_three(
            index >> 7,
            index & 127,
            lambda c, r: u[c : c + 1, r * 128 : (r + 1) * 128],
            range(kind.NR),
        )
        for c in range(3):
            blocks[c, w] = found[c]
    return blocks


def setup_compact(kind, recv_map, minv, node_s, hot, equal, minv_c, slot_j):
    rows = [recv_map[0, 0, i : i + 1, :] for i in range(2)]
    wide = jnp.concatenate(rows, axis=1)
    down = jnp.concatenate(
        [jnp.broadcast_to(row.astype(F32), (128, 128)).T for row in rows], axis=0
    ).astype(jnp.int32)
    across = jnp.concatenate([down, down], axis=1) == wide
    equal[...] = jnp.where(across, 1.0, 0.0).astype(BF16)
    row = iota2((256, 256), 0)
    col = iota2((256, 256), 1)
    earlier = jnp.where(across & (row < col), 1.0, 0.0)
    count = mm(jnp.ones((16, 256), F32), earlier)
    name = jnp.where(count < 0.5, iota2((16, 256), 1) + 1, 0).astype(F32)
    table = lax.dot_general(
        name.astype(BF16), hot[...], (((1,), (1,)), ((), ())), preferred_element_type=F32
    )
    spread_minv = jnp.broadcast_to(minv, (8, kind.N))
    for i in range(2):
        minv_c[:, i * 128 : (i + 1) * 128] = pick(kind, spread_minv, rows[i])
    for w in range(kind.W8):
        index = node_s[w * 8 : w * 8 + 8, :]
        idx_row, idx_lane = index >> 7, index & 127
        found = jnp.zeros((8, 128), F32)
        for r in range(kind.NR):
            part = lane_take(spread(table[0:1, r * 128 : (r + 1) * 128]), idx_lane)
            found = jnp.where(idx_row == r, part, found)
        found = found.astype(jnp.int32) - 1
        slot_j[0, w * 8 : w * 8 + 8, :] = jnp.where(found < 0, 1000, found >> 7)
        slot_j[1, w * 8 : w * 8 + 8, :] = jnp.where(found < 0, 0, found & 127)


def setup_wide(kind, table, wide_1, wide_2):
    for b in range(3):
        for q in range(kind.Q):
            entry = jnp.concatenate(
                [table[b * kind.Q + q : b * kind.Q + q + 1, :], jnp.zeros((1, 128 - kind.P), F32)],
                axis=1,
            )
            down = jnp.broadcast_to(entry, (128, 128)).T
            wide_2[b * kind.Q + q] = -down[0 : kind.PP]
    for p in range(kind.P):
        for b in range(3):
            for q in range(kind.Q):
                wide_1[p, b * 8 + q : b * 8 + q + 1, :] = -wide_2[b * kind.Q + q, p : p + 1, :]


def small_products(kind, values, coef, wide_1, wide_2, fe_s):
    for k in range(kind.LC):
        for c in range(3):
            grad = [None] * 3
            for p in range(kind.P):
                block = values[c, (k * kind.PP + p) // 8]
                row = jnp.broadcast_to(block[p % 8 : p % 8 + 1], (8, 128))
                for b in range(3):
                    term = wide_1[p, b * 8 : b * 8 + 8, :] * row
                    grad[b] = term if p == 0 else grad[b] + term
            terms = [None] * (kind.PP // 8)
            for a in range(3):
                flux = coef(a, 0, k) * grad[0] + coef(a, 1, k) * grad[1] + coef(a, 2, k) * grad[2]
                for q in range(kind.Q):
                    row = jnp.broadcast_to(flux[q : q + 1], (8, 128))
                    for v in range(kind.PP // 8):
                        term = wide_2[a * kind.Q + q, v * 8 : v * 8 + 8, :] * row
                        terms[v] = term if a + q == 0 else terms[v] + term
            for v in range(kind.PP // 8):
                fe_s[c, k * kind.PP + v * 8 : k * kind.PP + v * 8 + 8, :] = terms[v]


def large_products(kind, values, coef, d1, d2, fe_s):
    blocks = {}
    for k in range(kind.LC):
        for v in range(kind.PP // 8):
            for c in range(3):
                blocks[c, k, v] = values[c, (k * kind.PP) // 8 + v]
    chunks = [(c, k) for c in range(3) for k in range(kind.LC)]
    cols = []
    for c, k in chunks:
        ve = jnp.concatenate([blocks[c, k, v] for v in range(kind.PP // 8)], axis=0)
        hi, lo = split(ve)
        parts = [hi, lo, hi]
        left = 128 - 3 * kind.PP
        if left:
            parts.append(jnp.zeros((left, 128), F32))
        cols.append(jnp.concatenate(parts, axis=0).astype(BF16))
    gathered = jnp.concatenate(cols, axis=1)
    grad = jnp.dot(d1[0 : kind.KQ, :].astype(BF16), gathered, preferred_element_type=F32)
    cols = []
    depth = d2.shape[1]
    for i, (c, k) in enumerate(chunks):
        piece = grad[:, i * 128 : (i + 1) * 128]
        terms = []
        for a in range(3):
            total = coef(a, 0, k) * piece[0 : kind.QP]
            for b in (1, 2):
                total = total + coef(a, b, k) * piece[b * kind.QP : (b + 1) * kind.QP]
            terms.append(total)
        flux = jnp.concatenate(terms, axis=0)
        hi, lo = split(flux)
        parts = [hi, lo, hi]
        left = depth - 3 * kind.KQ
        if left:
            parts.append(jnp.zeros((left, 128), F32))
        cols.append(jnp.concatenate(parts, axis=0).astype(BF16))
    flux = jnp.concatenate(cols, axis=1)
    fe = jnp.dot(d2[0 : kind.PP, :].astype(BF16), flux, preferred_element_type=F32)
    for i, (c, k) in enumerate(chunks):
        fe_s[c, k * kind.PP : (k + 1) * kind.PP, :] = fe[:, i * 128 : (i + 1) * 128]


def sum_sorted(kind, plan_s, scan, fe_s, cx_s):
    sub = iota2((8, 128), 0)
    terms = {}
    both = []
    for w in range(kind.W8):
        found = gather_three(
            plan_s[0, w * 8 : w * 8 + 8, :],
            plan_s[1, w * 8 : w * 8 + 8, :],
            lambda c, r: fe_s[c, w * 8 + r : w * 8 + r + 1, :],
            [r for r in range(8) if (w * 8 + r) % kind.PP < kind.P],
        )
        for c in range(3):
            hi, lo = split(found[c])
            both.append(jnp.concatenate([hi, lo], axis=1))
            upto = found[c]
            for dist in (1, 2, 4):
                upto = upto + jnp.where(sub >= dist, pltpu.roll(upto, dist, 0), 0.0)
            terms[w, c] = upto
    sums = jnp.dot(
        jnp.concatenate(both, axis=0).astype(BF16), scan[...], preferred_element_type=F32
    )
    for w in range(kind.W8):
        for c in range(3):
            at = (w * 3 + c) * 8
            ahead = sums[at : at + 8]
            for dist in (4, 2, 1):
                ahead = ahead + pltpu.roll(ahead, dist, 0)
            cx_s[c, w * 8 : w * 8 + 8, :] = terms[w, c] + ahead


def read_ends(kind, v, pos_s, cx_s):
    total = None
    for w in range(kind.W8):
        found = gather_three(
            pos_s[v, w, 0],
            pos_s[v, w, 1],
            lambda c, r: cx_s[c, w * 8 + r : w * 8 + r + 1, :],
            range(8),
        )
        total = found if total is None else [a + b for a, b in zip(total, found)]
    return total


def node_forces(kind, pos_s, cx_s, f_s):
    corner_row = iota2((kind.NRP, 128), 0)
    corner_lane = iota2((kind.NRP, 128), 1)
    found = [read_ends(kind, v, pos_s, cx_s) for v in range(kind.NRP // 8)]
    for c in range(3):
        ends = jnp.concatenate([block[c] for block in found], axis=0)
        before = pltpu.roll(ends, 1, 1)
        above = pltpu.roll(before, 1, 0)
        before = jnp.where(corner_lane == 0, above, before)
        before = jnp.where((corner_lane == 0) & (corner_row == 0), 0.0, before)
        forces = ends - before
        for r in range(kind.NR):
            f_s[c : c + 1, r * 128 : (r + 1) * 128] = forces[r : r + 1, :]


def pick(kind, source, index):
    idx_row, idx_lane = spread(index >> 7), spread(index & 127)
    out = jnp.zeros((8, 128), F32)
    for r in range(kind.NR):
        out = jnp.where(
            idx_row == r, lane_take(source[:, r * 128 : (r + 1) * 128], idx_lane), out
        )
    return out


def drop(kind, parts, hot):
    r = jnp.concatenate(parts, axis=1)
    hi, lo = split(r)
    both = jnp.concatenate([hi, lo], axis=0).astype(BF16)
    out = lax.dot_general(
        both, hot[...], (((1,), (1,)), ((), ())), preferred_element_type=F32
    )
    return out[0:8] + out[8:16]


def body(
    reg, site, reg_groups, site_groups, sub_count,
    reg_disp, reg_vel, site_disp, site_vel, reg_nodes, site_nodes, reg_coefs, site_coefs,
    reg_table, site_table, reg_minv, site_minv, reg_send, reg_recv, site_send, site_recv,
    slot_fill, layer_src, layer_fill, layer_dst, layer_stiff,
    reg_out, site_out,
    u_r, prev_r, f_r, wide_1, wide_2, node_r, key_r, plan_r, pos_r, hot_r, fe_r, cx_r, coef_r,
    u_s, prev_s, f_s, tpad_s, d1_s, d2_s, node_s, key_s, plan_s, pos_s, hot_s, fe_s, cx_s,
    hot_l, kept, slot_c, equal, minv_c, small, scan, fills, sends, recvs, layer_out, layer_in,
    send_sem, recv_sem, layer_send_sem, layer_recv_sem,
):
    grp = lax.axis_index("grp")
    sub = lax.axis_index("sub")
    is_site = grp >= reg_groups
    has_lower = sub > 0
    has_upper = sub < sub_count - 1
    source = grp // site_groups
    target = reg_groups + grp % site_groups
    barrier = pltpu.get_barrier_semaphore()

    def hello(g, s):
        pl.semaphore_signal(barrier, inc=1, device_id=(g, s), device_id_type=MESH)

    @pl.when(has_lower)
    def _():
        hello(grp, sub - 1)

    @pl.when(has_upper)
    def _():
        hello(grp, sub + 1)

    @pl.when(is_site)
    def _():
        for m in range(3):
            hello(m * site_groups + grp - reg_groups, sub)

    @pl.when(jnp.logical_not(is_site))
    def _():
        hello(target, sub)

    for there, side in ((has_lower, 0), (has_upper, 1)):

        @pl.when(jnp.logical_not(there))
        def _():
            for n in range(STEPS):
                recvs[n, side] = jnp.zeros((8, 128), F32)

    lane = iota2((8, 128), 1)
    live = iota2((8, 128), 0) < 3
    greeted = has_lower.astype(jnp.int32) + has_upper.astype(jnp.int32) + jnp.where(is_site, 3, 1)

    def edge(n, side):
        peer = sub - 1 if side == 0 else sub + 1
        return pltpu.make_async_remote_copy(
            src_ref=sends.at[n, side, 0:3],
            dst_ref=recvs.at[n, 1 - side, 0:3],
            send_sem=send_sem.at[n, side],
            recv_sem=recv_sem.at[n, 1 - side],
            device_id=(grp, peer),
            device_id_type=MESH,
        )

    def layer_copy(n, m):
        return pltpu.make_async_remote_copy(
            src_ref=layer_out.at[n, 0:3],
            dst_ref=layer_in.at[n, m, 0:3],
            send_sem=layer_send_sem.at[n],
            recv_sem=layer_recv_sem.at[n, m],
            device_id=(target, sub),
            device_id_type=MESH,
        )

    sides = ((has_lower, 0), (has_upper, 1))

    def exchange(kind, n, pos, cx):
        found = read_ends(kind, kind.NRP // 8, pos, cx)
        for there, side in sides:
            for c in range(3):
                force = found[c][2 * side : 2 * side + 1] - found[c][2 * side + 1 : 2 * side + 2]
                sends[n, side, c : c + 1, :] = jnp.where(lane[0:1] < fills[side : side + 1, :], force, 0.0)

            @pl.when(there)
            def _():
                edge(n, side).start()

    def arrive(n):
        for there, side in sides:

            @pl.when(there)
            def _():
                edge(n, 1 - side).wait_recv()

    def arrived(n, side):
        return jnp.where(live, recvs[n, side], 0.0)

    def finish(n, carry):
        for there, side in sides:

            @pl.when(there)
            def _():
                edge(n, side).wait_send()

        return carry

    setup_scan(scan)
    sends[...] = jnp.zeros(sends.shape, F32)

    @pl.when(jnp.logical_not(is_site))
    def _():
        kind = reg
        setup_state(kind, reg_disp, reg_vel, u_r, prev_r)
        f_r[...] = jnp.zeros(f_r.shape, F32)
        wide_1[...] = jnp.zeros(wide_1.shape, F32)
        setup_wide(kind, reg_table, wide_1, wide_2)
        coef_r[...] = jnp.zeros(coef_r.shape, F32)
        coef_r[:, :, 0 : kind.Q, :] = reg_coefs[0, 0]
        setup_plan(kind, reg_nodes, reg_send, node_r, key_r, plan_r, pos_r)
        pl.semaphore_wait(barrier, greeted)
        for i in range(2):
            fills[i : i + 1, :] = jnp.broadcast_to(slot_fill[0, :, i : i + 1], (1, 128))
        fills[2:3, :] = jnp.broadcast_to(layer_fill[...], (1, 128))

        def step(n, carry):
            small_products(
                kind, gather_nodes(kind, u_r, node_r),
                lambda a, b, k: coef_r[a, b, :, k * 128 : (k + 1) * 128],
                wide_1, wide_2, fe_r,
            )
            sum_sorted(kind, plan_r, scan, fe_r, cx_r)
            exchange(kind, n, pos_r, cx_r)

            @pl.when(n == 0)
            def _():
                setup_ends(kind, key_r, pos_r)
                setup_hot(kind, [lambda i=i: reg_recv[0, 0, i : i + 1, :] for i in range(2)], hot_r)

            node_forces(kind, pos_r, cx_r, f_r)
            minv = reg_minv[0]
            now = u_r[...]
            ahead = 2.0 * now - prev_r[...] + minv * f_r[...]
            prev_r[...] = now
            arrive(n)
            u_r[...] = ahead + minv * drop(kind, [arrived(n, i) for i in range(2)], hot_r)
            found = pick(kind, u_r, layer_src[0])
            layer_out[n] = jnp.where(lane < fills[2:3, :], found, 0.0)
            layer_copy(n, source).start()
            return carry

        lax.fori_loop(0, STEPS, step, 0)
        for c in range(3):
            reg_out[0, c] = u_r[c : c + 1, :]
        site_out[...] = jnp.zeros(site_out.shape, F32)

        def drain(n, carry):
            layer_copy(n, source).wait_send()
            return finish(n, carry)

        lax.fori_loop(0, STEPS, drain, 0)

    @pl.when(is_site)
    def _():
        kind = site
        setup_state(kind, site_disp, site_vel, u_s, prev_s)
        f_s[...] = jnp.zeros(f_s.shape, F32)
        setup_tables(kind, site_table, tpad_s, d1_s, d2_s)
        setup_plan(kind, site_nodes, site_send, node_s, key_s, plan_s, pos_s)
        pl.semaphore_wait(barrier, greeted)
        for i in range(2):
            fills[i : i + 1, :] = jnp.broadcast_to(slot_fill[0, :, i + 2 : i + 3], (1, 128))

        slot_c[...] = jnp.full(slot_c.shape, 1000, jnp.int32)
        slot_c[1] = jnp.zeros(slot_c.shape[1:], jnp.int32)
        small[...] = jnp.zeros(small.shape, F32)
        hot_s[...] = jnp.zeros(hot_s.shape, BF16)

        def keep_gathered(field):
            for (c, w), block in gather_nodes(kind, field, node_s).items():
                kept[c, w * 8 : w * 8 + 8, :] = block

        def complete():
            last = jnp.concatenate([small[0:8], small[8:16]], axis=0)
            out = lax.dot_general(
                last.astype(BF16), hot_s[...], (((1,), (1,)), ((), ())), preferred_element_type=F32
            )
            return u_s[...] + site_minv[0] * (out[0:8] + out[8:16])

        keep_gathered(u_s)

        def step(n, carry):
            values = {}
            for w in range(kind.W8):
                found = gather_three(
                    slot_c[0, w * 8 : w * 8 + 8, :],
                    slot_c[1, w * 8 : w * 8 + 8, :],
                    lambda c, r: small[16 + c : 17 + c, r * 128 : (r + 1) * 128],
                    range(2),
                )
                for c in range(3):
                    values[c, w] = kept[c, w * 8 : w * 8 + 8, :] + found[c]
            large_products(
                kind, values, lambda a, b, k: site_coefs[0, 0, a, b], d1_s, d2_s, fe_s
            )
            sum_sorted(kind, plan_s, scan, fe_s, cx_s)
            exchange(kind, n, pos_s, cx_s)
            now = complete()

            @pl.when(n == 0)
            def _():
                setup_ends(kind, key_s, pos_s)
                setup_hot(kind, [lambda i=i: site_recv[0, 0, i : i + 1, :] for i in range(2)], hot_s)
                setup_hot(kind, [lambda i=i: layer_dst[0, i] for i in range(3)], hot_l)
                setup_compact(kind, site_recv, site_minv[0], node_s, hot_s, equal, minv_c, slot_c)

            node_forces(kind, pos_s, cx_s, f_s)
            minv = site_minv[0]
            ahead = 2.0 * now - prev_s[...] + minv * f_s[...]
            prev_s[...] = now
            parts = []
            for m in range(3):
                layer_copy(n, m).wait_recv()
                parts.append(jnp.where(live, layer_in[n, m], 0.0) * layer_stiff[0, m])
            u_s[...] = ahead + minv * drop(kind, parts, hot_l)

            @pl.when(n < STEPS - 1)
            def _():
                keep_gathered(u_s)

            arrive(n)
            hi, lo = split(jnp.concatenate([arrived(n, i) for i in range(2)], axis=1))
            small[0:8] = hi
            small[8:16] = lo
            sums = mm(jnp.concatenate([hi, lo], axis=0), equal[...])
            small[16:24] = (sums[0:8] + sums[8:16]) * minv_c[...]
            return carry

        lax.fori_loop(0, STEPS, step, 0)
        u_s[...] = complete()
        for c in range(3):
            site_out[0, c] = u_s[c : c + 1, :]
        reg_out[...] = jnp.zeros(reg_out.shape, F32)
        lax.fori_loop(0, STEPS, finish, 0)


def kind_scratch(kind, tables):
    i32 = jnp.int32
    return [
        pltpu.VMEM((8, kind.N), F32),
        pltpu.VMEM((8, kind.N), F32),
        pltpu.VMEM((8, kind.N), F32),
        *tables,
        pltpu.VMEM((kind.SR, 128), i32),
        pltpu.VMEM((kind.SR, 128), i32),
        pltpu.VMEM((2, kind.SR, 128), i32),
        pltpu.VMEM((kind.NRP // 8 + 1, kind.W8, 2, 8, 128), i32),
        pltpu.VMEM((kind.N, 256), BF16),
        pltpu.VMEM((3, kind.SR, 128), F32),
        pltpu.VMEM((3, kind.SR, 128), F32),
    ]


def shards(*args):
    group_count = lax.axis_size("grp")
    site_groups = group_count // 4
    reg_groups = 3 * site_groups
    reg = Kind(args[4].shape[2], args[6].shape[4], args[4].shape[3], args[0].shape[3])
    site = Kind(args[5].shape[2], args[7].shape[4], args[5].shape[3], args[2].shape[3])
    args = list(args)
    for i in (0, 1, 2, 3, 4, 5, 19, 20):
        args[i] = jnp.transpose(args[i], (0, 2, 1, 3))
    args[9] = args[9].T
    vmem = pl.BlockSpec(memory_space=pltpu.VMEM)
    in_specs = [vmem] * len(args)
    kernel = functools.partial(body, reg, site, reg_groups, site_groups, lax.axis_size("sub"))
    outs = pl.pallas_call(
        kernel,
        name="drm_window",
        out_shape=(
            pltpu.VMEM((1, 3, 1, reg.N), F32),
            pltpu.VMEM((1, 3, 1, site.N), F32),
        ),
        in_specs=in_specs,
        out_specs=(vmem, vmem),
        scratch_shapes=kind_scratch(
            reg,
            [
                pltpu.VMEM((reg.P, 24, 128), F32),
                pltpu.VMEM((3 * reg.Q, reg.PP, 128), F32),
            ],
        )
        + [pltpu.VMEM((3, 3, reg.QP, reg.E), F32)]
        + kind_scratch(
            site,
            [
                pltpu.VMEM((128, 128), F32),
                pltpu.VMEM((128, 128), F32),
                pltpu.VMEM((128, pad_to(3 * site.KQ, 128)), F32),
            ],
        )
        + [
            pltpu.VMEM((site.N, 384), BF16),
            pltpu.VMEM((3, site.SR, 128), F32),
            pltpu.VMEM((2, site.SR, 128), jnp.int32),
            pltpu.VMEM((256, 256), BF16),
            pltpu.VMEM((8, 256), F32),
            pltpu.VMEM((24, 256), F32),
            pltpu.VMEM((256, 128), BF16),
            pltpu.VMEM((8, 128), jnp.int32),
            pltpu.VMEM((STEPS, 2, 8, 128), F32),
            pltpu.VMEM((STEPS, 2, 8, 128), F32),
            pltpu.VMEM((STEPS, 8, 128), F32),
            pltpu.VMEM((STEPS, 3, 8, 128), F32),
            pltpu.SemaphoreType.DMA((STEPS, 2)),
            pltpu.SemaphoreType.DMA((STEPS, 2)),
            pltpu.SemaphoreType.DMA((STEPS,)),
            pltpu.SemaphoreType.DMA((STEPS, 3)),
        ],
        compiler_params=pltpu.CompilerParams(collective_id=0, has_side_effects=True),
    )(*args)
    return tuple(jnp.transpose(out, (0, 2, 1, 3)) for out in outs)


def solution(mesh):
    whole = P("grp", "sub")
    specs = [whole] * 21
    specs[8] = P()
    specs[9] = P()
    return jax.shard_map(
        shards,
        mesh=mesh,
        in_specs=tuple(specs),
        out_specs=(whole, whole),
        check_vma=False,
    )
```

```python
import functools

import jax
import jax.numpy as jnp
from jax import lax
from jax.experimental import pallas as pl
from jax.experimental.pallas import tpu as pltpu
from jax.sharding import PartitionSpec as P

STEPS = 8
MESH = pl.DeviceIdType.MESH
SHIFT = 13
BIG = 2047 << SHIFT
F32 = jnp.float32
BF16 = jnp.bfloat16


def pad_to(value, unit):
    return -(-value // unit) * unit


class Kind:
    def __init__(self, points, quads, elems, nodes):
        self.P, self.Q, self.E, self.N = points, quads, elems, nodes
        self.LC = elems // 128
        self.NR = nodes // 128
        self.NRP = pad_to(self.NR, 8)
        self.PP = pad_to(points, 8)
        self.QP = pad_to(quads, 8)
        self.KQ = 3 * self.QP
        self.SR = self.LC * self.PP
        self.W8 = self.SR // 8


def lane_take(x, idx):
    dims = lax.GatherDimensionNumbers(
        offset_dims=(),
        collapsed_slice_dims=(1,),
        start_index_map=(1,),
        operand_batching_dims=(0,),
        start_indices_batching_dims=(0,),
    )
    return lax.gather(
        x, idx[..., None], dims, (1, 1), mode=lax.GatherScatterMode.PROMISE_IN_BOUNDS
    )


def iota2(shape, dim):
    return lax.broadcasted_iota(jnp.int32, shape, dim)


def spread(row):
    return jnp.broadcast_to(row, (8, 128))


def split(x):
    hi = x.astype(BF16).astype(F32)
    return hi, x - hi


def mm(a, b):
    return jnp.dot(a.astype(BF16), b.astype(BF16), preferred_element_type=F32)


def sort_regs(regs):
    count = len(regs)
    depth = count * 8
    row_bits = depth.bit_length() - 1
    sub = iota2((8, 128), 0)
    lane = iota2((8, 128), 1)

    def bit_mask(bit, v):
        if bit < 3:
            return (sub >> bit) & 1
        if bit < row_bits:
            return (v >> (bit - 3)) & 1
        if bit >= row_bits + 7:
            return 0
        return (lane >> (bit - row_bits)) & 1

    total_bits = row_bits + 7
    for m in range(1, total_bits + 1):
        jb = m
        while jb > 0:
            jb -= 1
            new = list(regs)
            if jb - 1 >= row_bits:
                far, near = 1 << (jb - row_bits), 1 << (jb - 1 - row_bits)
                for v in range(count):
                    x = regs[v]
                    first = (bit_mask(jb, v) ^ bit_mask(m, v)) == 1
                    second = (bit_mask(jb - 1, v) ^ bit_mask(m, v)) == 1
                    other = lane_take(x, lane ^ far)
                    mine = jnp.where(first, jnp.maximum(x, other), jnp.minimum(x, other))
                    x = lane_take(regs[v], lane ^ near)
                    other = lane_take(regs[v], lane ^ (far + near))
                    theirs = jnp.where(first, jnp.maximum(x, other), jnp.minimum(x, other))
                    new[v] = jnp.where(
                        second, jnp.maximum(mine, theirs), jnp.minimum(mine, theirs)
                    )
                regs = new
                jb -= 1
                continue
            if 3 <= jb < row_bits:
                step = 1 << (jb - 3)
                for v in range(count):
                    if v & step:
                        continue
                    a, b = regs[v], regs[v + step]
                    low, high = jnp.minimum(a, b), jnp.maximum(a, b)
                    down = bit_mask(m, v)
                    if isinstance(down, int):
                        new[v], new[v + step] = (high, low) if down else (low, high)
                    else:
                        new[v] = jnp.where(down == 1, high, low)
                        new[v + step] = jnp.where(down == 1, low, high)
            else:
                for v in range(count):
                    x = regs[v]
                    if jb < 3:
                        dist = 1 << jb
                        if dist == 4:
                            other = pltpu.roll(x, 4, 0)
                        else:
                            other = jnp.where(
                                bit_mask(jb, v) == 1, pltpu.roll(x, dist, 0), pltpu.roll(x, 8 - dist, 0)
                            )
                    else:
                        dist = 1 << (jb - row_bits)
                        other = lane_take(x, lane ^ dist)
                    take_max = bit_mask(jb, v) ^ bit_mask(m, v)
                    new[v] = jnp.where(take_max == 1, jnp.maximum(x, other), jnp.minimum(x, other))
            regs = new
    return regs


def gather_three(idx_row, idx_lane, load_row, rows):
    out = [jnp.zeros((8, 128), F32) for _ in range(3)]
    for r in rows:
        here = idx_row == r
        for c in range(3):
            out[c] = jnp.where(here, lane_take(spread(load_row(c, r)), idx_lane), out[c])
    return out


def setup_state(kind, disp, vel, u, prev):
    for ref in (u, prev):
        ref[...] = jnp.zeros(ref.shape, F32)
    for c in range(3):
        u[c : c + 1, :] = disp[0, c]
        prev[c : c + 1, :] = disp[0, c] - vel[0, c]


def setup_tables(kind, table, tpad, d1, d2):
    tpad[...] = jnp.zeros(tpad.shape, F32)
    tpad[0 : kind.P, 0 : kind.KQ] = table[...]
    across = tpad[...]
    whole = across.T
    hi, lo = split(across[0 : kind.PP])
    stack = [hi, hi, lo]
    left = 128 - 3 * kind.PP
    if left:
        stack.append(jnp.zeros((left, 128), F32))
    d1[...] = jnp.concatenate(stack, axis=0).T
    hi, lo = split(-whole[0 : kind.KQ])
    depth = d2.shape[1]
    stack = [hi, hi, lo]
    left = depth - 3 * kind.KQ
    if left:
        stack.append(jnp.zeros((left, 128), F32))
    stack = jnp.concatenate(stack, axis=0)
    for k in range(depth // 128):
        d2[:, k * 128 : (k + 1) * 128] = stack[k * 128 : (k + 1) * 128].T


def setup_plan(kind, nodes, send_map, node_s, key_s, plan_s, pos_s):
    sub = iota2((8, 128), 0)
    lane = iota2((8, 128), 1)
    node_s[...] = jnp.zeros(node_s.shape, jnp.int32)
    for k in range(kind.LC):
        for p in range(kind.P):
            at = k * kind.PP + p
            node_s[at : at + 1, :] = nodes[0, p, :, k * 128 : (k + 1) * 128]
    for w in range(kind.W8):
        inside = ((sub + w * 8) % kind.PP) < kind.P
        found = jnp.where(inside, node_s[w * 8 : w * 8 + 8, :], BIG >> SHIFT)
        keys = sort_regs([(found << SHIFT) | (sub << 7) | lane])[0]
        key_s[w * 8 : w * 8 + 8, :] = keys
        slot = keys & ((1 << SHIFT) - 1)
        plan_s[0, w * 8 : w * 8 + 8, :] = jnp.where(keys < BIG, slot >> 7, 1000)
        plan_s[1, w * 8 : w * 8 + 8, :] = slot & 127
    sent = jnp.zeros((8, 128), jnp.int32)
    for side in range(2):
        wanted = spread(send_map[0, 0, side : side + 1, :])
        sent = jnp.where(sub == 2 * side, wanted + 1, sent)
        sent = jnp.where(sub == 2 * side + 1, wanted, sent)
    find_places(kind, [(kind.NRP // 8, sent << SHIFT)], key_s, pos_s)


def setup_ends(kind, key_s, pos_s):
    sub = iota2((8, 128), 0)
    lane = iota2((8, 128), 1)
    targets = [(v, ((sub + v * 8) * 128 + lane + 1) << SHIFT) for v in range(kind.NRP // 8)]
    find_places(kind, targets, key_s, pos_s)


def find_places(kind, targets, key_s, pos_s):
    for w in range(kind.W8):
        last = spread(key_s[w * 8 + 7 : w * 8 + 8, :])
        for v, target in targets:
            column = jnp.zeros((8, 128), jnp.int32)
            for step in (32, 8, 2):
                passed = [
                    jnp.where(lane_take(last, column + (i * step - 1)) < target, step, 0)
                    for i in (1, 2, 3)
                ]
                column = column + passed[0] + passed[1] + passed[2]
            column = jnp.where(lane_take(last, column) < target, column + 1, column)
            place = column * 8 - 1
            for r in range(8):
                row = spread(key_s[w * 8 + r : w * 8 + r + 1, :])
                place = place + jnp.where(lane_take(row, column) < target, 1, 0)
            pos_s[v, w, 0] = jnp.where(place < 0, 1000, place & 7)
            pos_s[v, w, 1] = jnp.where(place < 0, 0, place >> 3)


def setup_scan(scan):
    row = iota2(scan.shape, 0) % 128
    col = iota2(scan.shape, 1)
    scan[...] = jnp.where(row < col, 1.0, 0.0).astype(BF16)


def setup_hot(kind, maps, hot):
    rows = iota2((kind.N, 128), 0)
    for k, load in enumerate(maps):
        hot[:, k * 128 : (k + 1) * 128] = jnp.where(rows == load(), 1.0, 0.0).astype(BF16)


def gather_nodes(kind, u, node_s):
    blocks = {}
    for w in range(kind.W8):
        index = node_s[w * 8 : w * 8 + 8, :]
        found = gather_three(
            index >> 7,
            index & 127,
            lambda c, r: u[c : c + 1, r * 128 : (r + 1) * 128],
            range(kind.NR),
        )
        for c in range(3):
            blocks[c, w] = found[c]
    return blocks


def setup_compact(kind, recv_map, minv, node_s, hot, equal, minv_c, slot_j):
    rows = [recv_map[0, 0, i : i + 1, :] for i in range(2)]
    wide = jnp.concatenate(rows, axis=1)
    down = jnp.concatenate(
        [jnp.broadcast_to(row.astype(F32), (128, 128)).T for row in rows], axis=0
    ).astype(jnp.int32)
    across = jnp.concatenate([down, down], axis=1) == wide
    equal[...] = jnp.where(across, 1.0, 0.0).astype(BF16)
    row = iota2((256, 256), 0)
    col = iota2((256, 256), 1)
    earlier = jnp.where(across & (row < col), 1.0, 0.0)
    count = mm(jnp.ones((16, 256), F32), earlier)
    name = jnp.where(count < 0.5, iota2((16, 256), 1) + 1, 0).astype(F32)
    table = lax.dot_general(
        name.astype(BF16), hot[...], (((1,), (1,)), ((), ())), preferred_element_type=F32
    )
    spread_minv = jnp.broadcast_to(minv, (8, kind.N))
    for i in range(2):
        minv_c[:, i * 128 : (i + 1) * 128] = pick(kind, spread_minv, rows[i])
    for w in range(kind.W8):
        index = node_s[w * 8 : w * 8 + 8, :]
        idx_row, idx_lane = index >> 7, index & 127
        found = jnp.zeros((8, 128), F32)
        for r in range(kind.NR):
            part = lane_take(spread(table[0:1, r * 128 : (r + 1) * 128]), idx_lane)
            found = jnp.where(idx_row == r, part, found)
        found = found.astype(jnp.int32) - 1
        slot_j[0, w * 8 : w * 8 + 8, :] = jnp.where(found < 0, 1000, found >> 7)
        slot_j[1, w * 8 : w * 8 + 8, :] = jnp.where(found < 0, 0, found & 127)


def setup_wide(kind, table, wide_1, wide_2):
    for b in range(3):
        for q in range(kind.Q):
            entry = jnp.concatenate(
                [table[b * kind.Q + q : b * kind.Q + q + 1, :], jnp.zeros((1, 128 - kind.P), F32)],
                axis=1,
            )
            down = jnp.broadcast_to(entry, (128, 128)).T
            wide_2[b * kind.Q + q] = -down[0 : kind.PP]
    for p in range(kind.P):
        for b in range(3):
            for q in range(kind.Q):
                wide_1[p, b * 8 + q : b * 8 + q + 1, :] = -wide_2[b * kind.Q + q, p : p + 1, :]


def small_products(kind, values, coef, wide_1, wide_2, fe_s):
    for k in range(kind.LC):
        for c in range(3):
            grad = [None] * 3
            for p in range(kind.P):
                block = values[c, (k * kind.PP + p) // 8]
                row = jnp.broadcast_to(block[p % 8 : p % 8 + 1], (8, 128))
                for b in range(3):
                    term = wide_1[p, b * 8 : b * 8 + 8, :] * row
                    grad[b] = term if p == 0 else grad[b] + term
            terms = [None] * (kind.PP // 8)
            for a in range(3):
                flux = coef(a, 0, k) * grad[0] + coef(a, 1, k) * grad[1] + coef(a, 2, k) * grad[2]
                for q in range(kind.Q):
                    row = jnp.broadcast_to(flux[q : q + 1], (8, 128))
                    for v in range(kind.PP // 8):
                        term = wide_2[a * kind.Q + q, v * 8 : v * 8 + 8, :] * row
                        terms[v] = term if a + q == 0 else terms[v] + term
            for v in range(kind.PP // 8):
                fe_s[c, k * kind.PP + v * 8 : k * kind.PP + v * 8 + 8, :] = terms[v]


def large_products(kind, values, coef, d1, d2, fe_s):
    blocks = {}
    for k in range(kind.LC):
        for v in range(kind.PP // 8):
            for c in range(3):
                blocks[c, k, v] = values[c, (k * kind.PP) // 8 + v]
    chunks = [(c, k) for c in range(3) for k in range(kind.LC)]
    cols = []
    for c, k in chunks:
        ve = jnp.concatenate([blocks[c, k, v] for v in range(kind.PP // 8)], axis=0)
        hi, lo = split(ve)
        parts = [hi, lo, hi]
        left = 128 - 3 * kind.PP
        if left:
            parts.append(jnp.zeros((left, 128), F32))
        cols.append(jnp.concatenate(parts, axis=0).astype(BF16))
    gathered = jnp.concatenate(cols, axis=1)
    grad = jnp.dot(d1[0 : kind.KQ, :].astype(BF16), gathered, preferred_element_type=F32)
    cols = []
    depth = d2.shape[1]
    for i, (c, k) in enumerate(chunks):
        piece = grad[:, i * 128 : (i + 1) * 128]
        terms = []
        for a in range(3):
            total = coef(a, 0, k) * piece[0 : kind.QP]
            for b in (1, 2):
                total = total + coef(a, b, k) * piece[b * kind.QP : (b + 1) * kind.QP]
            terms.append(total)
        flux = jnp.concatenate(terms, axis=0)
        hi, lo = split(flux)
        parts = [hi, lo, hi]
        left = depth - 3 * kind.KQ
        if left:
            parts.append(jnp.zeros((left, 128), F32))
        cols.append(jnp.concatenate(parts, axis=0).astype(BF16))
    flux = jnp.concatenate(cols, axis=1)
    fe = jnp.dot(d2[0 : kind.PP, :].astype(BF16), flux, preferred_element_type=F32)
    for i, (c, k) in enumerate(chunks):
        fe_s[c, k * kind.PP : (k + 1) * kind.PP, :] = fe[:, i * 128 : (i + 1) * 128]


def sum_sorted(kind, plan_s, scan, fe_s, cx_s):
    sub = iota2((8, 128), 0)
    terms = {}
    both = []
    for w in range(kind.W8):
        found = gather_three(
            plan_s[0, w * 8 : w * 8 + 8, :],
            plan_s[1, w * 8 : w * 8 + 8, :],
            lambda c, r: fe_s[c, w * 8 + r : w * 8 + r + 1, :],
            [r for r in range(8) if (w * 8 + r) % kind.PP < kind.P],
        )
        for c in range(3):
            hi, lo = split(found[c])
            both.append(jnp.concatenate([hi, lo], axis=1))
            upto = found[c]
            for dist in (1, 2, 4):
                upto = upto + jnp.where(sub >= dist, pltpu.roll(upto, dist, 0), 0.0)
            terms[w, c] = upto
    sums = jnp.dot(
        jnp.concatenate(both, axis=0).astype(BF16), scan[...], preferred_element_type=F32
    )
    for w in range(kind.W8):
        for c in range(3):
            at = (w * 3 + c) * 8
            ahead = sums[at : at + 8]
            for dist in (4, 2, 1):
                ahead = ahead + pltpu.roll(ahead, dist, 0)
            cx_s[c, w * 8 : w * 8 + 8, :] = terms[w, c] + ahead


def read_ends(kind, v, pos_s, cx_s):
    total = None
    for w in range(kind.W8):
        found = gather_three(
            pos_s[v, w, 0],
            pos_s[v, w, 1],
            lambda c, r: cx_s[c, w * 8 + r : w * 8 + r + 1, :],
            range(8),
        )
        total = found if total is None else [a + b for a, b in zip(total, found)]
    return total


def node_forces(kind, pos_s, cx_s, f_s):
    corner_row = iota2((kind.NRP, 128), 0)
    corner_lane = iota2((kind.NRP, 128), 1)
    found = [read_ends(kind, v, pos_s, cx_s) for v in range(kind.NRP // 8)]
    for c in range(3):
        ends = jnp.concatenate([block[c] for block in found], axis=0)
        before = pltpu.roll(ends, 1, 1)
        above = pltpu.roll(before, 1, 0)
        before = jnp.where(corner_lane == 0, above, before)
        before = jnp.where((corner_lane == 0) & (corner_row == 0), 0.0, before)
        forces = ends - before
        for r in range(kind.NR):
            f_s[c : c + 1, r * 128 : (r + 1) * 128] = forces[r : r + 1, :]


def pick(kind, source, index):
    idx_row, idx_lane = spread(index >> 7), spread(index & 127)
    out = jnp.zeros((8, 128), F32)
    for r in range(kind.NR):
        out = jnp.where(
            idx_row == r, lane_take(source[:, r * 128 : (r + 1) * 128], idx_lane), out
        )
    return out


def drop(kind, parts, hot):
    r = jnp.concatenate(parts, axis=1)
    hi, lo = split(r)
    both = jnp.concatenate([hi, lo], axis=0).astype(BF16)
    out = lax.dot_general(
        both, hot[...], (((1,), (1,)), ((), ())), preferred_element_type=F32
    )
    return out[0:8] + out[8:16]


def body(
    reg, site, reg_groups, site_groups, sub_count,
    reg_disp, reg_vel, site_disp, site_vel, reg_nodes, site_nodes, reg_coefs, site_coefs,
    reg_table, site_table, reg_minv, site_minv, reg_send, reg_recv, site_send, site_recv,
    slot_fill, layer_src, layer_fill, layer_dst, layer_stiff,
    reg_out, site_out,
    u_r, prev_r, f_r, wide_1, wide_2, node_r, key_r, plan_r, pos_r, hot_r, fe_r, cx_r, coef_r,
    u_s, prev_s, f_s, tpad_s, d1_s, d2_s, node_s, key_s, plan_s, pos_s, hot_s, fe_s, cx_s,
    hot_l, kept, slot_c, equal, minv_c, small, scan, fills, sends, recvs, layer_out, layer_in,
    send_sem, recv_sem, layer_send_sem, layer_recv_sem,
):
    grp = lax.axis_index("grp")
    sub = lax.axis_index("sub")
    is_site = grp >= reg_groups
    has_lower = sub > 0
    has_upper = sub < sub_count - 1
    source = grp // site_groups
    target = reg_groups + grp % site_groups
    barrier = pltpu.get_barrier_semaphore()

    def hello(g, s):
        pl.semaphore_signal(barrier, inc=1, device_id=(g, s), device_id_type=MESH)

    @pl.when(has_lower)
    def _():
        hello(grp, sub - 1)

    @pl.when(has_upper)
    def _():
        hello(grp, sub + 1)

    @pl.when(is_site)
    def _():
        for m in range(3):
            hello(m * site_groups + grp - reg_groups, sub)

    @pl.when(jnp.logical_not(is_site))
    def _():
        hello(target, sub)

    for there, side in ((has_lower, 0), (has_upper, 1)):

        @pl.when(jnp.logical_not(there))
        def _():
            for n in range(STEPS):
                recvs[n, side] = jnp.zeros((8, 128), F32)

    lane = iota2((8, 128), 1)
    live = iota2((8, 128), 0) < 3
    greeted = has_lower.astype(jnp.int32) + has_upper.astype(jnp.int32) + jnp.where(is_site, 3, 1)

    def edge(n, side):
        peer = sub - 1 if side == 0 else sub + 1
        return pltpu.make_async_remote_copy(
            src_ref=sends.at[n, side, 0:3],
            dst_ref=recvs.at[n, 1 - side, 0:3],
            send_sem=send_sem.at[n, side],
            recv_sem=recv_sem.at[n, 1 - side],
            device_id=(grp, peer),
            device_id_type=MESH,
        )

    def layer_copy(n, m):
        return pltpu.make_async_remote_copy(
            src_ref=layer_out.at[n, 0:3],
            dst_ref=layer_in.at[n, m, 0:3],
            send_sem=layer_send_sem.at[n],
            recv_sem=layer_recv_sem.at[n, m],
            device_id=(target, sub),
            device_id_type=MESH,
        )

    sides = ((has_lower, 0), (has_upper, 1))

    def exchange(kind, n, pos, cx):
        found = read_ends(kind, kind.NRP // 8, pos, cx)
        for there, side in sides:
            for c in range(3):
                force = found[c][2 * side : 2 * side + 1] - found[c][2 * side + 1 : 2 * side + 2]
                sends[n, side, c : c + 1, :] = jnp.where(lane[0:1] < fills[side : side + 1, :], force, 0.0)

            @pl.when(there)
            def _():
                edge(n, side).start()

    def arrive(n):
        for there, side in sides:

            @pl.when(there)
            def _():
                edge(n, 1 - side).wait_recv()

    def arrived(n, side):
        return jnp.where(live, recvs[n, side], 0.0)

    def finish(n, carry):
        for there, side in sides:

            @pl.when(there)
            def _():
                edge(n, side).wait_send()

        return carry

    setup_scan(scan)
    sends[...] = jnp.zeros(sends.shape, F32)

    @pl.when(jnp.logical_not(is_site))
    def _():
        kind = reg
        setup_state(kind, reg_disp, reg_vel, u_r, prev_r)
        f_r[...] = jnp.zeros(f_r.shape, F32)
        wide_1[...] = jnp.zeros(wide_1.shape, F32)
        setup_wide(kind, reg_table, wide_1, wide_2)
        coef_r[...] = jnp.zeros(coef_r.shape, F32)
        coef_r[:, :, 0 : kind.Q, :] = reg_coefs[0, 0]
        setup_plan(kind, reg_nodes, reg_send, node_r, key_r, plan_r, pos_r)
        pl.semaphore_wait(barrier, greeted)
        for i in range(2):
            fills[i : i + 1, :] = jnp.broadcast_to(slot_fill[0, :, i : i + 1], (1, 128))
        fills[2:3, :] = jnp.broadcast_to(layer_fill[...], (1, 128))

        def send_layer(n):
            found = pick(kind, u_r, layer_src[0])
            layer_out[n] = jnp.where(lane < fills[2:3, :], found, 0.0)
            layer_copy(n, source).start()

        def step(n, carry):
            small_products(
                kind, gather_nodes(kind, u_r, node_r),
                lambda a, b, k: coef_r[a, b, :, k * 128 : (k + 1) * 128],
                wide_1, wide_2, fe_r,
            )
            sum_sorted(kind, plan_r, scan, fe_r, cx_r)
            exchange(kind, n, pos_r, cx_r)

            @pl.when(n > 0)
            def _():
                send_layer(n - 1)

            @pl.when(n == 0)
            def _():
                setup_ends(kind, key_r, pos_r)
                setup_hot(kind, [lambda i=i: reg_recv[0, 0, i : i + 1, :] for i in range(2)], hot_r)

            node_forces(kind, pos_r, cx_r, f_r)
            minv = reg_minv[0]
            now = u_r[...]
            ahead = 2.0 * now - prev_r[...] + minv * f_r[...]
            prev_r[...] = now
            arrive(n)
            u_r[...] = ahead + minv * drop(kind, [arrived(n, i) for i in range(2)], hot_r)
            return carry

        lax.fori_loop(0, STEPS, step, 0)
        send_layer(STEPS - 1)
        for c in range(3):
            reg_out[0, c] = u_r[c : c + 1, :]
        site_out[...] = jnp.zeros(site_out.shape, F32)

        def drain(n, carry):
            layer_copy(n, source).wait_send()
            return finish(n, carry)

        lax.fori_loop(0, STEPS, drain, 0)

    @pl.when(is_site)
    def _():
        kind = site
        setup_state(kind, site_disp, site_vel, u_s, prev_s)
        f_s[...] = jnp.zeros(f_s.shape, F32)
        setup_tables(kind, site_table, tpad_s, d1_s, d2_s)
        setup_plan(kind, site_nodes, site_send, node_s, key_s, plan_s, pos_s)
        pl.semaphore_wait(barrier, greeted)
        for i in range(2):
            fills[i : i + 1, :] = jnp.broadcast_to(slot_fill[0, :, i + 2 : i + 3], (1, 128))

        slot_c[...] = jnp.full(slot_c.shape, 1000, jnp.int32)
        slot_c[1] = jnp.zeros(slot_c.shape[1:], jnp.int32)
        small[...] = jnp.zeros(small.shape, F32)
        hot_s[...] = jnp.zeros(hot_s.shape, BF16)

        def keep_gathered(field):
            for (c, w), block in gather_nodes(kind, field, node_s).items():
                kept[c, w * 8 : w * 8 + 8, :] = block

        def complete():
            last = jnp.concatenate([small[0:8], small[8:16]], axis=0)
            out = lax.dot_general(
                last.astype(BF16), hot_s[...], (((1,), (1,)), ((), ())), preferred_element_type=F32
            )
            return u_s[...] + site_minv[0] * (out[0:8] + out[8:16])

        keep_gathered(u_s)

        def step(n, carry):
            values = {}
            for w in range(kind.W8):
                found = gather_three(
                    slot_c[0, w * 8 : w * 8 + 8, :],
                    slot_c[1, w * 8 : w * 8 + 8, :],
                    lambda c, r: small[16 + c : 17 + c, r * 128 : (r + 1) * 128],
                    range(2),
                )
                for c in range(3):
                    values[c, w] = kept[c, w * 8 : w * 8 + 8, :] + found[c]
            large_products(
                kind, values, lambda a, b, k: site_coefs[0, 0, a, b], d1_s, d2_s, fe_s
            )
            sum_sorted(kind, plan_s, scan, fe_s, cx_s)
            exchange(kind, n, pos_s, cx_s)
            now = complete()

            @pl.when(n == 0)
            def _():
                setup_ends(kind, key_s, pos_s)
                setup_hot(kind, [lambda i=i: site_recv[0, 0, i : i + 1, :] for i in range(2)], hot_s)
                setup_hot(kind, [lambda i=i: layer_dst[0, i] for i in range(3)], hot_l)
                setup_compact(kind, site_recv, site_minv[0], node_s, hot_s, equal, minv_c, slot_c)

            node_forces(kind, pos_s, cx_s, f_s)
            minv = site_minv[0]
            ahead = 2.0 * now - prev_s[...] + minv * f_s[...]
            prev_s[...] = now
            parts = []
            for m in range(3):
                layer_copy(n, m).wait_recv()
                parts.append(jnp.where(live, layer_in[n, m], 0.0) * layer_stiff[0, m])
            u_s[...] = ahead + minv * drop(kind, parts, hot_l)

            @pl.when(n < STEPS - 1)
            def _():
                keep_gathered(u_s)

            arrive(n)
            hi, lo = split(jnp.concatenate([arrived(n, i) for i in range(2)], axis=1))
            small[0:8] = hi
            small[8:16] = lo
            sums = mm(jnp.concatenate([hi, lo], axis=0), equal[...])
            small[16:24] = (sums[0:8] + sums[8:16]) * minv_c[...]
            return carry

        lax.fori_loop(0, STEPS, step, 0)
        u_s[...] = complete()
        for c in range(3):
            site_out[0, c] = u_s[c : c + 1, :]
        reg_out[...] = jnp.zeros(reg_out.shape, F32)
        lax.fori_loop(0, STEPS, finish, 0)


def kind_scratch(kind, tables):
    i32 = jnp.int32
    return [
        pltpu.VMEM((8, kind.N), F32),
        pltpu.VMEM((8, kind.N), F32),
        pltpu.VMEM((8, kind.N), F32),
        *tables,
        pltpu.VMEM((kind.SR, 128), i32),
        pltpu.VMEM((kind.SR, 128), i32),
        pltpu.VMEM((2, kind.SR, 128), i32),
        pltpu.VMEM((kind.NRP // 8 + 1, kind.W8, 2, 8, 128), i32),
        pltpu.VMEM((kind.N, 256), BF16),
        pltpu.VMEM((3, kind.SR, 128), F32),
        pltpu.VMEM((3, kind.SR, 128), F32),
    ]


def shards(*args):
    group_count = lax.axis_size("grp")
    site_groups = group_count // 4
    reg_groups = 3 * site_groups
    reg = Kind(args[4].shape[2], args[6].shape[4], args[4].shape[3], args[0].shape[3])
    site = Kind(args[5].shape[2], args[7].shape[4], args[5].shape[3], args[2].shape[3])
    args = list(args)
    for i in (0, 1, 2, 3, 4, 5, 19, 20):
        args[i] = jnp.transpose(args[i], (0, 2, 1, 3))
    args[9] = args[9].T
    vmem = pl.BlockSpec(memory_space=pltpu.VMEM)
    in_specs = [vmem] * len(args)
    kernel = functools.partial(body, reg, site, reg_groups, site_groups, lax.axis_size("sub"))
    outs = pl.pallas_call(
        kernel,
        name="drm_window",
        out_shape=(
            pltpu.VMEM((1, 3, 1, reg.N), F32),
            pltpu.VMEM((1, 3, 1, site.N), F32),
        ),
        in_specs=in_specs,
        out_specs=(vmem, vmem),
        scratch_shapes=kind_scratch(
            reg,
            [
                pltpu.VMEM((reg.P, 24, 128), F32),
                pltpu.VMEM((3 * reg.Q, reg.PP, 128), F32),
            ],
        )
        + [pltpu.VMEM((3, 3, reg.QP, reg.E), F32)]
        + kind_scratch(
            site,
            [
                pltpu.VMEM((128, 128), F32),
                pltpu.VMEM((128, 128), F32),
                pltpu.VMEM((128, pad_to(3 * site.KQ, 128)), F32),
            ],
        )
        + [
            pltpu.VMEM((site.N, 384), BF16),
            pltpu.VMEM((3, site.SR, 128), F32),
            pltpu.VMEM((2, site.SR, 128), jnp.int32),
            pltpu.VMEM((256, 256), BF16),
            pltpu.VMEM((8, 256), F32),
            pltpu.VMEM((24, 256), F32),
            pltpu.VMEM((256, 128), BF16),
            pltpu.VMEM((8, 128), jnp.int32),
            pltpu.VMEM((STEPS, 2, 8, 128), F32),
            pltpu.VMEM((STEPS, 2, 8, 128), F32),
            pltpu.VMEM((STEPS, 8, 128), F32),
            pltpu.VMEM((STEPS, 3, 8, 128), F32),
            pltpu.SemaphoreType.DMA((STEPS, 2)),
            pltpu.SemaphoreType.DMA((STEPS, 2)),
            pltpu.SemaphoreType.DMA((STEPS,)),
            pltpu.SemaphoreType.DMA((STEPS, 3)),
        ],
        compiler_params=pltpu.CompilerParams(collective_id=0, has_side_effects=True),
    )(*args)
    return tuple(jnp.transpose(out, (0, 2, 1, 3)) for out in outs)


def solution(mesh):
    whole = P("grp", "sub")
    specs = [whole] * 21
    specs[8] = P()
    specs[9] = P()
    return jax.shard_map(
        shards,
        mesh=mesh,
        in_specs=tuple(specs),
        out_specs=(whole, whole),
        check_vma=False,
    )
```
